32 devices in a mesh: lat: 4 (over y, x), lon: 8 (over z, core).
Axes of the slice: x: 2, y: 2, z: 4, core: 2. Of those that a mesh axis runs over, the one named last changes fastest.
Arguments:
- right_side: float32 [8, 768, 1024], P(None, 'lat', 'lon'), may hold values from -16 to 16
- center: float32 [768, 1024], P('lat', 'lon'), may hold values from 3.7 to 5.5
- couplings: float32 [4, 768, 1024], P(None, 'lat', 'lon'), may hold values from 0.15 to 0.45
- land_sea: int32 [768, 1024], P('lat', 'lon'), may hold values 0 or 1
- fold_partner: int32 [1024], replicated, may hold values from 0 to 1023, as said below
Outputs:
- solution: float32 [8, 768, 1024], P(None, 'lat', 'lon')
- residual: float32 [8, 768, 1024], P(None, 'lat', 'lon')
The draws below stay inside these ranges and needn't reach their ends.
Inputs may be any that keep to these rules, and one draw needn't show every extreme that they name: fold_partner[i] = (s - i) mod 1024 for one integer s, so fold_partner[fold_partner[i]] = i.
All inputs are finite; a program needn't handle non-finite values. No bound on the sum of `land_sea` on one device may be relied on, other than what follows from the above.
Results may differ from the reference program's by a relative error of at most 0.0003.
Values sent between devices are 32-bit elements; how exact they have to be, the bound alone decides.
A program may use at most 64 MiB of HBM per device.

```python
import math
import jax
import jax.numpy as jnp
from jax import lax

MEMBERS = 8
ITERS = 3
NLAT = 768
NLON = 1024


def draw_right_side(key, part):
    first_key = jax.random.fold_in(key, 11)
    row_pos = jnp.arange(NLAT, dtype=jnp.float32) / NLAT
    col_pos = jnp.arange(NLON, dtype=jnp.float32) / NLON
    scale_map = jnp.exp(0.55 * (row_pos[:, None] + col_pos[None, :]))
    base = jnp.clip(jax.random.normal(first_key, (MEMBERS, NLAT, NLON), jnp.float32), -4.0, 4.0)
    values = base * scale_map[None]
    return values.astype(jnp.float32)


def draw_fold_partner(key, part):
    offset = jax.random.randint(jax.random.fold_in(key, 21), (), 0, NLON)
    return ((offset - jnp.arange(NLON, dtype=jnp.int32)) % NLON).astype(jnp.int32)


def touch_ends(values, rng, least, top_value):
    longest = values.shape.index(max(values.shape))
    spots = []
    for shift in (0, 1):
        where = [jax.random.randint(jax.random.fold_in(rng, axis), (), 0, length) for axis, length in enumerate(values.shape)]
        where[longest] = (where[longest] + shift) % values.shape[longest]
        spots.append(tuple(where))
    return values.at[spots[0]].set(least).at[spots[1]].set(top_value)


def block_scale(key, shape, shards, low, top_value):
    def one(axis_at, blocks):
        steps = jax.random.uniform(jax.random.fold_in(jax.random.fold_in(key, 6), axis_at), (blocks,), jnp.float32, low / len(shards), top_value / len(shards))
        return jnp.repeat(jnp.exp(steps), shape[axis_at] // blocks).reshape((-1,) + (1,) * (len(shape) - axis_at - 1))

    loudness = one(*shards[0])
    for cut in shards[1:]:
        loudness = loudness * one(*cut)
    return loudness


def setup_inputs(seed: int = 0) -> dict:
    arg_keys = jax.random.split(jax.random.key(seed), 6)
    return {
        "right_side": draw_right_side(jax.random.fold_in(arg_keys[5], 71), 0),
        "center": jnp.clip(3.7 + 1.8 * jax.random.uniform(arg_keys[1], (NLAT, NLON), jnp.float32) ** block_scale(arg_keys[1], (NLAT, NLON), ((0, 4), (1, 8)), -0.2, 0.2), 3.7, 5.5),
        "couplings": jnp.clip(jnp.exp(math.log(0.45) - 1.0986122 * jax.random.uniform(arg_keys[2], (4, NLAT, NLON), jnp.float32) ** block_scale(arg_keys[2], (4, NLAT, NLON), ((1, 4), (2, 8)), -0.2, 0.2)), 0.15, 0.45),
        "land_sea": touch_ends((jax.random.randint(arg_keys[3], (NLAT, NLON), 0, 5) < 4).astype(jnp.int32), jax.random.fold_in(arg_keys[3], 1), 0, 1),
        "fold_partner": draw_fold_partner(jax.random.fold_in(arg_keys[5], 71), 0),
    }


def below(values):
    return jnp.concatenate([jnp.zeros_like(values[:1]), values[:-1]], axis=0)


def reference(right_side, center, couplings, land_sea, fold_partner):
    ocean_mask = land_sea.astype(jnp.float32)
    east_coeff = couplings[0]
    north_top = couplings[1][-1]
    fold_coeff = 0.5 * (north_top + north_top[fold_partner])
    top_rows = (jnp.arange(NLAT) == NLAT - 1)[:, None]
    north_coeff = jnp.where(top_rows, fold_coeff[None, :], couplings[1])
    northeast = jnp.where(top_rows, 0.0, couplings[2])
    northwest = jnp.where(top_rows, 0.0, couplings[3])
    west_coeff = jnp.roll(east_coeff, 1, axis=1)
    south_coeff = below(north_coeff)
    southwest = jnp.roll(below(northeast), 1, axis=1)
    southeast = jnp.roll(below(northwest), -1, axis=1)

    def operate(vector):
        fold_ghost = vector[-1][fold_partner]
        upper = jnp.concatenate([vector[1:], fold_ghost[None, :]], axis=0)
        lower = below(vector)
        beside = east_coeff * jnp.roll(vector, -1, axis=1) + west_coeff * jnp.roll(vector, 1, axis=1)
        beside = beside + north_coeff * upper + south_coeff * lower
        beside = beside + northeast * jnp.roll(upper, -1, axis=1) + southwest * jnp.roll(lower, 1, axis=1)
        beside = beside + northwest * jnp.roll(upper, 1, axis=1) + southeast * jnp.roll(lower, -1, axis=1)
        return ocean_mask * (center * vector - beside)

    def solve_one(member_rhs):
        residual = ocean_mask * member_rhs
        solution = jnp.zeros_like(residual)
        scaled = residual / center
        direction = scaled
        gamma_now = jnp.sum(residual * scaled)
        for iteration in range(ITERS):
            image = operate(direction)
            step_size = gamma_now / jnp.sum(direction * image)
            solution = solution + step_size * direction
            residual = residual - step_size * image
            scaled = residual / center
            gamma_next = jnp.sum(residual * scaled)
            direction = scaled + (gamma_next / gamma_now) * direction
            gamma_now = gamma_next
        return solution, residual

    solution, residual = lax.map(solve_one, right_side)
    return solution, residual
```

```python
import functools

import jax
import jax.numpy as jnp
from jax import lax
from jax.experimental import pallas as pl
from jax.experimental.pallas import tpu as pltpu
from jax.sharding import PartitionSpec as P

ITERS = 3
MESH = pl.DeviceIdType.MESH
S_, SE_, SW_, N_, NE_, NW_ = range(6)


def kernel(
    lat_count, lon_count,
    rhs, center_hbm, coup_hbm, land_hbm, partner_hbm, w, mix,
    center, coup, land, partner,
    dmask, coef, rowtop, rowbot, colw, cole, rrow, rcol, rfold, red, rred_lon, rred_lat,
    load_sem, row_ss, row_rs, col_ss, col_rs, fold_ss, fold_rs,
    rl_ss, rl_rs, rt_ss, rt_rs,
):
    f32 = jnp.float32
    members, rows, cols = rhs.shape
    groups = rows // 8
    halves = -(-rows // 120)
    half = rows // halves
    step_rows = 24 if half % 24 == 0 else 8
    steps = half // step_rows
    la, lo = lax.axis_index("lat"), lax.axis_index("lon")
    lat_first, lat_last = la == 0, la == lat_count - 1
    north, south = lax.rem(la + 1, lat_count), lax.rem(la + lat_count - 1, lat_count)
    east, west = lax.rem(lo + 1, lon_count), lax.rem(lo + lon_count - 1, lon_count)
    lane = lax.broadcasted_iota(jnp.int32, (members, cols), 1)
    sub = lax.broadcasted_iota(jnp.int32, (8, cols), 0)

    loads = [
        pltpu.make_async_copy(center_hbm, center, load_sem.at[0]),
        pltpu.make_async_copy(coup_hbm, coup, load_sem.at[1]),
        pltpu.make_async_copy(land_hbm, land, load_sem.at[2]),
        pltpu.make_async_copy(partner_hbm, partner, load_sem.at[3]),
    ]
    for m in range(members):
        loads.append(pltpu.make_async_copy(
            rhs.at[m], w.at[0, pl.ds(0, rows), m], load_sem.at[4 + m]))
    for c in loads:
        c.start()

    barrier = pltpu.get_barrier_semaphore()
    partners = [(la, lax.rem(lo + d, lon_count)) for d in range(1, lon_count)]
    partners += [(lax.rem(la + d, lat_count), lo) for d in range(1, lat_count)]
    partners += [(north, east), (north, west), (south, east), (south, west)]
    for p in partners:
        pl.semaphore_signal(barrier, inc=1, device_id=p, device_id_type=MESH)

    for c in loads:
        c.wait()

    def roll(x, shift, axis=1):
        return pltpu.roll(x, shift, axis)

    def packed_step(pw, pe, values):
        pw, pe = roll(pw, cols - step_rows), roll(pe, cols - step_rows)
        for r, v in enumerate(values):
            at = cols - step_rows + r
            pw = jnp.where(lane == at, roll(v, at), pw)
            pe = jnp.where(lane == at, roll(v, (at + 1) % cols), pe)
        return pw, pe

    for h in range(halves):
        def prep(gl, carry):
            pw, pe = carry
            j0 = pl.multiple_of((h * steps + gl) * step_rows, 8)
            rs = pl.ds(j0, step_rows)
            dmask[rs, :] = land[rs, :].astype(f32) / center[rs, :]
            values = []
            for r in range(step_rows):
                v = w[0, j0 + r] * dmask[pl.ds(j0 + r, 1), :]
                w[0, j0 + r] = v
                values.append(v)
            return packed_step(pw, pe, values)
        zero = jnp.zeros((members, cols), f32)
        pw, pe = lax.fori_loop(0, steps, prep, (zero, zero))
        colw[0, h] = roll(pw, half)
        cole[0, h] = roll(pe, half)
    cw = jnp.zeros((8, cols), f32)
    ce = jnp.zeros((8, cols), f32)
    for g in range(groups):
        rs = pl.ds(g * 8, 8)
        ce = jnp.where(lane == g, roll(coup[0, rs, :], g + 1), ce)
        ce = jnp.where(lane == groups + g, roll(coup[2, rs, :], groups + g + 1), ce)
        cw = jnp.where(lane == g, roll(coup[3, rs, :], g) if g else coup[3, rs, :], cw)
    colw[0, halves] = cw
    cole[0, halves] = ce
    rowtop[0, 0] = w[0, rows - 1]
    rowbot[0, 0] = w[0, 0]
    top = [coup[c, pl.ds(rows - 1, 1), :] for c in range(4)]
    packed = jnp.zeros((8, cols), f32)
    for c in (1, 2, 3):
        packed = jnp.where(sub == c, top[c], packed)
    rowtop[0, 1] = packed

    pl.semaphore_wait(barrier, len(partners))

    def exchange(k, between):
        tops = 2 if k == 0 else 1
        depth = halves + 1 if k == 0 else halves
        cps = []

        def rcopy(src, slot, n, dev):
            cps.append(pltpu.make_async_remote_copy(
                src_ref=src.at[k, pl.ds(0, n)], dst_ref=rrow.at[k, slot, pl.ds(0, n)],
                send_sem=row_ss.at[k, slot], recv_sem=row_rs.at[k, slot],
                device_id=dev, device_id_type=MESH))
        rcopy(rowtop, SW_, tops, (north, east))
        rcopy(rowtop, SE_, tops, (north, west))
        rcopy(rowbot, NW_, 1, (south, east))
        rcopy(rowbot, NE_, 1, (south, west))
        rcopy(rowtop, S_, tops, (north, lo))
        rcopy(rowbot, N_, 1, (south, lo))
        for src, side, dev in ((colw, 0, west), (cole, 1, east)):
            cps.append(pltpu.make_async_remote_copy(
                src_ref=src.at[k, pl.ds(0, depth)], dst_ref=rcol.at[k, side, pl.ds(0, depth)],
                send_sem=col_ss.at[k, side], recv_sem=col_rs.at[k, side],
                device_id=(la, dev), device_id_type=MESH))
        folds = []
        for d in range(1, lon_count):
            folds.append(pltpu.make_async_remote_copy(
                src_ref=rowtop.at[k, pl.ds(0, tops)], dst_ref=rfold.at[k, d, pl.ds(0, tops)],
                send_sem=fold_ss.at[k, d], recv_sem=fold_rs.at[k, d],
                device_id=(la, lax.rem(lo + d, lon_count)), device_id_type=MESH))

        @pl.when(lat_last)
        def _():
            for c in folds:
                c.start()
        for c in cps:
            c.start()
        between()
        for c in cps:
            c.wait_recv()

        @pl.when(lat_last)
        def _():
            for c in folds:
                c.wait_recv()
        return cps, folds

    def folded(k, slot, own):
        mine = partner[pl.ds(lo, 1), :]
        out = jnp.zeros((8, cols), f32)
        for d in range(lon_count):
            data = own if d == 0 else rfold[k, d, slot]
            first = lax.rem(lo + lon_count - d, lon_count) * cols
            at = jnp.broadcast_to(mine - first, (8, cols))
            inside = jnp.logical_and(at >= 0, at < cols)
            at = jnp.clip(at, 0, cols - 1)
            got = jnp.take_along_axis(data, at, axis=1, mode="promise_in_bounds")
            out = jnp.where(inside, got, out)
        return out

    done = []
    lane8 = lax.broadcasted_iota(jnp.int32, (8, cols), 1)

    def coefficients():
        smsg, semsg, swmsg = rrow[0, S_, 1], rrow[0, SE_, 1], rrow[0, SW_, 1]
        keep = jnp.where(lat_first, 0.0, 1.0).astype(f32)
        under_n = roll(smsg, 7, 0) * keep
        under_ne = roll(roll(jnp.where(lane8 == cols - 1, swmsg, smsg), 1), 6, 0) * keep
        under_nw = roll(roll(jnp.where(lane8 == 0, semsg, smsg), cols - 1), 5, 0) * keep
        from_east, from_west = rcol[0, 0, halves], rcol[0, 1, halves]

        @pl.when(lat_last)
        def _():
            got = folded(0, 1, rowtop[0, 1])
            last = rows - 1
            coup[1, pl.ds(last, 1), :] = 0.5 * (coup[1, pl.ds(last, 1), :] + got[1:2, :])
            coup[2, pl.ds(last, 1), :] = jnp.zeros((1, cols), f32)
            coup[3, pl.ds(last, 1), :] = jnp.zeros((1, cols), f32)

        def step(g, carry):
            pn, pne, pnw = carry
            rs = pl.ds(pl.multiple_of(g * 8, 8), 8)
            d = dmask[rs, :]
            e, n, ne, nw = (coup[c, rs, :] for c in range(4))
            gw = roll(from_west, lax.rem(2 * cols - 1 - g, cols))
            gne = roll(from_west, lax.rem(2 * cols - 1 - groups - g, cols))
            gnw = roll(from_east, lax.rem(cols - g, cols))
            coef[0, rs, :] = e * d
            coef[1, rs, :] = roll(jnp.where(lane8 == cols - 1, gw, e), 1) * d
            coef[2, rs, :] = n * d
            ns = roll(n, 1, 0)
            coef[3, rs, :] = jnp.where(sub == 0, pn, ns) * d
            coef[4, rs, :] = ne * d
            nes = roll(roll(jnp.where(lane8 == cols - 1, gne, ne), 1), 1, 0)
            coef[5, rs, :] = jnp.where(sub == 0, pne, nes) * d
            coef[6, rs, :] = nw * d
            nws = roll(roll(jnp.where(lane8 == 0, gnw, nw), cols - 1), 1, 0)
            coef[7, rs, :] = jnp.where(sub == 0, pnw, nws) * d
            return ns, nes, nws
        lax.fori_loop(0, groups, step, (under_n, under_ne, under_nw), unroll=12)

    zero = jnp.zeros((members, cols), f32)
    sums = []

    def add_sums():
        for acc in accs:
            sums.append(jnp.sum(acc, axis=1, keepdims=True))

    accs = []
    for k in range(ITERS):
        done.append(exchange(k, add_sums))
        if k == 0:
            coefficients()
        w[k, rows] = rrow[k, N_, 0]

        @pl.when(lat_last)
        def _():
            w[k, rows] = folded(k, 0, w[k, rows - 1])

        def sides(v, ge, gw):
            ve = roll(jnp.where(lane == 0, ge, v), cols - 1)
            vw = roll(jnp.where(lane == cols - 1, gw, v), 1)
            return v, ve, vw

        prev = sides(rrow[k, S_, 0], rrow[k, SE_, 0], rrow[k, SW_, 0])
        gws, ges = [], []
        for h in range(halves):
            if h + 1 < halves:
                fe = roll(rcol[k, 0, h + 1], half)
                fw = roll(rcol[k, 1, h + 1], half)
            else:
                fe = roll(rrow[k, NE_, 0], half)
                fw = roll(rrow[k, NW_, 0], half + 1)
            ges.append(jnp.where(lane == half, fe, rcol[k, 0, h]))
            gws.append(jnp.where(lane == half, fw, rcol[k, 1, h]))
        cur = sides(w[k, 0], ges[0], roll(gws[0], cols - 1))
        acc0, acc1 = zero, zero
        for h in range(halves):
            ge_h, gw_h = ges[h], gws[h]

            def step(gl, carry):
                prev, cur, acc0, acc1, pw, pe, ge, gw = carry
                j0 = pl.multiple_of((h * steps + gl) * step_rows, 8)
                values = []
                for r in range(step_rows):
                    j = j0 + r
                    nxt = sides(w[k, j + 1], roll(ge, cols - 1 - r), roll(gw, cols - 2 - r))
                    c = [coef[q, pl.ds(j, 1), :] for q in range(8)]
                    out = (c[0] * cur[1] + c[1] * cur[2]) + (c[2] * nxt[0] + c[3] * prev[0])
                    out = out + ((c[4] * nxt[1] + c[5] * prev[2]) + (c[6] * nxt[2] + c[7] * prev[1]))
                    w[k + 1, j] = out
                    t = center[pl.ds(j, 1), :] * cur[0]
                    acc0 = acc0 + t * cur[0]
                    acc1 = acc1 + t * out
                    values.append(out)
                    prev, cur = cur, nxt
                if k + 1 < ITERS:
                    pw, pe = packed_step(pw, pe, values)
                ge, gw = roll(ge, cols - step_rows), roll(gw, cols - step_rows)
                return prev, cur, acc0, acc1, pw, pe, ge, gw
            prev, cur, acc0, acc1, pw, pe, _, _ = lax.fori_loop(
                0, steps, step, (prev, cur, acc0, acc1, zero, zero, ge_h, gw_h))
            if k + 1 < ITERS:
                colw[k + 1, h] = roll(pw, half)
                cole[k + 1, h] = roll(pe, half)
        if k + 1 < ITERS:
            rowtop[k + 1, 0] = w[k + 1, rows - 1]
            rowbot[k + 1, 0] = w[k + 1, 0]
        accs[:] = [acc0, acc1]
    add_sums()
    moments = zero
    for i, total in enumerate(sums):
        moments = jnp.where(lane == i, total, moments)

    def reduce(slot, value, recv, ss, rs, count, dev):
        red[slot] = value
        cps = [
            pltpu.make_async_remote_copy(
                src_ref=red.at[slot], dst_ref=recv.at[d], send_sem=ss.at[d],
                recv_sem=rs.at[d], device_id=dev(d), device_id_type=MESH)
            for d in range(1, count)
        ]
        for c in cps:
            c.start()
        for c in cps:
            c.wait_recv()
        for d in range(1, count):
            value = value + recv[d]
        return value, cps

    moments, c1 = reduce(0, moments, rred_lon, rl_ss, rl_rs, lon_count,
                         lambda d: (la, lax.rem(lo + d, lon_count)))
    moments, c2 = reduce(1, moments, rred_lat, rt_ss, rt_rs, lat_count,
                         lambda d: (lax.rem(la + d, lat_count), lo))

    m0, m1, m2, m3, m4, m5 = (
        jnp.broadcast_to(moments[:, i:i + 1], (members, cols)) for i in range(6))
    a0 = m1 / m0
    h1 = m2 - a0 * m1
    a1 = (m3 - 2.0 * a0 * m2 + a0 * a0 * m1) / h1
    b1 = h1 / m0
    p1 = -(a0 + a1)
    p0 = a0 * a1 - b1
    h2 = m4 + p1 * m3 + p0 * m2
    a2 = (m5 + p1 * m4 + p0 * m3) / h2 + p1
    b2 = h2 / h1
    t2 = p1 - a2
    t1 = p0 - a2 * p1 - b2
    t0 = b2 * a0 - a2 * p0
    q3 = 1.0 / (1.0 + t2 + t1 + t0)
    q2, q1, q0 = t2 * q3, t1 * q3, t0 * q3
    s2, s1, s0 = q3, q2 + q3, q1 + q2 + q3

    for i, value in enumerate((s0, s1, s2, q0, q1, q2, q3)):
        mix[i] = value

    for cps, folds in done:
        for cp in cps:
            cp.wait_send()

        @pl.when(lat_last)
        def _():
            for cp in folds:
                cp.wait_send()
    for cp in c1 + c2:
        cp.wait_send()


def finish(w, mix, center, sol_out, res_out, obuf, store_sem):
    members, rows, cols = sol_out.shape
    s0, s1, s2, q0, q1, q2, q3 = (mix[i] for i in range(7))
    chunk = 4
    size = rows // 8 // chunk
    stores = []
    for c in range(chunk):

        def final(g, carry):
            for r in range(8):
                j = (c * size + g) * 8 + r
                v0, v1, v2, v3 = (w[i, j] for i in range(4))
                obuf[0, j] = s0 * v0 + s1 * v1 + s2 * v2
                obuf[1, j] = center[pl.ds(j, 1), :] * (q0 * v0 + q1 * v1 + q2 * v2 + q3 * v3)
            return carry
        lax.fori_loop(0, size, final, 0)
        rs = pl.ds(c * size * 8, size * 8)
        for o, dst in ((0, sol_out), (1, res_out)):
            for m in range(members):
                cp = pltpu.make_async_copy(
                    obuf.at[o, rs, m], dst.at[m, rs], store_sem.at[c, o, m])
                cp.start()
                stores.append(cp)
    for cp in stores:
        cp.wait()


def body(lat_count, lon_count, right_side, center, couplings, land_sea, fold_partner):
    members, rows, cols = right_side.shape
    f32 = jnp.float32
    halves = -(-rows // 120)
    hbm = pl.BlockSpec(memory_space=pl.ANY)
    dma = pltpu.SemaphoreType.DMA
    shape = jax.ShapeDtypeStruct(right_side.shape, f32)
    vmem = pl.BlockSpec(memory_space=pltpu.VMEM)
    w, mix = pl.pallas_call(
        functools.partial(kernel, lat_count, lon_count),
        out_shape=(pltpu.VMEM((ITERS + 1, rows + 1, members, cols), f32),
                   pltpu.VMEM((7, members, cols), f32)),
        in_specs=[hbm] * 5,
        out_specs=(vmem, vmem),
        scratch_shapes=[
            pltpu.VMEM((rows, cols), f32),
            pltpu.VMEM((4, rows, cols), f32),
            pltpu.VMEM((rows, cols), jnp.int32),
            pltpu.VMEM((lon_count, cols), jnp.int32),
            pltpu.VMEM((rows, cols), f32),
            pltpu.VMEM((8, rows, cols), f32),
            pltpu.VMEM((ITERS, 2, 8, cols), f32),
            pltpu.VMEM((ITERS, 1, 8, cols), f32),
            pltpu.VMEM((ITERS, halves + 1, 8, cols), f32),
            pltpu.VMEM((ITERS, halves + 1, 8, cols), f32),
            pltpu.VMEM((ITERS, 6, 2, 8, cols), f32),
            pltpu.VMEM((ITERS, 2, halves + 1, 8, cols), f32),
            pltpu.VMEM((ITERS, lon_count, 2, 8, cols), f32),
            pltpu.VMEM((2, 8, cols), f32),
            pltpu.VMEM((lon_count, 8, cols), f32),
            pltpu.VMEM((lat_count, 8, cols), f32),
            dma((4 + members,)),
            dma((ITERS, 6)), dma((ITERS, 6)),
            dma((ITERS, 2)), dma((ITERS, 2)),
            dma((ITERS, lon_count)), dma((ITERS, lon_count)),
            dma((lon_count,)), dma((lon_count,)),
            dma((lat_count,)), dma((lat_count,)),
        ],
        compiler_params=pltpu.CompilerParams(
            collective_id=0, has_side_effects=True, vmem_limit_bytes=32 * 1024 * 1024),
    )(right_side, center, couplings, land_sea, fold_partner.reshape(lon_count, cols))
    return pl.pallas_call(
        finish,
        out_shape=(shape, shape),
        in_specs=[vmem] * 3,
        out_specs=(hbm, hbm),
        scratch_shapes=[
            pltpu.VMEM((2, rows, members, cols), f32),
            dma((4, 2, members)),
        ],
        compiler_params=pltpu.CompilerParams(vmem_limit_bytes=32 * 1024 * 1024),
    )(w, mix, center)


def solution(mesh):
    return jax.shard_map(
        functools.partial(body, mesh.shape["lat"], mesh.shape["lon"]),
        mesh=mesh,
        in_specs=(
            P(None, "lat", "lon"),
            P("lat", "lon"),
            P(None, "lat", "lon"),
            P("lat", "lon"),
            P(),
        ),
        out_specs=(P(None, "lat", "lon"), P(None, "lat", "lon")),
        check_vma=False,
    )
```

```python
import functools

import jax
import jax.numpy as jnp
from jax import lax
from jax.experimental import pallas as pl
from jax.experimental.pallas import tpu as pltpu
from jax.sharding import PartitionSpec as P

ITERS = 3
MESH = pl.DeviceIdType.MESH
EDGE = 16
SLOT = 16
STRIP, KSTRIP, EAST, NORTH, NEAST, NWEST, SCALE, ARRAYS = range(8, 16)
COUPLED = (EAST, NORTH, NEAST, NWEST, SCALE)
FROM_S, FROM_N, FROM_SW, FROM_SE, FROM_NW, FROM_NE, FROM_W, FROM_E = range(8)


def roll(x, shift, axis=1):
    return pltpu.roll(x, shift, axis)


def kernel(
    lat_count, lon_count,
    rhs, center_hbm, coup_hbm, land_hbm, partner_hbm, st, vk, mix, cen,
    land, partner, strips, coefm, coefs, pack, packin, rowin, diagin, fold,
    macc, red, redlon, redlat,
    load_sem, send_sem, recv_sem, fold_ss, fold_rs, lon_ss, lon_rs, lat_ss, lat_rs,
):
    f32 = jnp.float32
    members, rows, cols = rhs.shape
    tiles = rows // 8
    first, last = 2, tiles + 1
    inner = tiles - 2
    unroll = max(u for u in range(1, 12) if inner % u == 0)
    la, lo = lax.axis_index("lat"), lax.axis_index("lon")
    lat_first, lat_last = la == 0, la == lat_count - 1
    not_first, not_last = la > 0, la < lat_count - 1
    north, south = lax.rem(la + 1, lat_count), lax.rem(la + lat_count - 1, lat_count)
    east, west = lax.rem(lo + 1, lon_count), lax.rem(lo + lon_count - 1, lon_count)
    lane = lax.broadcasted_iota(jnp.int32, (8, cols), 1)
    sub = lax.broadcasted_iota(jnp.int32, (8, cols), 0)
    place = jnp.bitwise_and(lane, SLOT - 1)
    group = lax.shift_right_logical(lane, 4)
    zero = jnp.zeros((8, cols), f32)

    def at(tile):
        start = tile * 8
        return pl.ds(start if isinstance(start, int) else pl.multiple_of(start, 8), 8)

    own = pl.ds(EDGE, rows)
    loads = [
        pltpu.make_async_copy(center_hbm, cen, load_sem.at[0]),
        pltpu.make_async_copy(land_hbm, land, load_sem.at[1]),
        pltpu.make_async_copy(partner_hbm.at[pl.ds(0, 1)], partner, load_sem.at[2]),
        pltpu.make_async_copy(coup_hbm, st.at[pl.ds(EAST, 4), own], load_sem.at[3]),
        pltpu.make_async_copy(rhs, st.at[pl.ds(0, members), own], load_sem.at[4]),
    ]
    for c in loads:
        c.start()

    barrier = pltpu.get_barrier_semaphore()
    partners = [(la, lax.rem(lo + d, lon_count)) for d in range(1, lon_count)]
    partners += [(lax.rem(la + d, lat_count), lo) for d in range(1, lat_count)]
    partners += [(north, east), (north, west), (south, east), (south, west)]
    for p in partners:
        pl.semaphore_signal(barrier, inc=1, device_id=p, device_id_type=MESH)

    for c in loads:
        c.wait()

    inside_w = jnp.logical_and(place >= 3, place < 8)
    inside_e = jnp.logical_and(place >= 8, place < 13)

    def own_strip(arrays):
        out = zero
        for g, x in enumerate(arrays):
            mine = group == g
            out = jnp.where(jnp.logical_and(mine, inside_w), roll(x, g * SLOT + 3), out)
            out = jnp.where(jnp.logical_and(mine, inside_e),
                            roll(x, (g * SLOT + 13) % cols), out)
        return out

    def prep(t, carry):
        pe, pw, ke, kw = zero, zero, zero, zero
        for q in range(4):
            tile = first + t * 4 + q
            rs = at(tile)
            near = at(tile - first)
            d = land[near, :].astype(f32) / cen[near, :]
            st[SCALE, rs, :] = d
            vals = []
            for m in range(members):
                v = st[m, rs, :] * d
                st[m, rs, :] = v
                vals.append(v)
            s = own_strip(vals)
            st[STRIP, rs, :] = s
            k = own_strip([st[c, rs, :] for c in COUPLED[:4]] + [d])
            st[KSTRIP, rs, :] = k
            mine = lax.shift_right_logical(place, 2) == q
            pe = jnp.where(mine, roll(s, (4 * q - 10) % cols), pe)
            pw = jnp.where(mine, roll(s, (4 * q - 3) % cols), pw)
            ke = jnp.where(mine, roll(k, (4 * q - 10) % cols), ke)
            kw = jnp.where(mine, roll(k, (4 * q - 3) % cols), kw)
        pack[0, 0, t] = pe
        pack[0, 1, t] = ke
        pack[1, 0, t] = pw
        pack[1, 1, t] = kw
        return carry
    lax.fori_loop(0, tiles // 4, prep, 0)

    top, bottom = pl.ds(EDGE + rows - 3, 3), pl.ds(EDGE, 3)

    def remote(src, dst, slot, dev):
        return pltpu.make_async_remote_copy(
            src_ref=src, dst_ref=dst, send_sem=send_sem.at[slot], recv_sem=recv_sem.at[slot],
            device_id=dev, device_id_type=MESH)

    sides = [remote(pack.at[0], packin.at[0], FROM_W, (la, east)),
             remote(pack.at[1], packin.at[1], FROM_E, (la, west))]
    pair = pl.ds(STRIP, 2)
    low, high = pl.ds(5, 3), pl.ds(0, 3)
    up = [remote(st.at[:, top], rowin.at[0, :, low], FROM_S, (north, lo)),
          remote(st.at[pair, top], diagin.at[0, :, low], FROM_SW, (north, east)),
          remote(st.at[pair, top], diagin.at[1, :, low], FROM_SE, (north, west))]
    down = [remote(st.at[:, bottom], rowin.at[1, :, high], FROM_N, (south, lo)),
            remote(st.at[pair, bottom], diagin.at[2, :, high], FROM_NW, (south, east)),
            remote(st.at[pair, bottom], diagin.at[3, :, high], FROM_NE, (south, west))]
    folds = [
        pltpu.make_async_remote_copy(
            src_ref=fold.at[0, :, high], dst_ref=fold.at[d, :, high],
            send_sem=fold_ss.at[d], recv_sem=fold_rs.at[d],
            device_id=(la, lax.rem(lo + d, lon_count)), device_id_type=MESH)
        for d in range(1, lon_count)
    ]
    fold_arrays = list(range(members)) + list(COUPLED)

    pl.semaphore_wait(barrier, len(partners))
    for c in sides:
        c.start()

    @pl.when(lat_last)
    def _():
        end = EDGE + rows - 1
        for i, a in enumerate(fold_arrays):
            if a == NORTH:
                picks = (end - 1, end - 2, end)
            elif a in (NEAST, NWEST):
                picks = (end - 1, end - 2, end - 2)
            else:
                picks = (end, end - 1, end - 2)
            for g, r in enumerate(picks):
                fold[0, i, pl.ds(g, 1), :] = st[a, pl.ds(r, 1), :]
        for c in folds:
            c.start()

    @pl.when(not_last)
    def _():
        for c in up:
            c.start()

    @pl.when(not_first)
    def _():
        for c in down:
            c.start()

    for c in sides:
        c.wait_recv()

    def merge(t, carry):
        for g in range(2):
            fw, fe = packin[0, g, t], packin[1, g, t]
            for q in range(4):
                rs = at(first + t * 4 + q)
                x = st[STRIP + g, rs, :]
                x = jnp.where(place < 3, roll(fw, (-4 * q) % cols) if q else fw, x)
                x = jnp.where(place > 12, roll(fe, 13 - 4 * q), x)
                strips[0, g, rs, :] = x
        return carry
    lax.fori_loop(0, tiles // 4, merge, 0)

    def lateral(x, s, g):
        xe = jnp.where(lane == cols - 1, roll(s, lax.rem(2 * cols - 14 - SLOT * g, cols)),
                       roll(x, cols - 1))
        xw = jnp.where(lane == 0, roll(s, lax.rem(2 * cols - 2 - SLOT * g, cols)), roll(x, 1))
        return xe, xw

    def main_coefs(tile):
        rs = at(tile)
        start = tile * 8
        below = pl.ds(start - 1, 8)
        above = pl.ds(start + 1, 8)
        k = strips[0, 1, rs, :]

        def from_west(a, g):
            return jnp.where(lane == 0, roll(k, cols - 2 - SLOT * g), roll(st[a, rs, :], 1))
        d, dn = st[SCALE, rs, :], st[SCALE, above, :]
        ds_ = st[SCALE, below, :]
        coefm[0, rs, :] = d * st[EAST, rs, :]
        coefm[1, rs, :] = d * from_west(EAST, 0)
        coefm[2, rs, :] = ds_ * st[NORTH, below, :]
        coefm[3, rs, :] = ds_ * st[NEAST, below, :]
        coefm[4, rs, :] = ds_ * st[NWEST, below, :]
        coefm[5, rs, :] = dn * st[NORTH, rs, :]
        coefm[6, rs, :] = dn * jnp.where(lane == cols - 1, roll(k, cols - 14 - SLOT * 3),
                                         roll(st[NWEST, rs, :], cols - 1))
        coefm[7, rs, :] = dn * from_west(NEAST, 2)

    def strip_coefs(tile):
        rs = at(tile)
        start = tile * 8
        here = strips[0, 1, rs, :]
        below = strips[0, 1, pl.ds(start - 1, 8), :]
        above = strips[0, 1, pl.ds(start + 1, 8), :]

        def spread(x, g, shift=0):
            where = jnp.bitwise_and(place + (g * SLOT + shift), cols - 1)
            return jnp.take_along_axis(x, where, axis=1, mode="promise_in_bounds")
        d, ds_, dn = spread(here, 4), spread(below, 4), spread(above, 4)
        coefs[0, rs, :] = d * spread(here, 0)
        coefs[1, rs, :] = d * spread(here, 0, -1)
        coefs[2, rs, :] = ds_ * spread(below, 1)
        coefs[3, rs, :] = ds_ * spread(below, 2)
        coefs[4, rs, :] = ds_ * spread(below, 3)
        coefs[5, rs, :] = dn * spread(here, 1)
        coefs[6, rs, :] = dn * spread(here, 3, 1)
        coefs[7, rs, :] = dn * spread(here, 2, -1)

    def all_coefs(t, carry):
        main_coefs(first + t)
        strip_coefs(first + t)
        return carry
    lax.fori_loop(0, tiles, all_coefs, 0, unroll=4)

    def parts(x, xe, xw, c):
        cross = c[0] * xe + c[1] * xw
        upper = c[2] * x + (c[3] * xe + c[4] * xw)
        lower = c[5] * x + (c[6] * xe + c[7] * xw)
        return cross, upper, lower

    def shift_up(u, u_next):
        return roll(jnp.where(sub == 0, u_next, u), 7, 0)

    def shift_down(d_prev, d):
        return roll(jnp.where(sub == 7, d_prev, d), 1, 0)

    def source(k, g, rs):
        return st[g, rs, :] if k == 0 else vk[k - 1, g, rs, :]

    def strip_parts(k, tile):
        rs = at(tile)
        x = strips[k, 0, rs, :]
        return parts(x, roll(x, cols - 1), roll(x, 1), [coefs[q, rs, :] for q in range(8)])

    def member_parts(k, g, tile, c=None):
        rs = at(tile)
        x = source(k, g, rs)
        xe, xw = lateral(x, strips[k, 0, rs, :], g)
        if c is None:
            c = [coefm[q, rs, :] for q in range(8)]
        return x, parts(x, xe, xw, c)

    for k in range(ITERS - 1):
        cross, upper, lower = strip_parts(k, first)

        def strip_step(b, carry):
            sofar, u_old, d_old = carry
            for u in range(unroll):
                tile = first + 1 + b * unroll + u
                cross, upper, lower = strip_parts(k, tile)
                strips[k + 1, 0, at(tile - 1), :] = sofar + shift_up(u_old, upper)
                sofar, u_old, d_old = cross + shift_down(d_old, lower), upper, lower
            return sofar, u_old, d_old
        sofar, u_old, d_old = lax.fori_loop(
            0, inner // unroll, strip_step, (cross + shift_down(zero, lower), upper, lower))
        cross, upper, lower = strip_parts(k, last)
        strips[k + 1, 0, at(last - 1), :] = sofar + shift_up(u_old, upper)
        strips[k + 1, 0, at(last), :] = cross + shift_down(d_old, lower) + shift_up(upper, zero)

    batch = 2
    for k in range(ITERS):
        def sweep(p, carry):
            gs = [p * batch + i for i in range(batch)]
            state = []
            for g in gs:
                _, (cross, upper, lower) = member_parts(k, g, first)
                state.append((cross + shift_down(zero, lower), upper, lower, zero, zero, zero))

            def step(b, state):
                state = list(state)
                for u in range(unroll):
                    tile = first + 1 + b * unroll + u
                    rs = at(tile)
                    c = [coefm[q, rs, :] for q in range(8)]
                    weight = cen[at(tile - first), :]
                    for i, g in enumerate(gs):
                        sofar, u_old, d_old, w_old, acc0, acc1 = state[i]
                        x, (cross, upper, lower) = member_parts(k, g, tile, c)
                        out = sofar + shift_up(u_old, upper)
                        vk[k, g, at(tile - 1), :] = out
                        acc1 = acc1 + w_old * out
                        w = weight * x
                        acc0 = acc0 + w * x
                        state[i] = (cross + shift_down(d_old, lower), upper, lower, w, acc0, acc1)
                return tuple(state)
            state = lax.fori_loop(0, inner // unroll, step, tuple(state))
            for i, g in enumerate(gs):
                sofar, u_old, d_old, w_old, acc0, acc1 = state[i]
                _, (cross, upper, lower) = member_parts(k, g, last)
                out = sofar + shift_up(u_old, upper)
                vk[k, g, at(last - 1), :] = out
                vk[k, g, at(last), :] = cross + shift_down(d_old, lower) + shift_up(upper, zero)
                macc[2 * k, g] = acc0
                macc[2 * k + 1, g] = acc1 + w_old * out
            return carry
        lax.fori_loop(0, members // batch, sweep, 0)

    @pl.when(not_first)
    def _():
        for s in (FROM_S, FROM_SW, FROM_SE):
            up[s if s == FROM_S else s - FROM_SW + 1].wait_recv()
        rs = at(first - 1)
        for a in range(ARRAYS):
            if a not in (STRIP, KSTRIP):
                st[a, rs, :] = rowin[0, a]
        for g in range(2):
            x = rowin[0, STRIP + g]
            x = jnp.where(place < 3, roll(diagin[0, g], cols - 10), x)
            strips[0, g, rs, :] = jnp.where(place > 12, roll(diagin[1, g], 10), x)

    @pl.when(lat_first)
    def _():
        rs = at(first - 1)
        for a in range(ARRAYS):
            st[a, rs, :] = zero
        for g in range(2):
            strips[0, g, rs, :] = zero

    @pl.when(not_last)
    def _():
        for c in down:
            c.wait_recv()
        rs = at(last + 1)
        for a in range(ARRAYS):
            if a not in (STRIP, KSTRIP):
                st[a, rs, :] = rowin[1, a]
        for g in range(2):
            x = rowin[1, STRIP + g]
            x = jnp.where(place < 3, roll(diagin[2, g], cols - 10), x)
            strips[0, g, rs, :] = jnp.where(place > 12, roll(diagin[3, g], 10), x)

    @pl.when(lat_last)
    def _():
        for c in folds:
            c.wait_recv()
        total = lon_count * cols
        rs = at(last + 1)
        shown = jnp.where(place < 8, place - 3, place + (cols - 13))
        origin = lax.rem(partner[0, 0] - lo * cols + total, total)

        def view(shift):
            start = lax.rem(origin + shift + total, total)
            chunk = lax.div(start, cols)
            head = start - chunk * cols
            slots = [lax.rem(lo - chunk - o + 3 * lon_count, lon_count) for o in (1, 0, -1, -2)]
            z = head - shown
            return (slots, jnp.bitwise_and(head - lane, cols - 1), lane <= head,
                    jnp.bitwise_and(z, cols - 1), (z >= cols, z >= 0, z >= -cols))

        def take(x, where):
            return jnp.take_along_axis(x, where, axis=1, mode="promise_in_bounds")
        views = {s: view(s) for s in (-1, 0, 1)}
        shifts = {EAST: -1, NEAST: -1, NWEST: 1}
        ghost = [zero, zero]
        for i, a in enumerate(fold_arrays):
            slots, where, within, where_s, (far, near, back) = views[shifts.get(a, 0)]
            chunks = [fold[s, i] for s in slots]
            block = jnp.where(within, take(chunks[1], where), take(chunks[2], where))
            st[a, rs, :] = block
            x = jnp.where(back, take(chunks[2], where_s), take(chunks[3], where_s))
            x = jnp.where(near, take(chunks[1], where_s), x)
            x = jnp.where(far, take(chunks[0], where_s), x)
            s, g = (0, a) if a < members else (1, COUPLED.index(a))
            ghost[s] = jnp.where(group == g, x, ghost[s])
            if a == NORTH:
                end = pl.ds(EDGE + rows - 1, 1)
                st[NORTH, end, :] = 0.5 * (st[NORTH, end, :] + block[2:3, :])
                mixed = 0.5 * (strips[0, 1, end, :] + x[2:3, :])
                g1 = group[0:1, :]
                dropped = jnp.logical_or(g1 == 2, g1 == 3)
                strips[0, 1, end, :] = jnp.where(
                    dropped, 0.0, jnp.where(g1 == 1, mixed, strips[0, 1, end, :]))
                st[NEAST, end, :] = jnp.zeros((1, cols), f32)
                st[NWEST, end, :] = jnp.zeros((1, cols), f32)
        for s in range(2):
            strips[0, s, rs, :] = ghost[s]

    for tile in (first - 1, first, last, last + 1):
        main_coefs(tile)
        strip_coefs(tile)

    def join(lo_parts, mid, hi_parts):
        out = mid[0]
        out = out + shift_down(zero if lo_parts is None else lo_parts[2], mid[2])
        return out + shift_up(mid[1], zero if hi_parts is None else hi_parts[1])

    for k in range(ITERS - 1):
        b = [strip_parts(k, t) for t in (first - 1, first, first + 1)]
        t = [strip_parts(k, t) for t in (last - 1, last, last + 1)]
        strips[k + 1, 0, at(first - 1), :] = join(None, b[0], b[1])
        strips[k + 1, 0, at(first), :] = join(b[0], b[1], b[2])
        strips[k + 1, 0, at(last), :] = join(t[0], t[1], t[2])
        strips[k + 1, 0, at(last + 1), :] = join(t[1], t[2], None)
    for k in range(ITERS):
        def band(p, carry):
            for i in range(batch):
                g = p * batch + i
                b = [member_parts(k, g, t) for t in (first - 1, first, first + 1)]
                t = [member_parts(k, g, t) for t in (last - 1, last, last + 1)]
                if k + 1 < ITERS:
                    vk[k, g, at(first - 1), :] = join(None, b[0][1], b[1][1])
                    vk[k, g, at(last + 1), :] = join(t[1][1], t[2][1], None)
                acc0, acc1 = macc[2 * k, g], macc[2 * k + 1, g]
                for tile, three in ((first, b), (last, t)):
                    out = join(three[0][1], three[1][1], three[2][1])
                    vk[k, g, at(tile), :] = out
                    x = three[1][0]
                    w = cen[at(tile - first), :] * x
                    acc0 = acc0 + w * x
                    acc1 = acc1 + w * out
                macc[2 * k, g] = acc0
                macc[2 * k + 1, g] = acc1
            return carry
        lax.fori_loop(0, members // batch, band, 0)

    row = zero
    for i in range(2 * ITERS):
        total = macc[i, :, 0, :]
        for s in range(1, 8):
            total = total + macc[i, :, s, :]
        total = jnp.sum(total, axis=1, keepdims=True)
        row = jnp.where(lane == 8 * i + sub, total, row)

    def column_sum(x):
        for s in (4, 2, 1):
            x = x + roll(x, s, 0)
        return x
    row = column_sum(row)

    def reduce(value, slot, recv, me, ss, rs, count, dev):
        red[slot] = value
        cps = [
            pltpu.make_async_remote_copy(
                src_ref=red.at[slot, pl.ds(0, 1)], dst_ref=recv.at[me, pl.ds(0, 1)],
                send_sem=ss.at[d], recv_sem=rs.at[d], device_id=dev(d), device_id_type=MESH)
            for d in range(1, count)
        ]
        for c in cps:
            c.start()
        recv[me] = value
        for c in cps:
            c.wait_recv()
        out = recv[0, pl.ds(0, 1), :]
        for d in range(1, count):
            out = out + recv[d, pl.ds(0, 1), :]
        return jnp.broadcast_to(out, (8, cols)), cps

    row, c1 = reduce(row, 0, redlon, lo, lon_ss, lon_rs, lon_count,
                     lambda d: (la, lax.rem(lo + d, lon_count)))
    row, c2 = reduce(row, 1, redlat, la, lat_ss, lat_rs, lat_count,
                     lambda d: (lax.rem(la + d, lat_count), lo))

    m0, m1, m2, m3, m4, m5 = (
        jnp.broadcast_to(
            jnp.sum(jnp.where(lane == 8 * i + sub, row, 0.0), axis=1, keepdims=True), (8, cols))
        for i in range(2 * ITERS))
    a0 = m1 / m0
    h1 = m2 - a0 * m1
    a1 = (m3 - 2.0 * a0 * m2 + a0 * a0 * m1) / h1
    b1 = h1 / m0
    p1 = -(a0 + a1)
    p0 = a0 * a1 - b1
    h2 = m4 + p1 * m3 + p0 * m2
    a2 = (m5 + p1 * m4 + p0 * m3) / h2 + p1
    b2 = h2 / h1
    t2 = p1 - a2
    t1 = p0 - a2 * p1 - b2
    t0 = b2 * a0 - a2 * p0
    q3 = 1.0 / (1.0 + t2 + t1 + t0)
    q2, q1, q0 = t2 * q3, t1 * q3, t0 * q3
    for i, value in enumerate((q3 + q2 + q1, q2 + q3, q3, q0, q1, q2, q3)):
        mix[i] = value

    for c in sides + c1 + c2:
        c.wait_send()

    @pl.when(not_last)
    def _():
        for c in up:
            c.wait_send()

    @pl.when(not_first)
    def _():
        for c in down:
            c.wait_send()

    @pl.when(lat_last)
    def _():
        for c in folds:
            c.wait_send()


def finish(st, vk, mix, center, sol_out, res_out, obuf, store_sem):
    members, rows, cols = sol_out.shape

    def one(m, carry):
        s0, s1, s2, q0, q1, q2, q3 = (
            jnp.broadcast_to(mix[i, pl.ds(m, 1), :], (8, cols)) for i in range(7))
        for t in range(rows // 8):
            here, rs = pl.ds(8 * t, 8), pl.ds(EDGE + 8 * t, 8)
            v0, v1, v2, v3 = st[m, rs, :], vk[0, m, rs, :], vk[1, m, rs, :], vk[2, m, rs, :]
            obuf[0, m, here, :] = s0 * v0 + s1 * v1 + s2 * v2
            obuf[1, m, here, :] = center[here, :] * (q0 * v0 + q1 * v1 + q2 * v2 + q3 * v3)
        for o, dst in ((0, sol_out), (1, res_out)):
            pltpu.make_async_copy(obuf.at[o, m], dst.at[m], store_sem.at[o, m]).start()
        return carry
    lax.fori_loop(0, members, one, 0)
    for m in range(members):
        for o, dst in ((0, sol_out), (1, res_out)):
            pltpu.make_async_copy(obuf.at[o, m], dst.at[m], store_sem.at[o, m]).wait()


def body(lat_count, lon_count, right_side, center, couplings, land_sea, fold_partner):
    members, rows, cols = right_side.shape
    f32 = jnp.float32
    hbm = pl.BlockSpec(memory_space=pltpu.HBM)
    vmem = pl.BlockSpec(memory_space=pltpu.VMEM)
    dma = pltpu.SemaphoreType.DMA
    shape = jax.ShapeDtypeStruct(right_side.shape, f32)
    high = rows + 2 * EDGE
    tiles = rows // 8
    folded = members + len(COUPLED)
    st, vk, mix, cen = pl.pallas_call(
        functools.partial(kernel, lat_count, lon_count),
        out_shape=(pltpu.VMEM((ARRAYS, high, cols), f32),
                   pltpu.VMEM((ITERS, members, high, cols), f32),
                   pltpu.VMEM((7, 8, cols), f32),
                   pltpu.VMEM((rows, cols), f32)),
        in_specs=[hbm] * 5,
        out_specs=(vmem, vmem, vmem, vmem),
        scratch_shapes=[
            pltpu.VMEM((rows, cols), jnp.int32),
            pltpu.SMEM((1, cols), jnp.int32),
            pltpu.VMEM((ITERS, 2, high, cols), f32),
            pltpu.VMEM((8, high, cols), f32),
            pltpu.VMEM((8, high, cols), f32),
            pltpu.VMEM((2, 2, tiles // 4, 8, cols), f32),
            pltpu.VMEM((2, 2, tiles // 4, 8, cols), f32),
            pltpu.VMEM((2, ARRAYS, 8, cols), f32),
            pltpu.VMEM((4, 2, 8, cols), f32),
            pltpu.VMEM((lon_count, folded, 8, cols), f32),
            pltpu.VMEM((2 * ITERS, members, 8, cols), f32),
            pltpu.VMEM((2, 8, cols), f32),
            pltpu.VMEM((lon_count, 8, cols), f32),
            pltpu.VMEM((lat_count, 8, cols), f32),
            dma((5,)), dma((8,)), dma((8,)),
            dma((lon_count,)), dma((lon_count,)),
            dma((lon_count,)), dma((lon_count,)),
            dma((lat_count,)), dma((lat_count,)),
        ],
        compiler_params=pltpu.CompilerParams(
            collective_id=0, has_side_effects=True, vmem_limit_bytes=32 * 1024 * 1024),
    )(*(pltpu.with_memory_space_constraint(x, pltpu.HBM) for x in (
        right_side, center, couplings, land_sea, fold_partner.reshape(lon_count, cols))))
    return pl.pallas_call(
        finish,
        out_shape=(shape, shape),
        in_specs=[vmem] * 4,
        out_specs=(hbm, hbm),
        scratch_shapes=[
            pltpu.VMEM((2, members, rows, cols), f32),
            dma((2, members)),
        ],
        compiler_params=pltpu.CompilerParams(vmem_limit_bytes=16 * 1024 * 1024),
    )(st, vk, mix, cen)


def solution(mesh):
    return jax.shard_map(
        functools.partial(body, mesh.shape["lat"], mesh.shape["lon"]),
        mesh=mesh,
        in_specs=(
            P(None, "lat", "lon"),
            P("lat", "lon"),
            P(None, "lat", "lon"),
            P("lat", "lon"),
            P(),
        ),
        out_specs=(P(None, "lat", "lon"), P(None, "lat", "lon")),
        check_vma=False,
    )
```

```python
import functools

import jax
import jax.numpy as jnp
from jax import lax
from jax.experimental import pallas as pl
from jax.experimental.pallas import tpu as pltpu
from jax.sharding import PartitionSpec as P

ITERS = 3
BATCH = 2
MESH = pl.DeviceIdType.MESH
EDGE = 16
SLOT = 16
RIM, KRIM, EAST, NORTH, NEAST, NWEST, SCALE, ARRAYS = range(8, 16)
EXTRA = 5 * SLOT
COUPLED = (EAST, NORTH, NEAST, NWEST, SCALE)
FROM_S, FROM_N, FROM_SW, FROM_SE, FROM_NW, FROM_NE, FROM_W, FROM_E = range(8)


def roll(x, shift, axis=1):
    return pltpu.roll(x, shift, axis)


def kernel(
    lat_count, lon_count,
    rhs, center_hbm, coup_hbm, land_hbm, partner_hbm, st, vk, mix, cen,
    land, partner, strips, kstrip, beyond, coefm, coefs, pack, packin, rowin, diagin, fold,
    macc, sacc, red, redlon, redlat,
    load_sem, send_sem, recv_sem, fold_ss, fold_rs, lon_ss, lon_rs, lat_ss, lat_rs,
):
    f32 = jnp.float32
    members, rows, cols = rhs.shape
    tiles = rows // 8
    first, last = 2, tiles + 1
    inner = tiles - 2

    def split(count, most):
        return max(u for u in range(1, most + 1) if count % u == 0)

    la, lo = lax.axis_index("lat"), lax.axis_index("lon")
    lat_first, lat_last = la == 0, la == lat_count - 1
    not_first, not_last = la > 0, la < lat_count - 1
    north, south = lax.rem(la + 1, lat_count), lax.rem(la + lat_count - 1, lat_count)
    east, west = lax.rem(lo + 1, lon_count), lax.rem(lo + lon_count - 1, lon_count)
    lane = lax.broadcasted_iota(jnp.int32, (8, cols), 1)
    sub = lax.broadcasted_iota(jnp.int32, (8, cols), 0)
    place = jnp.bitwise_and(lane, SLOT - 1)
    group = lax.shift_right_logical(lane, 4)
    zero = jnp.zeros((8, cols), f32)

    def at(tile):
        start = tile * 8
        return pl.ds(start if isinstance(start, int) else pl.multiple_of(start, 8), 8)

    own = pl.ds(EDGE, rows)
    loads = [
        pltpu.make_async_copy(center_hbm, cen, load_sem.at[0]),
        pltpu.make_async_copy(land_hbm, land, load_sem.at[1]),
        pltpu.make_async_copy(partner_hbm.at[pl.ds(0, 1)], partner, load_sem.at[2]),
        pltpu.make_async_copy(coup_hbm, st.at[pl.ds(EAST, 4), own], load_sem.at[3]),
        pltpu.make_async_copy(rhs, st.at[pl.ds(0, members), own], load_sem.at[4]),
    ]
    for c in loads:
        c.start()

    barrier = pltpu.get_barrier_semaphore()
    partners = [(la, lax.rem(lo + d, lon_count)) for d in range(1, lon_count)]
    partners += [(lax.rem(la + d, lat_count), lo) for d in range(1, lat_count)]
    partners += [(north, east), (north, west), (south, east), (south, west)]
    for p in partners:
        pl.semaphore_signal(barrier, inc=1, device_id=p, device_id_type=MESH)

    for c in loads:
        c.wait()

    rim_lanes = [jnp.bitwise_and(lane - (SLOT * g - 3), cols - 1) < 12 for g in range(8)]

    def rim(arrays):
        out = zero
        for g, x in enumerate(arrays):
            out = jnp.where(rim_lanes[g], roll(x, g * SLOT + 3), out)
        return out

    def prep(t, carry):
        pe, pw, ke, kw = zero, zero, zero, zero
        for q in range(4):
            tile = first + t * 4 + q
            rs = at(tile)
            near = at(tile - first)
            d = land[near, :].astype(f32) / cen[near, :]
            st[SCALE, rs, :] = d
            vals = []
            for m in range(members):
                v = st[m, rs, :] * d
                st[m, rs, :] = v
                vals.append(v)
            o = rim(vals)
            st[RIM, rs, :] = o
            k = rim([st[c, rs, :] for c in COUPLED[:4]] + [d])
            st[KRIM, rs, :] = k
            if q:
                o, k = roll(o, 3 * q), roll(k, 3 * q)
            here = jnp.logical_and(place >= 3 * q, place < 3 * q + 3)
            after = jnp.logical_and(place >= 3 * q + 3, place < 3 * q + 6)
            pe = jnp.where(here, o, pe)
            pw = jnp.where(after, o, pw)
            ke = jnp.where(here, k, ke)
            kw = jnp.where(after, k, kw)
        pack[0, 0, t] = pe
        pack[0, 1, t] = ke
        pack[1, 0, t] = pw
        pack[1, 1, t] = kw
        return carry
    lax.fori_loop(0, tiles // 4, prep, 0, unroll=split(tiles // 4, 3))

    top, bottom = pl.ds(EDGE + rows - 3, 3), pl.ds(EDGE, 3)

    def remote(src, dst, slot, dev):
        return pltpu.make_async_remote_copy(
            src_ref=src, dst_ref=dst, send_sem=send_sem.at[slot], recv_sem=recv_sem.at[slot],
            device_id=dev, device_id_type=MESH)

    sides = [remote(pack.at[0], packin.at[0], FROM_W, (la, east)),
             remote(pack.at[1], packin.at[1], FROM_E, (la, west))]
    pair = pl.ds(RIM, 2)
    low, high = pl.ds(5, 3), pl.ds(0, 3)
    up = [remote(st.at[:, top], rowin.at[0, :, low], FROM_S, (north, lo)),
          remote(st.at[pair, top], diagin.at[0, :, low], FROM_SW, (north, east)),
          remote(st.at[pair, top], diagin.at[1, :, low], FROM_SE, (north, west))]
    down = [remote(st.at[:, bottom], rowin.at[1, :, high], FROM_N, (south, lo)),
            remote(st.at[pair, bottom], diagin.at[2, :, high], FROM_NW, (south, east)),
            remote(st.at[pair, bottom], diagin.at[3, :, high], FROM_NE, (south, west))]
    folds = [
        pltpu.make_async_remote_copy(
            src_ref=fold.at[0, :, high], dst_ref=fold.at[d, :, high],
            send_sem=fold_ss.at[d], recv_sem=fold_rs.at[d],
            device_id=(la, lax.rem(lo + d, lon_count)), device_id_type=MESH)
        for d in range(1, lon_count)
    ]
    fold_arrays = list(range(members)) + list(COUPLED)

    pl.semaphore_wait(barrier, len(partners))
    for c in sides:
        c.start()

    @pl.when(lat_last)
    def _():
        end = EDGE + rows - 1
        for i, a in enumerate(fold_arrays):
            if a == NORTH:
                picks = (end - 1, end - 2, end)
            elif a in (NEAST, NWEST):
                picks = (end - 1, end - 2, end - 2)
            else:
                picks = (end, end - 1, end - 2)
            for g, r in enumerate(picks):
                fold[0, i, pl.ds(g, 1), :] = st[a, pl.ds(r, 1), :]
        for c in folds:
            c.start()

    @pl.when(not_last)
    def _():
        for c in up:
            c.start()

    @pl.when(not_first)
    def _():
        for c in down:
            c.start()

    def unfold(o, k, ow, kw, oe, ke):
        def windows(x, w, e):
            x = jnp.where(place < 8, x, roll(x, 10))
            x = jnp.where(place < 3, w, x)
            return jnp.where(place < 13, x, e)
        ring = jnp.where(place == 7, roll(o, cols - 1), jnp.where(place == 8, roll(o, 11), 0.0))
        return windows(o, ow, oe), ring, extras(windows(k, kw, ke), k)

    def extras(x, k):
        x = jnp.where(lane == EXTRA, roll(k, EXTRA + 3), x)
        x = jnp.where(lane == EXTRA + 1, roll(k, EXTRA + 1 - 2 * SLOT + 3), x)
        return jnp.where(lane == EXTRA + 2, roll(k, EXTRA + 2 - 3 * SLOT - 8), x)

    def put_strip(rs, parts_):
        strips[0, rs, :], beyond[rs, :], kstrip[rs, :] = parts_

    def open_rims(t, carry):
        rs = at(first + t)
        put_strip(rs, unfold(st[RIM, rs, :], st[KRIM, rs, :], zero, zero, zero, zero))
        return carry

    def main_coefs(tile):
        rs = at(tile)
        start = tile * 8
        below = pl.ds(start - 1, 8)
        above = pl.ds(start + 1, 8)
        d, dn = st[SCALE, rs, :], st[SCALE, above, :]
        ds_ = st[SCALE, below, :]
        coefm[0, rs, :] = d * st[EAST, rs, :]
        coefm[1, rs, :] = d * roll(st[EAST, rs, :], 1)
        coefm[2, rs, :] = ds_ * st[NORTH, below, :]
        coefm[3, rs, :] = ds_ * st[NEAST, below, :]
        coefm[4, rs, :] = ds_ * st[NWEST, below, :]
        coefm[5, rs, :] = dn * st[NORTH, rs, :]
        coefm[6, rs, :] = dn * roll(st[NWEST, rs, :], cols - 1)
        coefm[7, rs, :] = dn * roll(st[NEAST, rs, :], 1)

    def strip_coefs(tile):
        rs = at(tile)
        start = tile * 8
        here = kstrip[rs, :]
        below = kstrip[pl.ds(start - 1, 8), :]
        above = kstrip[pl.ds(start + 1, 8), :]

        def spread(x, g, shift=0):
            where = jnp.bitwise_and(place + (g * SLOT + shift), cols - 1)
            if shift < 0:
                where = jnp.where(place == 8, EXTRA + g // 2, where)
            if shift > 0:
                where = jnp.where(place == 7, EXTRA + 2, where)
            return jnp.take_along_axis(x, where, axis=1, mode="promise_in_bounds")
        d, ds_, dn = spread(here, 4), spread(below, 4), spread(above, 4)
        coefs[0, rs, :] = d * spread(here, 0)
        coefs[1, rs, :] = d * spread(here, 0, -1)
        coefs[2, rs, :] = ds_ * spread(below, 1)
        coefs[3, rs, :] = ds_ * spread(below, 2)
        coefs[4, rs, :] = ds_ * spread(below, 3)
        coefs[5, rs, :] = dn * spread(here, 1)
        coefs[6, rs, :] = dn * spread(here, 3, 1)
        coefs[7, rs, :] = dn * spread(here, 2, -1)
        edge = jnp.logical_or(jnp.logical_and(place >= 3, place < 6),
                              jnp.logical_and(place >= 10, place < 13))
        used = jnp.logical_and(edge, d > 0.0)
        coefs[8, rs, :] = jnp.where(used, 1.0 / jnp.where(used, d, 1.0), 0.0)

    def all_coefs(t, carry):
        main_coefs(first + t)
        return carry
    lax.fori_loop(0, tiles, all_coefs, 0, unroll=split(tiles, 24))
    lax.fori_loop(0, tiles, open_rims, 0, unroll=split(tiles, 24))

    def parts(x, xe, xw, c):
        cross = c[0] * xe + c[1] * xw
        upper = c[2] * x + (c[3] * xe + c[4] * xw)
        lower = c[5] * x + (c[6] * xe + c[7] * xw)
        return cross, upper, lower

    def shift_up(u, u_next):
        return roll(jnp.where(sub == 0, u_next, u), 7, 0)

    def shift_down(d_prev, d):
        return roll(jnp.where(sub == 7, d_prev, d), 1, 0)

    def source(k, g, rs):
        return st[g, rs, :] if k == 0 else vk[k - 1, g, rs, :]

    def strip_parts(k, tile):
        rs = at(tile)
        x = strips[k, rs, :]
        xe, xw = roll(x, cols - 1), roll(x, 1)
        if k == 0:
            near = beyond[rs, :]
            xe, xw = jnp.where(place == 7, near, xe), jnp.where(place == 8, near, xw)
        return x, parts(x, xe, xw, [coefs[q, rs, :] for q in range(8)])

    def member_parts(k, g, tile, c=None):
        rs = at(tile)
        x = source(k, g, rs)
        if c is None:
            c = [coefm[q, rs, :] for q in range(8)]
        return x, parts(x, roll(x, cols - 1), roll(x, 1), c)

    batch = BATCH
    for k in range(ITERS):
        def sweep(p, carry):
            gs = [p * batch + i for i in range(batch)]
            state = []
            for g in gs:
                _, (cross, upper, lower) = member_parts(k, g, first)
                state.append((cross + shift_down(zero, lower), upper, lower, zero, zero, zero))

            def step(t, state):
                state = list(state)
                tile = first + 1 + t
                c = [coefm[q, at(tile), :] for q in range(8)]
                weight = cen[at(tile - first), :]
                for i, g in enumerate(gs):
                    sofar, u_old, d_old, w_old, acc0, acc1 = state[i]
                    x, (cross, upper, lower) = member_parts(k, g, tile, c)
                    out = sofar + shift_up(u_old, upper)
                    vk[k, g, at(tile - 1), :] = out
                    acc1 = acc1 + w_old * out
                    w = weight * x
                    acc0 = acc0 + w * x
                    state[i] = (cross + shift_down(d_old, lower), upper, lower, w, acc0, acc1)
                return tuple(state)
            state = lax.fori_loop(0, inner, step, tuple(state), unroll=split(inner, 22))
            for i, g in enumerate(gs):
                sofar, u_old, d_old, w_old, acc0, acc1 = state[i]
                _, (cross, upper, lower) = member_parts(k, g, last)
                out = sofar + shift_up(u_old, upper)
                vk[k, g, at(last - 1), :] = out
                vk[k, g, at(last), :] = cross + shift_down(d_old, lower) + shift_up(upper, zero)
                macc[2 * k, g] = acc0
                macc[2 * k + 1, g] = acc1 + w_old * out
            return carry
        lax.fori_loop(0, members // batch, sweep, 0)

    for c in sides:
        c.wait_recv()

    def merge(t, carry):
        fw, fe = [packin[0, g, t] for g in range(2)], [packin[1, g, t] for g in range(2)]
        for q in range(4):
            rs = at(first + t * 4 + q)
            for g, ref in enumerate((strips.at[0], kstrip)):
                x = ref[rs, :]
                keep = lane < EXTRA if g else lane >= 0
                x = jnp.where(jnp.logical_and(place < 3, keep),
                              roll(fw[g], (-3 * q) % cols) if q else fw[g], x)
                x = jnp.where(jnp.logical_and(place > 12, keep), roll(fe[g], 10 - 3 * q), x)
                ref[rs, :] = x
        return carry
    lax.fori_loop(0, tiles // 4, merge, 0, unroll=split(tiles // 4, 6))

    def take_rows(side, tile, seen):
        rs = at(tile)

        def clean(x):
            return jnp.where(seen, x, 0.0)
        for a in range(ARRAYS):
            if a not in (RIM, KRIM):
                st[a, rs, :] = clean(rowin[side, a])
        o, k = clean(rowin[side, RIM]), clean(rowin[side, KRIM])
        ow, kw = (clean(diagin[2 * side, i]) for i in range(2))
        oe, ke = (roll(clean(diagin[2 * side + 1, i]), 10) for i in range(2))
        put_strip(rs, unfold(o, k, ow, kw, oe, ke))

    @pl.when(not_first)
    def _():
        for c in up:
            c.wait_recv()
        take_rows(0, first - 1, sub > 4)

    @pl.when(lat_first)
    def _():
        rs = at(first - 1)
        for a in range(ARRAYS):
            st[a, rs, :] = zero
        put_strip(rs, (zero, zero, zero))

    @pl.when(not_last)
    def _():
        for c in down:
            c.wait_recv()
        take_rows(1, last + 1, sub < 3)

    @pl.when(lat_last)
    def _():
        for c in folds:
            c.wait_recv()
        total = lon_count * cols
        rs = at(last + 1)
        shown = jnp.where(place < 8, place - 3, place + (cols - 13))
        origin = lax.rem(partner[0, 0] - lo * cols + total, total)

        def view(shift):
            start = lax.rem(origin + shift + total, total)
            chunk = lax.div(start, cols)
            head = start - chunk * cols
            slots = [lax.rem(lo - chunk - o + 3 * lon_count, lon_count) for o in (1, 0, -1, -2)]
            z = head - shown
            return (slots, jnp.bitwise_and(head - lane, cols - 1), lane <= head,
                    jnp.bitwise_and(z, cols - 1), (z >= cols, z >= 0, z >= -cols))

        def take(x, where):
            return jnp.take_along_axis(x, where, axis=1, mode="promise_in_bounds")
        views = {s: view(s) for s in (-1, 0, 1)}
        shifts = {EAST: -1, NEAST: -1, NWEST: 1}
        ghost = [zero, zero]
        blocks = []
        for i, a in enumerate(fold_arrays):
            slots, where, within, where_s, (far, near, back) = views[shifts.get(a, 0)]
            chunks = [jnp.where(sub < 3, fold[s, i], 0.0) for s in slots]
            block = jnp.where(within, take(chunks[1], where), take(chunks[2], where))
            st[a, rs, :] = block
            blocks.append(block)
            x = jnp.where(back, take(chunks[2], where_s), take(chunks[3], where_s))
            x = jnp.where(near, take(chunks[1], where_s), x)
            x = jnp.where(far, take(chunks[0], where_s), x)
            s, g = (0, a) if a < members else (1, COUPLED.index(a))
            ghost[s] = jnp.where(group == g, x, ghost[s])
            if a == NORTH:
                end = pl.ds(EDGE + rows - 1, 1)
                st[NORTH, end, :] = 0.5 * (st[NORTH, end, :] + block[2:3, :])
                mixed = 0.5 * (kstrip[end, :] + x[2:3, :])
                g1, l1 = group[0:1, :], lane[0:1, :]
                dropped = jnp.logical_or(jnp.logical_or(g1 == 2, g1 == 3),
                                         jnp.logical_or(l1 == EXTRA + 1, l1 == EXTRA + 2))
                kstrip[end, :] = jnp.where(
                    dropped, 0.0, jnp.where(g1 == 1, mixed, kstrip[end, :]))
                st[NEAST, end, :] = jnp.zeros((1, cols), f32)
                st[NWEST, end, :] = jnp.zeros((1, cols), f32)
        o, k = rim(blocks[:members]), rim(blocks[members:])
        ring = unfold(o, k, zero, zero, zero, zero)[1]
        put_strip(rs, (ghost[0], ring, extras(ghost[1], k)))

    for tile in (first - 1, first, last, last + 1):
        main_coefs(tile)

    def edge_coefs(t, carry):
        strip_coefs(first - 1 + t)
        return carry
    lax.fori_loop(0, tiles + 2, edge_coefs, 0, unroll=split(tiles + 2, 26))

    def join(lo_parts, mid, hi_parts):
        out = mid[0]
        out = out + shift_down(zero if lo_parts is None else lo_parts[2], mid[2])
        return out + shift_up(mid[1], zero if hi_parts is None else hi_parts[1])

    for k in range(ITERS):
        _, (cross, upper, lower) = strip_parts(k, first - 1)

        def strip_step(t, carry):
            sofar, u_old, d_old, w_old, acc0, acc1 = carry
            tile = first + t
            x, (cross, upper, lower) = strip_parts(k, tile)
            out = sofar + shift_up(u_old, upper)
            strips[k + 1, at(tile - 1), :] = out
            acc1 = acc1 + w_old * out
            w_old = coefs[8, at(tile), :] * x
            acc0 = acc0 + w_old * x
            return cross + shift_down(d_old, lower), upper, lower, w_old, acc0, acc1
        sofar, u_old, d_old, w_old, acc0, acc1 = lax.fori_loop(
            0, tiles, strip_step,
            (cross + shift_down(zero, lower), upper, lower, zero, zero, zero),
            unroll=split(tiles, 24))
        _, (cross, upper, lower) = strip_parts(k, last + 1)
        out = sofar + shift_up(u_old, upper)
        strips[k + 1, at(last), :] = out
        strips[k + 1, at(last + 1), :] = cross + shift_down(d_old, lower) + shift_up(upper, zero)
        sacc[2 * k] = acc0
        sacc[2 * k + 1] = acc1 + w_old * out

        def band(g, carry):
            b = [member_parts(k, g, t) for t in (first - 1, first, first + 1)]
            t = [member_parts(k, g, t) for t in (last - 1, last, last + 1)]
            if k + 1 < ITERS:
                vk[k, g, at(first - 1), :] = join(None, b[0][1], b[1][1])
                vk[k, g, at(last + 1), :] = join(t[1][1], t[2][1], None)
            acc0, acc1 = macc[2 * k, g], macc[2 * k + 1, g]
            for tile, three in ((first, b), (last, t)):
                out = join(three[0][1], three[1][1], three[2][1])
                vk[k, g, at(tile), :] = out
                x = three[1][0]
                w = cen[at(tile - first), :] * x
                acc0 = acc0 + w * x
                acc1 = acc1 + w * out
            macc[2 * k, g] = acc0
            macc[2 * k + 1, g] = acc1
            return carry
        lax.fori_loop(0, members, band, 0, unroll=members)

    def column_sum(x):
        for s in (4, 2, 1):
            x = x + roll(x, s, 0)
        return x
    row = zero
    for i in range(2 * ITERS):
        total = macc[i, :, 0, :]
        for s in range(1, 8):
            total = total + macc[i, :, s, :]
        total = jnp.where(jnp.logical_and(lane > 2, lane < cols - 3), total, 0.0)
        total = total + jnp.where(group == sub, column_sum(sacc[i]), 0.0)
        total = jnp.sum(total, axis=1, keepdims=True)
        row = jnp.where(lane == 8 * i + sub, total, row)

    row = column_sum(row)

    def reduce(value, slot, recv, me, ss, rs, count, dev, between=None):
        red[slot] = value
        cps = [
            pltpu.make_async_remote_copy(
                src_ref=red.at[slot, pl.ds(0, 1)], dst_ref=recv.at[me, pl.ds(0, 1)],
                send_sem=ss.at[d], recv_sem=rs.at[d], device_id=dev(d), device_id_type=MESH)
            for d in range(1, count)
        ]
        for c in cps:
            c.start()
        recv[me] = value
        if between:
            between()
        for c in cps:
            c.wait_recv()
        out = recv[0, pl.ds(0, 1), :]
        for d in range(1, count):
            out = out + recv[d, pl.ds(0, 1), :]
        return jnp.broadcast_to(out, (8, cols)), cps

    outer = jnp.logical_or(lane < 3, lane > cols - 4)

    def close_rims():
        for k in range(1, ITERS + 1):
            def close(t, carry):
                rs = at(first + t)
                x = strips[k, rs, :]
                x = jnp.where(place < 3, roll(x, cols - 10), x)
                for m in range(members):
                    edge = roll(x, (cols - 3 - SLOT * m) % cols)
                    vk[k - 1, m, rs, :] = jnp.where(outer, edge, vk[k - 1, m, rs, :])
                return carry
            lax.fori_loop(0, tiles, close, 0, unroll=split(tiles, 8))

    row, c1 = reduce(row, 0, redlon, lo, lon_ss, lon_rs, lon_count,
                     lambda d: (la, lax.rem(lo + d, lon_count)), close_rims)
    row, c2 = reduce(row, 1, redlat, la, lat_ss, lat_rs, lat_count,
                     lambda d: (lax.rem(la + d, lat_count), lo))

    m0, m1, m2, m3, m4, m5 = (
        jnp.broadcast_to(
            jnp.sum(jnp.where(lane == 8 * i + sub, row, 0.0), axis=1, keepdims=True), (8, cols))
        for i in range(2 * ITERS))
    a0 = m1 / m0
    h1 = m2 - a0 * m1
    a1 = (m3 - 2.0 * a0 * m2 + a0 * a0 * m1) / h1
    b1 = h1 / m0
    p1 = -(a0 + a1)
    p0 = a0 * a1 - b1
    h2 = m4 + p1 * m3 + p0 * m2
    a2 = (m5 + p1 * m4 + p0 * m3) / h2 + p1
    b2 = h2 / h1
    t2 = p1 - a2
    t1 = p0 - a2 * p1 - b2
    t0 = b2 * a0 - a2 * p0
    q3 = 1.0 / (1.0 + t2 + t1 + t0)
    q2, q1, q0 = t2 * q3, t1 * q3, t0 * q3
    for i, value in enumerate((q3 + q2 + q1, q2 + q3, q3, q0, q1, q2, q3)):
        mix[i] = value

    for c in sides + c1 + c2:
        c.wait_send()

    @pl.when(not_last)
    def _():
        for c in up:
            c.wait_send()

    @pl.when(not_first)
    def _():
        for c in down:
            c.wait_send()

    @pl.when(lat_last)
    def _():
        for c in folds:
            c.wait_send()


def finish(st, vk, mix, center, sol_out, res_out, obuf, store_sem):
    members, rows, cols = sol_out.shape

    def one(m, carry):
        s0, s1, s2, q0, q1, q2, q3 = (
            jnp.broadcast_to(mix[i, pl.ds(m, 1), :], (8, cols)) for i in range(7))
        for t in range(rows // 8):
            here, rs = pl.ds(8 * t, 8), pl.ds(EDGE + 8 * t, 8)
            v0, v1, v2, v3 = st[m, rs, :], vk[0, m, rs, :], vk[1, m, rs, :], vk[2, m, rs, :]
            obuf[0, m, here, :] = s0 * v0 + s1 * v1 + s2 * v2
            obuf[1, m, here, :] = center[here, :] * (q0 * v0 + q1 * v1 + q2 * v2 + q3 * v3)
        for o, dst in ((0, sol_out), (1, res_out)):
            pltpu.make_async_copy(obuf.at[o, m], dst.at[m], store_sem.at[o, m]).start()
        return carry
    lax.fori_loop(0, members, one, 0)
    for m in range(members):
        for o, dst in ((0, sol_out), (1, res_out)):
            pltpu.make_async_copy(obuf.at[o, m], dst.at[m], store_sem.at[o, m]).wait()


def body(lat_count, lon_count, right_side, center, couplings, land_sea, fold_partner):
    members, rows, cols = right_side.shape
    f32 = jnp.float32
    hbm = pl.BlockSpec(memory_space=pltpu.HBM)
    vmem = pl.BlockSpec(memory_space=pltpu.VMEM)
    dma = pltpu.SemaphoreType.DMA
    shape = jax.ShapeDtypeStruct(right_side.shape, f32)
    high = rows + 2 * EDGE
    tiles = rows // 8
    folded = members + len(COUPLED)
    st, vk, mix, cen = pl.pallas_call(
        functools.partial(kernel, lat_count, lon_count),
        out_shape=(pltpu.VMEM((ARRAYS, high, cols), f32),
                   pltpu.VMEM((ITERS, members, high, cols), f32),
                   pltpu.VMEM((7, 8, cols), f32),
                   pltpu.VMEM((rows, cols), f32)),
        in_specs=[hbm] * 5,
        out_specs=(vmem, vmem, vmem, vmem),
        scratch_shapes=[
            pltpu.VMEM((rows, cols), jnp.int32),
            pltpu.SMEM((1, cols), jnp.int32),
            pltpu.VMEM((ITERS + 1, high, cols), f32),
            pltpu.VMEM((high, cols), f32),
            pltpu.VMEM((high, cols), f32),
            pltpu.VMEM((8, high, cols), f32),
            pltpu.VMEM((9, high, cols), f32),
            pltpu.VMEM((2, 2, tiles // 4, 8, cols), f32),
            pltpu.VMEM((2, 2, tiles // 4, 8, cols), f32),
            pltpu.VMEM((2, ARRAYS, 8, cols), f32),
            pltpu.VMEM((4, 2, 8, cols), f32),
            pltpu.VMEM((lon_count, folded, 8, cols), f32),
            pltpu.VMEM((2 * ITERS, members, 8, cols), f32),
            pltpu.VMEM((2 * ITERS, 8, cols), f32),
            pltpu.VMEM((2, 8, cols), f32),
            pltpu.VMEM((lon_count, 8, cols), f32),
            pltpu.VMEM((lat_count, 8, cols), f32),
            dma((5,)), dma((8,)), dma((8,)),
            dma((lon_count,)), dma((lon_count,)),
            dma((lon_count,)), dma((lon_count,)),
            dma((lat_count,)), dma((lat_count,)),
        ],
        compiler_params=pltpu.CompilerParams(
            collective_id=0, has_side_effects=True, vmem_limit_bytes=32 * 1024 * 1024),
    )(*(pltpu.with_memory_space_constraint(x, pltpu.HBM) for x in (
        right_side, center, couplings, land_sea, fold_partner.reshape(lon_count, cols))))
    return pl.pallas_call(
        finish,
        out_shape=(shape, shape),
        in_specs=[vmem] * 4,
        out_specs=(hbm, hbm),
        scratch_shapes=[
            pltpu.VMEM((2, members, rows, cols), f32),
            dma((2, members)),
        ],
        compiler_params=pltpu.CompilerParams(vmem_limit_bytes=16 * 1024 * 1024),
    )(st, vk, mix, cen)


def solution(mesh):
    return jax.shard_map(
        functools.partial(body, mesh.shape["lat"], mesh.shape["lon"]),
        mesh=mesh,
        in_specs=(
            P(None, "lat", "lon"),
            P("lat", "lon"),
            P(None, "lat", "lon"),
            P("lat", "lon"),
            P(),
        ),
        out_specs=(P(None, "lat", "lon"), P(None, "lat", "lon")),
        check_vma=False,
    )
```

```python
import functools

import jax
import jax.numpy as jnp
from jax import lax
from jax.experimental import pallas as pl
from jax.experimental.pallas import tpu as pltpu
from jax.sharding import PartitionSpec as P

ITERS = 3
BATCH = 2
MESH = pl.DeviceIdType.MESH
EDGE = 16
SLOT = 16
RIM, KRIM, EAST, NORTH, NEAST, NWEST, SCALE, ARRAYS = range(8, 16)
EXTRA = 5 * SLOT
COUPLED = (EAST, NORTH, NEAST, NWEST, SCALE)
FROM_S, FROM_N, FROM_SW, FROM_SE, FROM_NW, FROM_NE, FROM_W, FROM_E = range(8)


def roll(x, shift, axis=1):
    return pltpu.roll(x, shift, axis)


def kernel(
    lat_count, lon_count,
    rhs, center_hbm, coup_hbm, land_hbm, partner_hbm, st, vk, mix, cen,
    land, partner, strips, kstrip, beyond, coefm, coefs, wide, pack, packin, rowin, diagin, fold,
    macc, sacc, red, redlon, redlat,
    load_sem, send_sem, recv_sem, fold_ss, fold_rs, lon_ss, lon_rs, lat_ss, lat_rs,
):
    f32 = jnp.float32
    members, rows, cols = rhs.shape
    tiles = rows // 8
    first, last = 2, tiles + 1
    inner = tiles - 2

    def split(count, most):
        return max(u for u in range(1, most + 1) if count % u == 0)

    la, lo = lax.axis_index("lat"), lax.axis_index("lon")
    lat_first, lat_last = la == 0, la == lat_count - 1
    not_first, not_last = la > 0, la < lat_count - 1
    north, south = lax.rem(la + 1, lat_count), lax.rem(la + lat_count - 1, lat_count)
    east, west = lax.rem(lo + 1, lon_count), lax.rem(lo + lon_count - 1, lon_count)
    lane = lax.broadcasted_iota(jnp.int32, (8, cols), 1)
    sub = lax.broadcasted_iota(jnp.int32, (8, cols), 0)
    place = jnp.bitwise_and(lane, SLOT - 1)
    group = lax.shift_right_logical(lane, 4)
    zero = jnp.zeros((8, cols), f32)

    def at(tile):
        start = tile * 8
        return pl.ds(start if isinstance(start, int) else pl.multiple_of(start, 8), 8)

    loads = []
    for i, (start, size) in enumerate(((0, 8), (rows - 8, 8), (8, rows - 16))):
        rs, own = pl.ds(start, size), pl.ds(EDGE + start, size)
        loads += [
            pltpu.make_async_copy(center_hbm.at[rs], cen.at[rs], load_sem.at[i, 0]),
            pltpu.make_async_copy(land_hbm.at[rs], land.at[rs], load_sem.at[i, 1]),
            pltpu.make_async_copy(coup_hbm.at[:, rs], st.at[pl.ds(EAST, 4), own],
                                  load_sem.at[i, 2]),
            pltpu.make_async_copy(rhs.at[:, rs], st.at[pl.ds(0, members), own],
                                  load_sem.at[i, 3]),
        ]
    loads.append(pltpu.make_async_copy(partner_hbm.at[pl.ds(0, 1)], partner, load_sem.at[0, 4]))
    for c in loads:
        c.start()

    barrier = pltpu.get_barrier_semaphore()
    partners = [(la, lax.rem(lo + d, lon_count)) for d in range(1, lon_count)]
    partners += [(lax.rem(la + d, lat_count), lo) for d in range(1, lat_count)]
    for p in partners:
        pl.semaphore_signal(barrier, inc=1, device_id=p, device_id_type=MESH)

    @pl.when(not_last)
    def _():
        for p in ((north, east), (north, west)):
            pl.semaphore_signal(barrier, inc=1, device_id=p, device_id_type=MESH)

    @pl.when(not_first)
    def _():
        for p in ((south, east), (south, west)):
            pl.semaphore_signal(barrier, inc=1, device_id=p, device_id_type=MESH)
    arrivals = (len(partners) + 2 * jnp.where(not_last, 1, 0) + 2 * jnp.where(not_first, 1, 0))

    rim_lanes = [jnp.bitwise_and(lane - (SLOT * g - 3), cols - 1) < 12 for g in range(8)]

    def rim(arrays):
        out = zero
        for g, x in enumerate(arrays):
            out = jnp.where(rim_lanes[g], roll(x, g * SLOT + 3), out)
        return out

    def prep_tile(tile):
        rs = at(tile)
        near = at(tile - first)
        d = land[near, :].astype(f32) / cen[near, :]
        st[SCALE, rs, :] = d
        vals = []
        for m in range(members):
            v = st[m, rs, :] * d
            st[m, rs, :] = v
            vals.append(v)
        st[RIM, rs, :] = rim(vals)
        st[KRIM, rs, :] = rim([st[c, rs, :] for c in COUPLED[:4]] + [d])

    def prep(t, carry):
        prep_tile(first + 1 + t)
        return carry

    def fill(t, carry):
        packs = [zero] * 4
        for q in range(4):
            rs = at(first + t * 4 + q)
            here = jnp.logical_and(place >= 3 * q, place < 3 * q + 3)
            after = jnp.logical_and(place >= 3 * q + 3, place < 3 * q + 6)
            for g in range(2):
                x = st[RIM + g, rs, :]
                x = roll(x, 3 * q) if q else x
                packs[g] = jnp.where(here, x, packs[g])
                packs[2 + g] = jnp.where(after, x, packs[2 + g])
        for side in range(2):
            for g in range(2):
                pack[side, g, t] = packs[2 * side + g]
        return carry

    top, bottom = pl.ds(EDGE + rows - 3, 3), pl.ds(EDGE, 3)

    def remote(src, dst, slot, dev):
        return pltpu.make_async_remote_copy(
            src_ref=src, dst_ref=dst, send_sem=send_sem.at[slot], recv_sem=recv_sem.at[slot],
            device_id=dev, device_id_type=MESH)

    sides = [remote(pack.at[0], packin.at[0], FROM_W, (la, east)),
             remote(pack.at[1], packin.at[1], FROM_E, (la, west))]
    pair = pl.ds(RIM, 2)
    low, high = pl.ds(5, 3), pl.ds(0, 3)
    up = [remote(st.at[:, top], rowin.at[0, :, low], FROM_S, (north, lo)),
          remote(st.at[pair, top], diagin.at[0, :, low], FROM_SW, (north, east)),
          remote(st.at[pair, top], diagin.at[1, :, low], FROM_SE, (north, west))]
    down = [remote(st.at[:, bottom], rowin.at[1, :, high], FROM_N, (south, lo)),
            remote(st.at[pair, bottom], diagin.at[2, :, high], FROM_NW, (south, east)),
            remote(st.at[pair, bottom], diagin.at[3, :, high], FROM_NE, (south, west))]
    fold_arrays = list(range(members)) + list(COUPLED)
    fold_picks = {a: (0, 1, 2) for a in range(members)}
    fold_picks.update({EAST: (0, 1), NORTH: (1, 2, 0), NEAST: (1, 2), NWEST: (1, 2), SCALE: (0, 1)})
    fold_start = [0]
    for a in fold_arrays:
        fold_start.append(fold_start[-1] + len(fold_picks[a]))
    sent = pl.ds(0, fold_start[-1])
    mate = lo + 1 - 2 * lax.rem(lo, 2)
    half = lon_count // 2

    def fold_copy(sender, slot, dev):
        return pltpu.make_async_remote_copy(
            src_ref=fold.at[sender, sent], dst_ref=fold.at[sender, sent],
            send_sem=fold_ss.at[slot], recv_sem=fold_rs.at[slot],
            device_id=(la, dev), device_id_type=MESH)
    folds = [fold_copy(lo, 0, mate)]
    folds += [fold_copy(lo, j, lax.rem(lo + 2 * j, lon_count)) for j in range(1, half)]
    relays = [fold_copy(lax.rem(lo + lon_count - 2 * j, lon_count), half + j, mate)
              for j in range(1, half)]

    for c in loads[:8]:
        c.wait()
    prep_tile(first)
    prep_tile(last)

    late = lo >= half
    send_first = jnp.logical_and(lat_last, late)

    @pl.when(lat_last)
    def _():
        end = EDGE + rows - 1
        for i, a in enumerate(fold_arrays):
            for g, r in enumerate(fold_picks[a]):
                fold[lo, pl.ds(fold_start[i] + g, 1), :] = st[a, pl.ds(end - r, 1), :]
        for i in range(fold_start[-1], fold.shape[1]):
            fold[lo, pl.ds(i, 1), :] = jnp.zeros((1, cols), f32)

    def send_folds():
        if lat_count > 1:
            for c in down:
                c.start()
        for c in folds[half // 2:] + folds[:half // 2]:
            c.start()

    @pl.when(send_first)
    def _():
        pl.semaphore_wait(barrier, arrivals)
        send_folds()

    for c in loads[8:]:
        c.wait()
    lax.fori_loop(0, inner, prep, 0, unroll=split(inner, 11))
    lax.fori_loop(0, tiles // 4, fill, 0, unroll=split(tiles // 4, 6))

    @pl.when(jnp.logical_not(send_first))
    def _():
        pl.semaphore_wait(barrier, arrivals)

    send_later = jnp.logical_and(lat_last, jnp.logical_not(late))

    @pl.when(send_later)
    def _():
        if lat_count > 1:
            for c in down:
                c.start()
        for c in folds[:half // 2:-1]:
            c.start()

    sides[1].start()

    @pl.when(send_later)
    def _():
        for c in folds[:1] + folds[half // 2:0:-1]:
            c.start()

    sides[0].start()

    @pl.when(not_last)
    def _():
        for c in up:
            c.start()

    @pl.when(jnp.logical_and(not_first, not_last))
    def _():
        for c in down:
            c.start()

    def unfold(o, k, ow, kw, oe, ke):
        def windows(x, w, e):
            x = jnp.where(place < 8, x, roll(x, 10))
            x = jnp.where(place < 3, w, x)
            return jnp.where(place < 13, x, e)
        ring = jnp.where(place == 7, roll(o, cols - 1), jnp.where(place == 8, roll(o, 11), 0.0))
        return windows(o, ow, oe), ring, extras(windows(k, kw, ke), k)

    def extras(x, k):
        x = jnp.where(lane == EXTRA, roll(k, EXTRA + 3), x)
        x = jnp.where(lane == EXTRA + 1, roll(k, EXTRA + 1 - 2 * SLOT + 3), x)
        return jnp.where(lane == EXTRA + 2, roll(k, EXTRA + 2 - 3 * SLOT - 8), x)

    def put_strip(rs, parts_):
        strips[0, rs, :], beyond[rs, :], kstrip[rs, :] = parts_

    def open_rims(t, carry):
        rs = at(first + t)
        put_strip(rs, unfold(st[RIM, rs, :], st[KRIM, rs, :], zero, zero, zero, zero))
        return carry

    def main_coefs(tile):
        rs = at(tile)
        start = tile * 8
        below = pl.ds(start - 1, 8)
        above = pl.ds(start + 1, 8)
        d, dn = st[SCALE, rs, :], st[SCALE, above, :]
        ds_ = st[SCALE, below, :]
        coefm[0, rs, :] = d * st[EAST, rs, :]
        coefm[1, rs, :] = d * roll(st[EAST, rs, :], 1)
        coefm[2, rs, :] = ds_ * st[NORTH, below, :]
        coefm[3, rs, :] = ds_ * st[NEAST, below, :]
        coefm[4, rs, :] = ds_ * st[NWEST, below, :]
        coefm[5, rs, :] = dn * st[NORTH, rs, :]
        coefm[6, rs, :] = dn * roll(st[NWEST, rs, :], cols - 1)
        coefm[7, rs, :] = dn * roll(st[NEAST, rs, :], 1)

    def spread_tile(tile):
        rs = at(tile)
        x = kstrip[rs, :]

        def spread(g, shift=0):
            where = jnp.bitwise_and(place + (g * SLOT + shift), cols - 1)
            if shift < 0:
                where = jnp.where(place == 8, EXTRA + g // 2, where)
            if shift > 0:
                where = jnp.where(place == 7, EXTRA + 2, where)
            return jnp.take_along_axis(x, where, axis=1, mode="promise_in_bounds")
        d = spread(4)
        wide[0, rs, :] = d
        for g in range(1, 4):
            wide[g, rs, :] = spread(g)
        coefs[0, rs, :] = d * spread(0)
        coefs[1, rs, :] = d * spread(0, -1)
        coefs[6, rs, :] = spread(3, 1)
        coefs[7, rs, :] = spread(2, -1)
        edge = jnp.logical_or(jnp.logical_and(place >= 3, place < 6),
                              jnp.logical_and(place >= 10, place < 13))
        used = jnp.logical_and(edge, d > 0.0)
        coefs[8, rs, :] = jnp.where(used, 1.0 / jnp.where(used, d, 1.0), 0.0)

    def strip_coefs(tile):
        rs = at(tile)
        start = tile * 8
        below = pl.ds(start - 1, 8)
        above = pl.ds(start + 1, 8)
        ds_, dn = wide[0, below, :], wide[0, above, :]
        for g in range(1, 4):
            coefs[1 + g, rs, :] = ds_ * wide[g, below, :]
        coefs[5, rs, :] = dn * wide[1, rs, :]
        coefs[6, rs, :] = dn * coefs[6, rs, :]
        coefs[7, rs, :] = dn * coefs[7, rs, :]

    def all_coefs(t, carry):
        main_coefs(first + t)
        return carry
    lax.fori_loop(0, tiles, all_coefs, 0, unroll=split(tiles, 24))
    lax.fori_loop(0, tiles, open_rims, 0, unroll=split(tiles, 24))

    def parts(x, xe, xw, c):
        cross = c[0] * xe + c[1] * xw
        upper = c[2] * x + (c[3] * xe + c[4] * xw)
        lower = c[5] * x + (c[6] * xe + c[7] * xw)
        return cross, upper, lower

    def shift_up(u, u_next):
        return roll(jnp.where(sub == 0, u_next, u), 7, 0)

    def shift_down(d_prev, d):
        return roll(jnp.where(sub == 7, d_prev, d), 1, 0)

    def source(k, g, rs):
        return st[g, rs, :] if k == 0 else vk[k - 1, g, rs, :]

    def strip_parts(k, tile):
        rs = at(tile)
        x = strips[k, rs, :]
        xe, xw = roll(x, cols - 1), roll(x, 1)
        if k == 0:
            near = beyond[rs, :]
            xe, xw = jnp.where(place == 7, near, xe), jnp.where(place == 8, near, xw)
        return x, parts(x, xe, xw, [coefs[q, rs, :] for q in range(8)])

    def member_parts(k, g, tile, c=None):
        rs = at(tile)
        x = source(k, g, rs)
        if c is None:
            c = [coefm[q, rs, :] for q in range(8)]
        return x, parts(x, roll(x, cols - 1), roll(x, 1), c)

    batch = BATCH
    for k in range(ITERS):
        def sweep(p, carry):
            gs = [p * batch + i for i in range(batch)]
            state = []
            for g in gs:
                _, (cross, upper, lower) = member_parts(k, g, first)
                state.append((cross + shift_down(zero, lower), upper, lower, zero, zero, zero))

            def step(t, state):
                state = list(state)
                tile = first + 1 + t
                c = [coefm[q, at(tile), :] for q in range(8)]
                weight = cen[at(tile - first), :]
                for i, g in enumerate(gs):
                    sofar, u_old, d_old, w_old, acc0, acc1 = state[i]
                    x, (cross, upper, lower) = member_parts(k, g, tile, c)
                    out = sofar + shift_up(u_old, upper)
                    vk[k, g, at(tile - 1), :] = out
                    acc1 = acc1 + w_old * out
                    w = weight * x
                    acc0 = acc0 + w * x
                    state[i] = (cross + shift_down(d_old, lower), upper, lower, w, acc0, acc1)
                return tuple(state)
            state = lax.fori_loop(0, inner, step, tuple(state), unroll=split(inner, 22))
            for i, g in enumerate(gs):
                sofar, u_old, d_old, w_old, acc0, acc1 = state[i]
                _, (cross, upper, lower) = member_parts(k, g, last)
                out = sofar + shift_up(u_old, upper)
                vk[k, g, at(last - 1), :] = out
                vk[k, g, at(last), :] = cross + shift_down(d_old, lower) + shift_up(upper, zero)
                macc[2 * k, g] = acc0
                macc[2 * k + 1, g] = acc1 + w_old * out
            return carry
        lax.fori_loop(0, members // batch, sweep, 0)

    @pl.when(lat_last)
    def _():
        for c in folds[1:]:
            c.wait_recv()
        for c in relays:
            c.start()

    def join(lo_parts, mid, hi_parts):
        out = mid[0]
        out = out + shift_down(zero if lo_parts is None else lo_parts[2], mid[2])
        return out + shift_up(mid[1], zero if hi_parts is None else hi_parts[1])

    def bands(outer_tile, edge_tile, inner_tile):
        south_edge = outer_tile < edge_tile
        main_coefs(outer_tile)
        main_coefs(edge_tile)
        for k in range(ITERS):
            def band(g, carry):
                far, mid, near = (
                    member_parts(k, g, t) for t in (outer_tile, edge_tile, inner_tile))
                ordered = (far[1], mid[1], near[1]) if south_edge else (near[1], mid[1], far[1])
                if k + 1 < ITERS:
                    vk[k, g, at(outer_tile), :] = (
                        join(None, far[1], mid[1]) if south_edge else join(mid[1], far[1], None))
                out = join(*ordered)
                vk[k, g, at(edge_tile), :] = out
                x = mid[0]
                w = cen[at(edge_tile - first), :] * x
                macc[2 * k, g] = macc[2 * k, g] + w * x
                macc[2 * k + 1, g] = macc[2 * k + 1, g] + w * out
                return carry
            lax.fori_loop(0, members, band, 0, unroll=members)

    def take_rows(side, tile, seen):
        rs = at(tile)

        def clean(x):
            return jnp.where(seen, x, 0.0)
        for a in range(ARRAYS):
            if a not in (RIM, KRIM):
                st[a, rs, :] = clean(rowin[side, a])

    def take_corners(side, tile, seen):
        def clean(x):
            return jnp.where(seen, x, 0.0)
        o, k = clean(rowin[side, RIM]), clean(rowin[side, KRIM])
        ow, kw = (clean(diagin[2 * side, i]) for i in range(2))
        oe, ke = (roll(clean(diagin[2 * side + 1, i]), 10) for i in range(2))
        put_strip(at(tile), unfold(o, k, ow, kw, oe, ke))

    @pl.when(not_first)
    def _():
        up[0].wait_recv()
        take_rows(0, first - 1, sub > 4)

    @pl.when(lat_first)
    def _():
        rs = at(first - 1)
        for a in range(ARRAYS):
            st[a, rs, :] = zero
        put_strip(rs, (zero, zero, zero))

    bands(first - 1, first, first + 1)

    @pl.when(not_last)
    def _():
        down[0].wait_recv()
        take_rows(1, last + 1, sub < 3)
        bands(last + 1, last, last - 1)

    for c in sides:
        c.wait_recv()

    def merge(t, carry):
        fw, fe = [packin[0, g, t] for g in range(2)], [packin[1, g, t] for g in range(2)]
        for q in range(4):
            rs = at(first + t * 4 + q)
            for g, ref in enumerate((strips.at[0], kstrip)):
                x = ref[rs, :]
                keep = lane < EXTRA if g else lane >= 0
                x = jnp.where(jnp.logical_and(place < 3, keep),
                              roll(fw[g], (-3 * q) % cols) if q else fw[g], x)
                x = jnp.where(jnp.logical_and(place > 12, keep), roll(fe[g], 10 - 3 * q), x)
                ref[rs, :] = x
        return carry
    lax.fori_loop(0, tiles // 4, merge, 0, unroll=split(tiles // 4, 6))

    @pl.when(not_first)
    def _():
        for c in up[1:]:
            c.wait_recv()
        take_corners(0, first - 1, sub > 4)

    @pl.when(not_last)
    def _():
        for c in down[1:]:
            c.wait_recv()
        take_corners(1, last + 1, sub < 3)

    def edge_spread(t, carry):
        spread_tile(first - 1 + t)
        return carry
    lax.fori_loop(0, tiles, edge_spread, 0, unroll=split(tiles, 24))

    @pl.when(lat_last)
    def _():
        for c in folds[:1] + relays:
            c.wait_recv()
        total = lon_count * cols
        rs = at(last + 1)
        shown = jnp.where(place < 8, place - 3, place + (cols - 13))
        origin = lax.rem(partner[0, 0] - lo * cols + total, total)

        def view(shift):
            start = lax.rem(origin + shift + total, total)
            chunk = lax.div(start, cols)
            head = start - chunk * cols
            slots = [lax.rem(chunk + o + 2 * lon_count, lon_count) for o in (1, 0, -1, -2)]
            z = head - shown
            return (slots, jnp.bitwise_and(head - lane, cols - 1), lane <= head,
                    jnp.bitwise_and(z, cols - 1), (z >= cols, z >= 0, z >= -cols))

        def take(x, where):
            return jnp.take_along_axis(x, where, axis=1, mode="promise_in_bounds")
        views = {s: view(s) for s in (-1, 0, 1)}
        shifts = {EAST: -1, NEAST: -1, NWEST: 1}
        ghost = [zero, zero]
        blocks = []
        for i, a in enumerate(fold_arrays):
            slots, where, within, where_s, (far, near, back) = views[shifts.get(a, 0)]
            chunks = [jnp.where(sub < len(fold_picks[a]), fold[s, pl.ds(fold_start[i], 8), :], 0.0) for s in slots]
            block = jnp.where(within, take(chunks[1], where), take(chunks[2], where))
            st[a, rs, :] = block
            blocks.append(block)
            x = jnp.where(back, take(chunks[2], where_s), take(chunks[3], where_s))
            x = jnp.where(near, take(chunks[1], where_s), x)
            x = jnp.where(far, take(chunks[0], where_s), x)
            s, g = (0, a) if a < members else (1, COUPLED.index(a))
            ghost[s] = jnp.where(group == g, x, ghost[s])
            if a == NORTH:
                end = pl.ds(EDGE + rows - 1, 1)
                st[NORTH, end, :] = 0.5 * (st[NORTH, end, :] + block[2:3, :])
                red[0] = x
                st[NEAST, end, :] = jnp.zeros((1, cols), f32)
                st[NWEST, end, :] = jnp.zeros((1, cols), f32)
        o, k = rim(blocks[:members]), rim(blocks[members:])
        ring = unfold(o, k, zero, zero, zero, zero)[1]
        put_strip(rs, (ghost[0], ring, extras(ghost[1], k)))
        end = pl.ds(EDGE + rows - 1, 1)
        mixed = 0.5 * (kstrip[end, :] + red[0, pl.ds(2, 1), :])
        g1, l1 = group[0:1, :], lane[0:1, :]
        dropped = jnp.logical_or(jnp.logical_or(g1 == 2, g1 == 3),
                                 jnp.logical_or(l1 == EXTRA + 1, l1 == EXTRA + 2))
        kstrip[end, :] = jnp.where(dropped, 0.0, jnp.where(g1 == 1, mixed, kstrip[end, :]))
        bands(last + 1, last, last - 1)

    spread_tile(last)
    spread_tile(last + 1)

    def edge_coefs(t, carry):
        strip_coefs(first - 1 + t)
        return carry
    lax.fori_loop(0, tiles + 2, edge_coefs, 0, unroll=split(tiles + 2, 26))

    for k in range(ITERS):
        _, (cross, upper, lower) = strip_parts(k, first - 1)

        def strip_step(t, carry):
            sofar, u_old, d_old, w_old, acc0, acc1 = carry
            tile = first + t
            x, (cross, upper, lower) = strip_parts(k, tile)
            out = sofar + shift_up(u_old, upper)
            strips[k + 1, at(tile - 1), :] = out
            acc1 = acc1 + w_old * out
            w_old = coefs[8, at(tile), :] * x
            acc0 = acc0 + w_old * x
            return cross + shift_down(d_old, lower), upper, lower, w_old, acc0, acc1
        sofar, u_old, d_old, w_old, acc0, acc1 = lax.fori_loop(
            0, tiles, strip_step,
            (cross + shift_down(zero, lower), upper, lower, zero, zero, zero),
            unroll=split(tiles, 24))
        _, (cross, upper, lower) = strip_parts(k, last + 1)
        out = sofar + shift_up(u_old, upper)
        strips[k + 1, at(last), :] = out
        strips[k + 1, at(last + 1), :] = cross + shift_down(d_old, lower) + shift_up(upper, zero)
        sacc[2 * k] = acc0
        sacc[2 * k + 1] = acc1 + w_old * out

    def column_sum(x):
        for s in (4, 2, 1):
            x = x + roll(x, s, 0)
        return x
    row = zero
    for i in range(2 * ITERS):
        total = macc[i, :, 0, :]
        for s in range(1, 8):
            total = total + macc[i, :, s, :]
        total = jnp.where(jnp.logical_and(lane > 2, lane < cols - 3), total, 0.0)
        total = total + jnp.where(group == sub, column_sum(sacc[i]), 0.0)
        total = jnp.sum(total, axis=1, keepdims=True)
        row = jnp.where(lane == 8 * i + sub, total, row)

    row = column_sum(row)

    def reduce(value, slot, recv, me, ss, rs, count, dev, between=None):
        red[slot] = value
        cps = [
            pltpu.make_async_remote_copy(
                src_ref=red.at[slot, pl.ds(0, 1)], dst_ref=recv.at[me, pl.ds(0, 1)],
                send_sem=ss.at[d], recv_sem=rs.at[d], device_id=dev(d), device_id_type=MESH)
            for d in range(1, count)
        ]
        for c in cps:
            c.start()
        recv[me] = value
        if between:
            between()
        for c in cps:
            c.wait_recv()
        out = recv[0, pl.ds(0, 1), :]
        for d in range(1, count):
            out = out + recv[d, pl.ds(0, 1), :]
        return jnp.broadcast_to(out, (8, cols)), cps

    outer = jnp.logical_or(lane < 3, lane > cols - 4)

    def close_rims(stages):
        for k in stages:
            def close(t, carry):
                rs = at(first + t)
                x = strips[k, rs, :]
                x = jnp.where(place < 3, roll(x, cols - 10), x)
                for m in range(members):
                    edge = roll(x, (cols - 3 - SLOT * m) % cols)
                    vk[k - 1, m, rs, :] = jnp.where(outer, edge, vk[k - 1, m, rs, :])
                return carry
            lax.fori_loop(0, tiles, close, 0, unroll=split(tiles, 8))

    row, c1 = reduce(row, 0, redlon, lo, lon_ss, lon_rs, lon_count,
                     lambda d: (la, lax.rem(lo + d, lon_count)), lambda: close_rims((1, 2)))
    row, c2 = reduce(row, 1, redlat, la, lat_ss, lat_rs, lat_count,
                     lambda d: (lax.rem(la + d, lat_count), lo), lambda: close_rims((3,)))

    m0, m1, m2, m3, m4, m5 = (
        jnp.broadcast_to(
            jnp.sum(jnp.where(lane == 8 * i + sub, row, 0.0), axis=1, keepdims=True), (8, cols))
        for i in range(2 * ITERS))
    a0 = m1 / m0
    h1 = m2 - a0 * m1
    a1 = (m3 - 2.0 * a0 * m2 + a0 * a0 * m1) / h1
    b1 = h1 / m0
    p1 = -(a0 + a1)
    p0 = a0 * a1 - b1
    h2 = m4 + p1 * m3 + p0 * m2
    a2 = (m5 + p1 * m4 + p0 * m3) / h2 + p1
    b2 = h2 / h1
    t2 = p1 - a2
    t1 = p0 - a2 * p1 - b2
    t0 = b2 * a0 - a2 * p0
    q3 = 1.0 / (1.0 + t2 + t1 + t0)
    q2, q1, q0 = t2 * q3, t1 * q3, t0 * q3
    for i, value in enumerate((q3 + q2 + q1, q2 + q3, q3, q0, q1, q2, q3)):
        mix[i] = value

    for c in sides + c1 + c2:
        c.wait_send()

    @pl.when(not_last)
    def _():
        for c in up:
            c.wait_send()

    @pl.when(not_first)
    def _():
        for c in down:
            c.wait_send()

    @pl.when(lat_last)
    def _():
        for c in folds + relays:
            c.wait_send()


def finish(st, vk, mix, center, sol_out, res_out, obuf, store_sem):
    members, rows, cols = sol_out.shape

    def one(m, carry):
        s0, s1, s2, q0, q1, q2, q3 = (
            jnp.broadcast_to(mix[i, pl.ds(m, 1), :], (8, cols)) for i in range(7))
        for t in range(rows // 8):
            here, rs = pl.ds(8 * t, 8), pl.ds(EDGE + 8 * t, 8)
            v0, v1, v2, v3 = st[m, rs, :], vk[0, m, rs, :], vk[1, m, rs, :], vk[2, m, rs, :]
            obuf[0, m, here, :] = s0 * v0 + s1 * v1 + s2 * v2
            obuf[1, m, here, :] = center[here, :] * (q0 * v0 + q1 * v1 + q2 * v2 + q3 * v3)
        for o, dst in ((0, sol_out), (1, res_out)):
            pltpu.make_async_copy(obuf.at[o, m], dst.at[m], store_sem.at[o, m]).start()
        return carry
    lax.fori_loop(0, members, one, 0)
    for m in range(members):
        for o, dst in ((0, sol_out), (1, res_out)):
            pltpu.make_async_copy(obuf.at[o, m], dst.at[m], store_sem.at[o, m]).wait()


def body(lat_count, lon_count, right_side, center, couplings, land_sea, fold_partner):
    members, rows, cols = right_side.shape
    f32 = jnp.float32
    hbm = pl.BlockSpec(memory_space=pltpu.HBM)
    vmem = pl.BlockSpec(memory_space=pltpu.VMEM)
    dma = pltpu.SemaphoreType.DMA
    shape = jax.ShapeDtypeStruct(right_side.shape, f32)
    high = rows + 2 * EDGE
    tiles = rows // 8
    folded = -(-3 * (members + len(COUPLED)) // 8) * 8 + 8
    st, vk, mix, cen = pl.pallas_call(
        functools.partial(kernel, lat_count, lon_count),
        out_shape=(pltpu.VMEM((ARRAYS, high, cols), f32),
                   pltpu.VMEM((ITERS, members, high, cols), f32),
                   pltpu.VMEM((7, 8, cols), f32),
                   pltpu.VMEM((rows, cols), f32)),
        in_specs=[hbm] * 5,
        out_specs=(vmem, vmem, vmem, vmem),
        scratch_shapes=[
            pltpu.VMEM((rows, cols), jnp.int32),
            pltpu.SMEM((1, cols), jnp.int32),
            pltpu.VMEM((ITERS + 1, high, cols), f32),
            pltpu.VMEM((high, cols), f32),
            pltpu.VMEM((high, cols), f32),
            pltpu.VMEM((8, high, cols), f32),
            pltpu.VMEM((9, high, cols), f32),
            pltpu.VMEM((4, high, cols), f32),
            pltpu.VMEM((2, 2, tiles // 4, 8, cols), f32),
            pltpu.VMEM((2, 2, tiles // 4, 8, cols), f32),
            pltpu.VMEM((2, ARRAYS, 8, cols), f32),
            pltpu.VMEM((4, 2, 8, cols), f32),
            pltpu.VMEM((lon_count, folded, cols), f32),
            pltpu.VMEM((2 * ITERS, members, 8, cols), f32),
            pltpu.VMEM((2 * ITERS, 8, cols), f32),
            pltpu.VMEM((2, 8, cols), f32),
            pltpu.VMEM((lon_count, 8, cols), f32),
            pltpu.VMEM((lat_count, 8, cols), f32),
            dma((3, 5)), dma((8,)), dma((8,)),
            dma((lon_count,)), dma((lon_count,)),
            dma((lon_count,)), dma((lon_count,)),
            dma((lat_count,)), dma((lat_count,)),
        ],
        compiler_params=pltpu.CompilerParams(
            collective_id=0, has_side_effects=True, vmem_limit_bytes=32 * 1024 * 1024),
    )(*(pltpu.with_memory_space_constraint(x, pltpu.HBM) for x in (
        right_side, center, couplings, land_sea, fold_partner.reshape(lon_count, cols))))
    return pl.pallas_call(
        finish,
        out_shape=(shape, shape),
        in_specs=[vmem] * 4,
        out_specs=(hbm, hbm),
        scratch_shapes=[
            pltpu.VMEM((2, members, rows, cols), f32),
            dma((2, members)),
        ],
        compiler_params=pltpu.CompilerParams(vmem_limit_bytes=16 * 1024 * 1024),
    )(st, vk, mix, cen)


def solution(mesh):
    return jax.shard_map(
        functools.partial(body, mesh.shape["lat"], mesh.shape["lon"]),
        mesh=mesh,
        in_specs=(
            P(None, "lat", "lon"),
            P("lat", "lon"),
            P(None, "lat", "lon"),
            P("lat", "lon"),
            P(),
        ),
        out_specs=(P(None, "lat", "lon"), P(None, "lat", "lon")),
        check_vma=False,
    )
```

```python
import functools

import jax
import jax.numpy as jnp
from jax import lax
from jax.experimental import pallas as pl
from jax.experimental.pallas import tpu as pltpu
from jax.sharding import PartitionSpec as P

ITERS = 3
BATCH = 2
MESH = pl.DeviceIdType.MESH
EDGE = 16
SLOT = 16
RIM, KRIM, EAST, NORTH, NEAST, NWEST, SCALE, ARRAYS = range(8, 16)
EXTRA = 5 * SLOT
COUPLED = (EAST, NORTH, NEAST, NWEST, SCALE)
SIDES, UP, DOWN, UP_CORNERS, DOWN_CORNERS = range(5)


def roll(x, shift, axis=1):
    return pltpu.roll(x, shift, axis)


def kernel(
    lat_count, lon_count,
    rhs, center_hbm, coup_hbm, land_hbm, partner_hbm, st, vk, mix, cen,
    land, partner, strips, kstrip, beyond, coefm, coefs, wide, pack, packin, rowin, diagin, fold,
    macc, sacc, red, redlon, redlat,
    load_sem, send_sem, recv_sem, fold_sem, red_sem,
):
    f32 = jnp.float32
    members, rows, cols = rhs.shape
    tiles = rows // 8
    first, last = 2, tiles + 1
    inner = tiles - 2

    def split(count, most):
        return max(u for u in range(1, most + 1) if count % u == 0)

    la, lo = lax.axis_index("lat"), lax.axis_index("lon")
    lat_first, lat_last = la == 0, la == lat_count - 1
    not_first, not_last = la > 0, la < lat_count - 1
    north, south = lax.rem(la + 1, lat_count), lax.rem(la + lat_count - 1, lat_count)
    east, west = lax.rem(lo + 1, lon_count), lax.rem(lo + lon_count - 1, lon_count)
    lane = lax.broadcasted_iota(jnp.int32, (8, cols), 1)
    sub = lax.broadcasted_iota(jnp.int32, (8, cols), 0)
    place = jnp.bitwise_and(lane, SLOT - 1)
    group = lax.shift_right_logical(lane, 4)
    zero = jnp.zeros((8, cols), f32)

    def at(tile):
        start = tile * 8
        return pl.ds(start if isinstance(start, int) else pl.multiple_of(start, 8), 8)

    loads = []
    for i, (start, size) in enumerate(((0, 8), (rows - 8, 8), (8, rows - 16))):
        rs, own = pl.ds(start, size), pl.ds(EDGE + start, size)
        loads += [
            pltpu.make_async_copy(center_hbm.at[rs], cen.at[rs], load_sem.at[i // 2]),
            pltpu.make_async_copy(land_hbm.at[rs], land.at[rs], load_sem.at[i // 2]),
            pltpu.make_async_copy(coup_hbm.at[:, rs], st.at[pl.ds(EAST, 4), own],
                                  load_sem.at[i // 2]),
            pltpu.make_async_copy(rhs.at[:, rs], st.at[pl.ds(0, members), own],
                                  load_sem.at[i // 2]),
        ]
    loads.append(pltpu.make_async_copy(partner_hbm.at[pl.ds(0, 1)], partner, load_sem.at[2]))
    for c in loads:
        c.start()

    barrier = pltpu.get_barrier_semaphore()
    partners = [(la, lax.rem(lo + d, lon_count)) for d in range(1, lon_count)]
    partners += [(lax.rem(la + d, lat_count), lo) for d in range(1, lat_count)]
    for p in partners:
        pl.semaphore_signal(barrier, inc=1, device_id=p, device_id_type=MESH)

    @pl.when(not_last)
    def _():
        for p in ((north, east), (north, west)):
            pl.semaphore_signal(barrier, inc=1, device_id=p, device_id_type=MESH)

    @pl.when(not_first)
    def _():
        for p in ((south, east), (south, west)):
            pl.semaphore_signal(barrier, inc=1, device_id=p, device_id_type=MESH)
    arrivals = (len(partners) + 2 * jnp.where(not_last, 1, 0) + 2 * jnp.where(not_first, 1, 0))

    rim_lanes = [jnp.bitwise_and(lane - (SLOT * g - 3), cols - 1) < 12 for g in range(8)]

    def rim(arrays):
        out = zero
        for g, x in enumerate(arrays):
            out = jnp.where(rim_lanes[g], roll(x, g * SLOT + 3), out)
        return out

    def prep_tile(tile):
        rs = at(tile)
        near = at(tile - first)
        d = land[near, :].astype(f32) / cen[near, :]
        st[SCALE, rs, :] = d
        vals = []
        for m in range(members):
            v = st[m, rs, :] * d
            st[m, rs, :] = v
            vals.append(v)
        st[RIM, rs, :] = rim(vals)
        st[KRIM, rs, :] = rim([st[c, rs, :] for c in COUPLED[:4]] + [d])

    def prep(t, carry):
        prep_tile(first + 1 + t)
        return carry

    def fill(t, carry):
        packs = [zero] * 4
        for q in range(4):
            rs = at(first + t * 4 + q)
            here = jnp.logical_and(place >= 3 * q, place < 3 * q + 3)
            after = jnp.logical_and(place >= 3 * q + 3, place < 3 * q + 6)
            for g in range(2):
                x = st[RIM + g, rs, :]
                x = roll(x, 3 * q) if q else x
                packs[g] = jnp.where(here, x, packs[g])
                packs[2 + g] = jnp.where(after, x, packs[2 + g])
        for side in range(2):
            for g in range(2):
                pack[side, g, t] = packs[2 * side + g]
        return carry

    top, bottom = pl.ds(EDGE + rows - 3, 3), pl.ds(EDGE, 3)

    def remote(src, dst, slot, landing, dev):
        return pltpu.make_async_remote_copy(
            src_ref=src, dst_ref=dst, send_sem=send_sem.at[slot], recv_sem=recv_sem.at[landing],
            device_id=dev, device_id_type=MESH)

    sides = [remote(pack.at[0], packin.at[0], SIDES, SIDES, (la, east)),
             remote(pack.at[1], packin.at[1], SIDES, SIDES, (la, west))]
    pair = pl.ds(RIM, 2)
    low, high = pl.ds(5, 3), pl.ds(0, 3)
    up = [remote(st.at[:, top], rowin.at[0, :, low], UP, UP, (north, lo)),
          remote(st.at[pair, top], diagin.at[0, :, low], UP, UP_CORNERS, (north, east)),
          remote(st.at[pair, top], diagin.at[1, :, low], UP, UP_CORNERS, (north, west))]
    down = [remote(st.at[:, bottom], rowin.at[1, :, high], DOWN, DOWN, (south, lo)),
            remote(st.at[pair, bottom], diagin.at[2, :, high], DOWN, DOWN_CORNERS, (south, east)),
            remote(st.at[pair, bottom], diagin.at[3, :, high], DOWN, DOWN_CORNERS, (south, west))]
    fold_arrays = list(range(members)) + list(COUPLED)
    fold_picks = {a: (0, 1, 2) for a in range(members)}
    fold_picks.update({EAST: (0, 1), NORTH: (1, 2, 0), NEAST: (1, 2), NWEST: (1, 2), SCALE: (0, 1)})
    fold_start = [0]
    for a in fold_arrays:
        fold_start.append(fold_start[-1] + len(fold_picks[a]))
    sent = pl.ds(0, fold_start[-1])
    mate = lo + 1 - 2 * lax.rem(lo, 2)
    half = lon_count // 2

    def fold_copy(sender, landing, dev):
        return pltpu.make_async_remote_copy(
            src_ref=fold.at[sender, sent], dst_ref=fold.at[sender, sent],
            send_sem=fold_sem.at[0], recv_sem=fold_sem.at[landing],
            device_id=(la, dev), device_id_type=MESH)
    folds = [fold_copy(lo, 2, mate)]
    folds += [fold_copy(lo, 1, lax.rem(lo + 2 * j, lon_count)) for j in range(1, half)]
    relays = [fold_copy(lax.rem(lo + lon_count - 2 * j, lon_count), 2, mate)
              for j in range(1, half)]

    def settle(ref, sem):
        pltpu.make_async_copy(ref, ref, sem).wait()

    blocks = members + 6
    settle(st.at[pl.ds(0, blocks), pl.ds(0, 16)], load_sem.at[0])
    prep_tile(first)
    prep_tile(last)

    late = lo >= half
    send_first = jnp.logical_and(lat_last, late)

    @pl.when(lat_last)
    def _():
        end = EDGE + rows - 1
        for i, a in enumerate(fold_arrays):
            for g, r in enumerate(fold_picks[a]):
                fold[lo, pl.ds(fold_start[i] + g, 1), :] = st[a, pl.ds(end - r, 1), :]
        for i in range(fold_start[-1], fold.shape[1]):
            fold[lo, pl.ds(i, 1), :] = jnp.zeros((1, cols), f32)

    def send_folds():
        if lat_count > 1:
            for c in down:
                c.start()
        for c in folds[half // 2:] + folds[:half // 2]:
            c.start()

    @pl.when(send_first)
    def _():
        pl.semaphore_wait(barrier, arrivals)
        send_folds()

    settle(st.at[pl.ds(0, blocks), pl.ds(0, rows - 16)], load_sem.at[1])
    loads[-1].wait()
    lax.fori_loop(0, inner, prep, 0, unroll=split(inner, 11))
    lax.fori_loop(0, tiles // 4, fill, 0, unroll=split(tiles // 4, 6))

    @pl.when(jnp.logical_not(send_first))
    def _():
        pl.semaphore_wait(barrier, arrivals)

    send_later = jnp.logical_and(lat_last, jnp.logical_not(late))

    @pl.when(send_later)
    def _():
        if lat_count > 1:
            for c in down:
                c.start()
        for c in folds[:half // 2:-1]:
            c.start()

    sides[1].start()

    @pl.when(send_later)
    def _():
        for c in folds[:1] + folds[half // 2:0:-1]:
            c.start()

    sides[0].start()

    @pl.when(not_last)
    def _():
        for c in up:
            c.start()

    @pl.when(jnp.logical_and(not_first, not_last))
    def _():
        for c in down:
            c.start()

    def unfold(o, k, ow, kw, oe, ke):
        def windows(x, w, e):
            x = jnp.where(place < 8, x, roll(x, 10))
            x = jnp.where(place < 3, w, x)
            return jnp.where(place < 13, x, e)
        ring = jnp.where(place == 7, roll(o, cols - 1), jnp.where(place == 8, roll(o, 11), 0.0))
        return windows(o, ow, oe), ring, extras(windows(k, kw, ke), k)

    def extras(x, k):
        x = jnp.where(lane == EXTRA, roll(k, EXTRA + 3), x)
        x = jnp.where(lane == EXTRA + 1, roll(k, EXTRA + 1 - 2 * SLOT + 3), x)
        return jnp.where(lane == EXTRA + 2, roll(k, EXTRA + 2 - 3 * SLOT - 8), x)

    def put_strip(rs, parts_):
        strips[0, rs, :], beyond[rs, :], kstrip[rs, :] = parts_

    def open_rims(t, carry):
        rs = at(first + t)
        put_strip(rs, unfold(st[RIM, rs, :], st[KRIM, rs, :], zero, zero, zero, zero))
        return carry

    def main_coefs(tile):
        rs = at(tile)
        start = tile * 8
        below = pl.ds(start - 1, 8)
        above = pl.ds(start + 1, 8)
        d, dn = st[SCALE, rs, :], st[SCALE, above, :]
        ds_ = st[SCALE, below, :]
        coefm[0, rs, :] = d * st[EAST, rs, :]
        coefm[1, rs, :] = d * roll(st[EAST, rs, :], 1)
        coefm[2, rs, :] = ds_ * st[NORTH, below, :]
        coefm[3, rs, :] = ds_ * st[NEAST, below, :]
        coefm[4, rs, :] = ds_ * st[NWEST, below, :]
        coefm[5, rs, :] = dn * st[NORTH, rs, :]
        coefm[6, rs, :] = dn * roll(st[NWEST, rs, :], cols - 1)
        coefm[7, rs, :] = dn * roll(st[NEAST, rs, :], 1)

    def spread_tile(tile):
        rs = at(tile)
        x = kstrip[rs, :]

        def spread(g, shift=0):
            where = jnp.bitwise_and(place + (g * SLOT + shift), cols - 1)
            if shift < 0:
                where = jnp.where(place == 8, EXTRA + g // 2, where)
            if shift > 0:
                where = jnp.where(place == 7, EXTRA + 2, where)
            return jnp.take_along_axis(x, where, axis=1, mode="promise_in_bounds")
        d = spread(4)
        wide[0, rs, :] = d
        for g in range(1, 4):
            wide[g, rs, :] = spread(g)
        coefs[0, rs, :] = d * spread(0)
        coefs[1, rs, :] = d * spread(0, -1)
        coefs[6, rs, :] = spread(3, 1)
        coefs[7, rs, :] = spread(2, -1)
        edge = jnp.logical_or(jnp.logical_and(place >= 3, place < 6),
                              jnp.logical_and(place >= 10, place < 13))
        used = jnp.logical_and(edge, d > 0.0)
        coefs[8, rs, :] = jnp.where(used, 1.0 / jnp.where(used, d, 1.0), 0.0)

    def strip_coefs(tile):
        rs = at(tile)
        start = tile * 8
        below = pl.ds(start - 1, 8)
        above = pl.ds(start + 1, 8)
        ds_, dn = wide[0, below, :], wide[0, above, :]
        for g in range(1, 4):
            coefs[1 + g, rs, :] = ds_ * wide[g, below, :]
        coefs[5, rs, :] = dn * wide[1, rs, :]
        coefs[6, rs, :] = dn * coefs[6, rs, :]
        coefs[7, rs, :] = dn * coefs[7, rs, :]

    def all_coefs(t, carry):
        main_coefs(first + t)
        return carry
    lax.fori_loop(0, tiles, all_coefs, 0, unroll=split(tiles, 24))
    lax.fori_loop(0, tiles, open_rims, 0, unroll=split(tiles, 24))

    def parts(x, xe, xw, c):
        cross = c[0] * xe + c[1] * xw
        upper = c[2] * x + (c[3] * xe + c[4] * xw)
        lower = c[5] * x + (c[6] * xe + c[7] * xw)
        return cross, upper, lower

    def shift_up(u, u_next):
        return roll(jnp.where(sub == 0, u_next, u), 7, 0)

    def shift_down(d_prev, d):
        return roll(jnp.where(sub == 7, d_prev, d), 1, 0)

    def source(k, g, rs):
        return st[g, rs, :] if k == 0 else vk[k - 1, g, rs, :]

    def strip_parts(k, tile):
        rs = at(tile)
        x = strips[k, rs, :]
        xe, xw = roll(x, cols - 1), roll(x, 1)
        if k == 0:
            near = beyond[rs, :]
            xe, xw = jnp.where(place == 7, near, xe), jnp.where(place == 8, near, xw)
        return x, parts(x, xe, xw, [coefs[q, rs, :] for q in range(8)])

    def member_parts(k, g, tile, c=None):
        rs = at(tile)
        x = source(k, g, rs)
        if c is None:
            c = [coefm[q, rs, :] for q in range(8)]
        return x, parts(x, roll(x, cols - 1), roll(x, 1), c)

    batch = BATCH
    for k in range(ITERS):
        def sweep(p, carry):
            gs = [p * batch + i for i in range(batch)]
            state = []
            for g in gs:
                _, (cross, upper, lower) = member_parts(k, g, first)
                state.append((cross + shift_down(zero, lower), upper, lower, zero, zero, zero))

            def step(t, state):
                state = list(state)
                tile = first + 1 + t
                c = [coefm[q, at(tile), :] for q in range(8)]
                weight = cen[at(tile - first), :]
                for i, g in enumerate(gs):
                    sofar, u_old, d_old, w_old, acc0, acc1 = state[i]
                    x, (cross, upper, lower) = member_parts(k, g, tile, c)
                    out = sofar + shift_up(u_old, upper)
                    vk[k, g, at(tile - 1), :] = out
                    acc1 = acc1 + w_old * out
                    w = weight * x
                    acc0 = acc0 + w * x
                    state[i] = (cross + shift_down(d_old, lower), upper, lower, w, acc0, acc1)
                return tuple(state)
            state = lax.fori_loop(0, inner, step, tuple(state), unroll=split(inner, 22))
            for i, g in enumerate(gs):
                sofar, u_old, d_old, w_old, acc0, acc1 = state[i]
                _, (cross, upper, lower) = member_parts(k, g, last)
                out = sofar + shift_up(u_old, upper)
                vk[k, g, at(last - 1), :] = out
                vk[k, g, at(last), :] = cross + shift_down(d_old, lower) + shift_up(upper, zero)
                macc[2 * k, g] = acc0
                macc[2 * k + 1, g] = acc1 + w_old * out
            return carry
        lax.fori_loop(0, members // batch, sweep, 0)

    @pl.when(lat_last)
    def _():
        settle(fold.at[pl.ds(0, half - 1), sent], fold_sem.at[1])
        for c in relays:
            c.start()

    def join(lo_parts, mid, hi_parts):
        out = mid[0]
        out = out + shift_down(zero if lo_parts is None else lo_parts[2], mid[2])
        return out + shift_up(mid[1], zero if hi_parts is None else hi_parts[1])

    def bands(outer_tile, edge_tile, inner_tile):
        south_edge = outer_tile < edge_tile
        main_coefs(outer_tile)
        main_coefs(edge_tile)
        for k in range(ITERS):
            def band(g, carry):
                far, mid, near = (
                    member_parts(k, g, t) for t in (outer_tile, edge_tile, inner_tile))
                ordered = (far[1], mid[1], near[1]) if south_edge else (near[1], mid[1], far[1])
                if k + 1 < ITERS:
                    vk[k, g, at(outer_tile), :] = (
                        join(None, far[1], mid[1]) if south_edge else join(mid[1], far[1], None))
                out = join(*ordered)
                vk[k, g, at(edge_tile), :] = out
                x = mid[0]
                w = cen[at(edge_tile - first), :] * x
                macc[2 * k, g] = macc[2 * k, g] + w * x
                macc[2 * k + 1, g] = macc[2 * k + 1, g] + w * out
                return carry
            lax.fori_loop(0, members, band, 0, unroll=members)

    def take_rows(side, tile, seen):
        rs = at(tile)

        def clean(x):
            return jnp.where(seen, x, 0.0)
        for a in range(ARRAYS):
            if a not in (RIM, KRIM):
                st[a, rs, :] = clean(rowin[side, a])

    def take_corners(side, tile, seen):
        def clean(x):
            return jnp.where(seen, x, 0.0)
        o, k = clean(rowin[side, RIM]), clean(rowin[side, KRIM])
        ow, kw = (clean(diagin[2 * side, i]) for i in range(2))
        oe, ke = (roll(clean(diagin[2 * side + 1, i]), 10) for i in range(2))
        put_strip(at(tile), unfold(o, k, ow, kw, oe, ke))

    @pl.when(not_first)
    def _():
        settle(rowin.at[0, :, low], recv_sem.at[UP])
        take_rows(0, first - 1, sub > 4)

    @pl.when(lat_first)
    def _():
        rs = at(first - 1)
        for a in range(ARRAYS):
            st[a, rs, :] = zero
        put_strip(rs, (zero, zero, zero))

    bands(first - 1, first, first + 1)

    @pl.when(not_last)
    def _():
        settle(rowin.at[1, :, high], recv_sem.at[DOWN])
        take_rows(1, last + 1, sub < 3)
        bands(last + 1, last, last - 1)

    settle(packin, recv_sem.at[SIDES])

    def merge(t, carry):
        fw, fe = [packin[0, g, t] for g in range(2)], [packin[1, g, t] for g in range(2)]
        for q in range(4):
            rs = at(first + t * 4 + q)
            for g, ref in enumerate((strips.at[0], kstrip)):
                x = ref[rs, :]
                keep = lane < EXTRA if g else lane >= 0
                x = jnp.where(jnp.logical_and(place < 3, keep),
                              roll(fw[g], (-3 * q) % cols) if q else fw[g], x)
                x = jnp.where(jnp.logical_and(place > 12, keep), roll(fe[g], 10 - 3 * q), x)
                ref[rs, :] = x
        return carry
    lax.fori_loop(0, tiles // 4, merge, 0, unroll=split(tiles // 4, 6))

    def edge_spread(t, carry):
        spread_tile(first + t)
        return carry
    lax.fori_loop(0, tiles - 1, edge_spread, 0, unroll=split(tiles - 1, 23))

    @pl.when(not_first)
    def _():
        settle(diagin.at[pl.ds(0, 2), :, low], recv_sem.at[UP_CORNERS])
        take_corners(0, first - 1, sub > 4)

    @pl.when(not_last)
    def _():
        settle(diagin.at[pl.ds(2, 2), :, high], recv_sem.at[DOWN_CORNERS])
        take_corners(1, last + 1, sub < 3)

    @pl.when(lat_last)
    def _():
        settle(fold.at[pl.ds(0, half), sent], fold_sem.at[2])
        total = lon_count * cols
        rs = at(last + 1)
        shown = jnp.where(place < 8, place - 3, place + (cols - 13))
        origin = lax.rem(partner[0, 0] - lo * cols + total, total)

        def view(shift):
            start = lax.rem(origin + shift + total, total)
            chunk = lax.div(start, cols)
            head = start - chunk * cols
            slots = [lax.rem(chunk + o + 2 * lon_count, lon_count) for o in (1, 0, -1, -2)]
            z = head - shown
            return (slots, jnp.bitwise_and(head - lane, cols - 1), lane <= head,
                    jnp.bitwise_and(z, cols - 1), (z >= cols, z >= 0, z >= -cols))

        def take(x, where):
            return jnp.take_along_axis(x, where, axis=1, mode="promise_in_bounds")
        views = {s: view(s) for s in (-1, 0, 1)}
        shifts = {EAST: -1, NEAST: -1, NWEST: 1}
        ghost = [zero, zero]
        blocks = []
        for i, a in enumerate(fold_arrays):
            slots, where, within, where_s, (far, near, back) = views[shifts.get(a, 0)]
            chunks = [jnp.where(sub < len(fold_picks[a]), fold[s, pl.ds(fold_start[i], 8), :], 0.0) for s in slots]
            block = jnp.where(within, take(chunks[1], where), take(chunks[2], where))
            st[a, rs, :] = block
            blocks.append(block)
            x = jnp.where(back, take(chunks[2], where_s), take(chunks[3], where_s))
            x = jnp.where(near, take(chunks[1], where_s), x)
            x = jnp.where(far, take(chunks[0], where_s), x)
            s, g = (0, a) if a < members else (1, COUPLED.index(a))
            ghost[s] = jnp.where(group == g, x, ghost[s])
            if a == NORTH:
                end = pl.ds(EDGE + rows - 1, 1)
                st[NORTH, end, :] = 0.5 * (st[NORTH, end, :] + block[2:3, :])
                red[0] = x
                st[NEAST, end, :] = jnp.zeros((1, cols), f32)
                st[NWEST, end, :] = jnp.zeros((1, cols), f32)
        o, k = rim(blocks[:members]), rim(blocks[members:])
        ring = unfold(o, k, zero, zero, zero, zero)[1]
        put_strip(rs, (ghost[0], ring, extras(ghost[1], k)))
        end = pl.ds(EDGE + rows - 1, 1)
        mixed = 0.5 * (kstrip[end, :] + red[0, pl.ds(2, 1), :])
        g1, l1 = group[0:1, :], lane[0:1, :]
        dropped = jnp.logical_or(jnp.logical_or(g1 == 2, g1 == 3),
                                 jnp.logical_or(l1 == EXTRA + 1, l1 == EXTRA + 2))
        kstrip[end, :] = jnp.where(dropped, 0.0, jnp.where(g1 == 1, mixed, kstrip[end, :]))
        bands(last + 1, last, last - 1)

    spread_tile(first - 1)
    spread_tile(last)
    spread_tile(last + 1)

    def edge_coefs(t, carry):
        strip_coefs(first - 1 + t)
        return carry
    lax.fori_loop(0, tiles + 2, edge_coefs, 0, unroll=split(tiles + 2, 26))

    for k in range(ITERS):
        _, (cross, upper, lower) = strip_parts(k, first - 1)

        def strip_step(t, carry):
            sofar, u_old, d_old, w_old, acc0, acc1 = carry
            tile = first + t
            x, (cross, upper, lower) = strip_parts(k, tile)
            out = sofar + shift_up(u_old, upper)
            strips[k + 1, at(tile - 1), :] = out
            acc1 = acc1 + w_old * out
            w_old = coefs[8, at(tile), :] * x
            acc0 = acc0 + w_old * x
            return cross + shift_down(d_old, lower), upper, lower, w_old, acc0, acc1
        sofar, u_old, d_old, w_old, acc0, acc1 = lax.fori_loop(
            0, tiles, strip_step,
            (cross + shift_down(zero, lower), upper, lower, zero, zero, zero),
            unroll=split(tiles, 24))
        _, (cross, upper, lower) = strip_parts(k, last + 1)
        out = sofar + shift_up(u_old, upper)
        strips[k + 1, at(last), :] = out
        strips[k + 1, at(last + 1), :] = cross + shift_down(d_old, lower) + shift_up(upper, zero)
        sacc[2 * k] = acc0
        sacc[2 * k + 1] = acc1 + w_old * out

    def column_sum(x):
        for s in (4, 2, 1):
            x = x + roll(x, s, 0)
        return x
    row = zero
    for i in range(2 * ITERS):
        total = macc[i, :, 0, :]
        for s in range(1, 8):
            total = total + macc[i, :, s, :]
        total = jnp.where(jnp.logical_and(lane > 2, lane < cols - 3), total, 0.0)
        total = total + jnp.where(group == sub, column_sum(sacc[i]), 0.0)
        total = jnp.sum(total, axis=1, keepdims=True)
        row = jnp.where(lane == 8 * i + sub, total, row)

    row = column_sum(row)

    def reduce(value, slot, recv, me, count, dev, between):
        red[slot] = value
        mine = pl.ds(me, 1)
        cps = [
            pltpu.make_async_remote_copy(
                src_ref=red.at[slot, pl.ds(0, 1)], dst_ref=recv.at[mine],
                send_sem=red_sem.at[2 * slot], recv_sem=red_sem.at[2 * slot + 1],
                device_id=dev(d), device_id_type=MESH)
            for d in range(1, count)
        ]
        for c in cps:
            c.start()
        recv[mine, :] = value[0:1, :]
        between()
        settle(recv.at[pl.ds(0, count - 1)], red_sem.at[2 * slot + 1])
        out = recv[pl.ds(0, 1), :]
        for d in range(1, count):
            out = out + recv[pl.ds(d, 1), :]
        return jnp.broadcast_to(out, (8, cols))

    outer = jnp.logical_or(lane < 3, lane > cols - 4)

    def close_rims(stages):
        for k in stages:
            def close(t, carry):
                rs = at(first + t)
                x = strips[k, rs, :]
                x = jnp.where(place < 3, roll(x, cols - 10), x)
                for m in range(members):
                    edge = roll(x, (cols - 3 - SLOT * m) % cols)
                    vk[k - 1, m, rs, :] = jnp.where(outer, edge, vk[k - 1, m, rs, :])
                return carry
            lax.fori_loop(0, tiles, close, 0, unroll=split(tiles, 8))

    row = reduce(row, 0, redlon, lo, lon_count,
                 lambda d: (la, lax.rem(lo + d, lon_count)), lambda: close_rims((1, 2)))
    row = reduce(row, 1, redlat, la, lat_count,
                 lambda d: (lax.rem(la + d, lat_count), lo), lambda: close_rims((3,)))

    m0, m1, m2, m3, m4, m5 = (
        jnp.broadcast_to(
            jnp.sum(jnp.where(lane == 8 * i + sub, row, 0.0), axis=1, keepdims=True), (8, cols))
        for i in range(2 * ITERS))
    a0 = m1 / m0
    h1 = m2 - a0 * m1
    a1 = (m3 - 2.0 * a0 * m2 + a0 * a0 * m1) / h1
    b1 = h1 / m0
    p1 = -(a0 + a1)
    p0 = a0 * a1 - b1
    h2 = m4 + p1 * m3 + p0 * m2
    a2 = (m5 + p1 * m4 + p0 * m3) / h2 + p1
    b2 = h2 / h1
    t2 = p1 - a2
    t1 = p0 - a2 * p1 - b2
    t0 = b2 * a0 - a2 * p0
    q3 = 1.0 / (1.0 + t2 + t1 + t0)
    q2, q1, q0 = t2 * q3, t1 * q3, t0 * q3
    for i, value in enumerate((q3 + q2 + q1, q2 + q3, q3, q0, q1, q2, q3)):
        mix[i] = value

    settle(pack, send_sem.at[SIDES])
    settle(redlon.at[pl.ds(0, lon_count - 1)], red_sem.at[0])
    settle(redlat.at[pl.ds(0, lat_count - 1)], red_sem.at[2])

    @pl.when(not_last)
    def _():
        settle(st.at[0, pl.ds(0, 3 * (ARRAYS + 4))], send_sem.at[UP])

    @pl.when(not_first)
    def _():
        settle(st.at[0, pl.ds(0, 3 * (ARRAYS + 4))], send_sem.at[DOWN])

    @pl.when(lat_last)
    def _():
        settle(fold.at[pl.ds(0, 2 * half - 1), sent], fold_sem.at[0])


def finish(st, vk, mix, center, sol_out, res_out, obuf, store_sem):
    members, rows, cols = sol_out.shape

    def one(m, carry):
        s0, s1, s2, q0, q1, q2, q3 = (
            jnp.broadcast_to(mix[i, pl.ds(m, 1), :], (8, cols)) for i in range(7))
        for t in range(rows // 8):
            here, rs = pl.ds(8 * t, 8), pl.ds(EDGE + 8 * t, 8)
            v0, v1, v2, v3 = st[m, rs, :], vk[0, m, rs, :], vk[1, m, rs, :], vk[2, m, rs, :]
            obuf[0, m, here, :] = s0 * v0 + s1 * v1 + s2 * v2
            obuf[1, m, here, :] = center[here, :] * (q0 * v0 + q1 * v1 + q2 * v2 + q3 * v3)
        for o, dst in ((0, sol_out), (1, res_out)):
            pltpu.make_async_copy(obuf.at[o, m], dst.at[m], store_sem.at[0]).start()
        return carry
    lax.fori_loop(0, members, one, 0)
    pltpu.make_async_copy(obuf, obuf, store_sem.at[0]).wait()


def body(lat_count, lon_count, right_side, center, couplings, land_sea, fold_partner):
    members, rows, cols = right_side.shape
    f32 = jnp.float32
    hbm = pl.BlockSpec(memory_space=pltpu.HBM)
    vmem = pl.BlockSpec(memory_space=pltpu.VMEM)
    dma = pltpu.SemaphoreType.DMA
    shape = jax.ShapeDtypeStruct(right_side.shape, f32)
    high = rows + 2 * EDGE
    tiles = rows // 8
    folded = -(-3 * (members + len(COUPLED)) // 8) * 8 + 8
    st, vk, mix, cen = pl.pallas_call(
        functools.partial(kernel, lat_count, lon_count),
        out_shape=(pltpu.VMEM((ARRAYS, high, cols), f32),
                   pltpu.VMEM((ITERS, members, high, cols), f32),
                   pltpu.VMEM((7, 8, cols), f32),
                   pltpu.VMEM((rows, cols), f32)),
        in_specs=[hbm] * 5,
        out_specs=(vmem, vmem, vmem, vmem),
        scratch_shapes=[
            pltpu.VMEM((rows, cols), jnp.int32),
            pltpu.SMEM((1, cols), jnp.int32),
            pltpu.VMEM((ITERS + 1, high, cols), f32),
            pltpu.VMEM((high, cols), f32),
            pltpu.VMEM((high, cols), f32),
            pltpu.VMEM((8, high, cols), f32),
            pltpu.VMEM((9, high, cols), f32),
            pltpu.VMEM((4, high, cols), f32),
            pltpu.VMEM((2, 2, tiles // 4, 8, cols), f32),
            pltpu.VMEM((2, 2, tiles // 4, 8, cols), f32),
            pltpu.VMEM((2, ARRAYS, 8, cols), f32),
            pltpu.VMEM((4, 2, 8, cols), f32),
            pltpu.VMEM((lon_count, folded, cols), f32),
            pltpu.VMEM((2 * ITERS, members, 8, cols), f32),
            pltpu.VMEM((2 * ITERS, 8, cols), f32),
            pltpu.VMEM((2, 8, cols), f32),
            pltpu.VMEM((-(-lon_count // 8) * 8, cols), f32),
            pltpu.VMEM((-(-lat_count // 8) * 8, cols), f32),
            dma((3,)), dma((3,)), dma((5,)), dma((3,)), dma((4,)),
        ],
        compiler_params=pltpu.CompilerParams(
            collective_id=0, has_side_effects=True, vmem_limit_bytes=32 * 1024 * 1024),
    )(*(pltpu.with_memory_space_constraint(x, pltpu.HBM) for x in (
        right_side, center, couplings, land_sea, fold_partner.reshape(lon_count, cols))))
    return pl.pallas_call(
        finish,
        out_shape=(shape, shape),
        in_specs=[vmem] * 4,
        out_specs=(hbm, hbm),
        scratch_shapes=[
            pltpu.VMEM((2, members, rows, cols), f32),
            dma((1,)),
        ],
        compiler_params=pltpu.CompilerParams(vmem_limit_bytes=16 * 1024 * 1024),
    )(st, vk, mix, cen)


def solution(mesh):
    return jax.shard_map(
        functools.partial(body, mesh.shape["lat"], mesh.shape["lon"]),
        mesh=mesh,
        in_specs=(
            P(None, "lat", "lon"),
            P("lat", "lon"),
            P(None, "lat", "lon"),
            P("lat", "lon"),
            P(),
        ),
        out_specs=(P(None, "lat", "lon"), P(None, "lat", "lon")),
        check_vma=False,
    )
```

```python
import functools

import jax
import jax.numpy as jnp
from jax import lax
from jax.experimental import pallas as pl
from jax.experimental.pallas import tpu as pltpu
from jax.sharding import PartitionSpec as P

ITERS = 3
BATCH = 2
MESH = pl.DeviceIdType.MESH
EDGE = 16
SLOT = 16
RIM, KRIM, EAST, NORTH, NEAST, NWEST, SCALE, ARRAYS = range(8, 16)
EXTRA = 5 * SLOT
COUPLED = (EAST, NORTH, NEAST, NWEST, SCALE)
SIDES, UP, DOWN, UP_CORNERS, DOWN_CORNERS, SIDES_K = range(6)


def roll(x, shift, axis=1):
    return pltpu.roll(x, shift, axis)


def kernel(
    lat_count, lon_count,
    rhs, center_hbm, coup_hbm, land_hbm, partner_hbm, st, vk, mix, cen,
    land, partner, strips, kstrip, beyond, coefm, coefs, wide, pack, packin, rowin, diagin, fold,
    macc, sacc, red, spare, redin,
    load_sem, send_sem, recv_sem, fold_sem, red_sem, known,
):
    f32 = jnp.float32
    members, rows, cols = rhs.shape
    tiles = rows // 8
    first, last = 2, tiles + 1
    inner = tiles - 2

    def split(count, most):
        return max(u for u in range(1, most + 1) if count % u == 0)

    la, lo = lax.axis_index("lat"), lax.axis_index("lon")
    lat_first, lat_last = la == 0, la == lat_count - 1
    not_first, not_last = la > 0, la < lat_count - 1
    north, south = lax.rem(la + 1, lat_count), lax.rem(la + lat_count - 1, lat_count)
    east, west = lax.rem(lo + 1, lon_count), lax.rem(lo + lon_count - 1, lon_count)
    lane = lax.broadcasted_iota(jnp.int32, (8, cols), 1)
    sub = lax.broadcasted_iota(jnp.int32, (8, cols), 0)
    place = jnp.bitwise_and(lane, SLOT - 1)
    group = lax.shift_right_logical(lane, 4)
    zero = jnp.zeros((8, cols), f32)

    def at(tile):
        start = tile * 8
        return pl.ds(start if isinstance(start, int) else pl.multiple_of(start, 8), 8)

    loads = []
    for i, (start, size) in enumerate(((0, 8), (rows - 8, 8), (8, rows - 16))):
        rs, own = pl.ds(start, size), pl.ds(EDGE + start, size)
        loads += [
            pltpu.make_async_copy(center_hbm.at[rs], cen.at[rs], load_sem.at[i // 2]),
            pltpu.make_async_copy(land_hbm.at[rs], land.at[rs], load_sem.at[i // 2]),
            pltpu.make_async_copy(coup_hbm.at[:, rs], st.at[pl.ds(EAST, 4), own],
                                  load_sem.at[i // 2]),
            pltpu.make_async_copy(rhs.at[:, rs], st.at[pl.ds(0, members), own],
                                  load_sem.at[i // 2]),
        ]
    loads.append(pltpu.make_async_copy(partner_hbm.at[pl.ds(0, 1)], partner, load_sem.at[2]))
    for c in loads[:8]:
        c.start()
    barrier = pltpu.get_barrier_semaphore()
    partners = [(la, lax.rem(lo + d, lon_count)) for d in range(1, lon_count)]
    partners += [(lax.rem(la + d, lat_count), lo) for d in range(1, lat_count)]
    for p in partners:
        pl.semaphore_signal(barrier, inc=1, device_id=p, device_id_type=MESH)

    @pl.when(not_last)
    def _():
        for p in ((north, east), (north, west)):
            pl.semaphore_signal(barrier, inc=1, device_id=p, device_id_type=MESH)

    @pl.when(not_first)
    def _():
        for p in ((south, east), (south, west)):
            pl.semaphore_signal(barrier, inc=1, device_id=p, device_id_type=MESH)
    arrivals = (len(partners) + 2 * jnp.where(not_last, 1, 0) + 2 * jnp.where(not_first, 1, 0))
    for c in loads[8:]:
        c.start()

    rim_lanes = [jnp.bitwise_and(lane - (SLOT * g - 3), cols - 1) < 12 for g in range(8)]

    def rim(arrays):
        out = zero
        for g, x in enumerate(arrays):
            out = jnp.where(rim_lanes[g], roll(x, g * SLOT + 3), out)
        return out

    def prep_tile(tile):
        rs = at(tile)
        near = at(tile - first)
        d = land[near, :].astype(f32) / cen[near, :]
        st[SCALE, rs, :] = d
        vals = []
        for m in range(members):
            v = st[m, rs, :] * d
            st[m, rs, :] = v
            vals.append(v)
        st[RIM, rs, :] = rim(vals)
        st[KRIM, rs, :] = rim([st[c, rs, :] for c in COUPLED[:4]] + [d])

    def prep(t, carry):
        prep_tile(first + 1 + t)
        return carry

    def fill(t, carry):
        packs = [zero] * 4
        for q in range(4):
            rs = at(first + t * 4 + q)
            here = jnp.logical_and(place >= 3 * q, place < 3 * q + 3)
            after = jnp.logical_and(place >= 3 * q + 3, place < 3 * q + 6)
            for g in range(2):
                x = st[RIM + g, rs, :]
                x = roll(x, 3 * q) if q else x
                packs[g] = jnp.where(here, x, packs[g])
                packs[2 + g] = jnp.where(after, x, packs[2 + g])
        for side in range(2):
            for g in range(2):
                pack[side, g, t] = packs[2 * side + g]
        return carry

    top, bottom = pl.ds(EDGE + rows - 3, 3), pl.ds(EDGE, 3)

    def remote(src, dst, slot, landing, dev):
        return pltpu.make_async_remote_copy(
            src_ref=src, dst_ref=dst, send_sem=send_sem.at[slot], recv_sem=recv_sem.at[landing],
            device_id=dev, device_id_type=MESH)

    def side_copies(g, landing):
        return [remote(pack.at[0, g], packin.at[0, g], SIDES, landing, (la, east)),
                remote(pack.at[1, g], packin.at[1, g], SIDES, landing, (la, west))]
    sides, sides_k = side_copies(0, SIDES), side_copies(1, SIDES_K)
    pair = pl.ds(RIM, 2)
    low, high = pl.ds(5, 3), pl.ds(0, 3)
    up = [remote(st.at[:, top], rowin.at[0, :, low], UP, UP, (north, lo)),
          remote(st.at[pair, top], diagin.at[0, :, low], UP, UP_CORNERS, (north, east)),
          remote(st.at[pair, top], diagin.at[1, :, low], UP, UP_CORNERS, (north, west))]
    down = [remote(st.at[:, bottom], rowin.at[1, :, high], DOWN, DOWN, (south, lo)),
            remote(st.at[pair, bottom], diagin.at[2, :, high], DOWN, DOWN_CORNERS, (south, east)),
            remote(st.at[pair, bottom], diagin.at[3, :, high], DOWN, DOWN_CORNERS, (south, west))]
    fold_arrays = list(range(members)) + list(COUPLED)
    fold_picks = {a: (0, 1, 2) for a in range(members)}
    fold_picks.update({EAST: (0, 1), NORTH: (1, 2, 0), NEAST: (1, 2), NWEST: (1, 2), SCALE: (0, 1)})
    fold_start = [0]
    for a in fold_arrays:
        fold_start.append(fold_start[-1] + len(fold_picks[a]))
    sent = pl.ds(0, fold_start[-1])
    mate = lo + 1 - 2 * lax.rem(lo, 2)
    half = lon_count // 2

    def fold_copy(sender, landing, dev):
        return pltpu.make_async_remote_copy(
            src_ref=fold.at[sender, sent], dst_ref=fold.at[sender, sent],
            send_sem=fold_sem.at[0], recv_sem=fold_sem.at[landing],
            device_id=(la, dev), device_id_type=MESH)
    folds = [fold_copy(lo, 2, mate)]
    folds += [fold_copy(lo, 1, lax.rem(lo + 2 * j, lon_count)) for j in range(1, half)]
    relays = [fold_copy(lax.rem(lo + lon_count - 2 * j, lon_count), 2, mate)
              for j in range(1, half)]

    def settle(ref, sem):
        pltpu.make_async_copy(ref, ref, sem).wait()

    blocks = members + 6
    settle(st.at[pl.ds(0, blocks), pl.ds(0, 16)], load_sem.at[0])
    prep_tile(first)
    prep_tile(last)

    late = lo >= half
    send_first = jnp.logical_and(lat_last, late)

    @pl.when(lat_last)
    def _():
        end = EDGE + rows - 1
        for i, a in enumerate(fold_arrays):
            for g, r in enumerate(fold_picks[a]):
                fold[lo, pl.ds(fold_start[i] + g, 1), :] = st[a, pl.ds(end - r, 1), :]
        for i in range(fold_start[-1], fold.shape[1]):
            fold[lo, pl.ds(i, 1), :] = jnp.zeros((1, cols), f32)

    def send_folds():
        if lat_count > 1:
            for c in down:
                c.start()
        for c in folds[half // 2:] + folds[:half // 2]:
            c.start()

    @pl.when(send_first)
    def _():
        pl.semaphore_wait(barrier, arrivals)
        send_folds()

    settle(st.at[pl.ds(0, blocks), pl.ds(0, rows - 16)], load_sem.at[1])
    loads[-1].wait()
    lax.fori_loop(0, inner, prep, 0, unroll=split(inner, 11))
    lax.fori_loop(0, tiles // 4, fill, 0, unroll=split(tiles // 4, 6))

    @pl.when(jnp.logical_not(send_first))
    def _():
        pl.semaphore_wait(barrier, arrivals)

    send_later = jnp.logical_and(lat_last, jnp.logical_not(late))

    @pl.when(send_later)
    def _():
        if lat_count > 1:
            for c in down:
                c.start()
        for c in folds[::-1]:
            c.start()

    for c in (sides_k[1], sides[1], sides_k[0], sides[0]):
        c.start()
    for d in range(1, lat_count):
        pl.semaphore_signal(known, inc=1, device_id=(lax.rem(la + d, lat_count), lo),
                            device_id_type=MESH)

    @pl.when(not_last)
    def _():
        for c in up:
            c.start()

    @pl.when(jnp.logical_and(not_first, not_last))
    def _():
        for c in down:
            c.start()

    def unfold(o, k, ow, kw, oe, ke):
        def windows(x, w, e):
            x = jnp.where(place < 8, x, roll(x, 10))
            x = jnp.where(place < 3, w, x)
            return jnp.where(place < 13, x, e)
        ring = jnp.where(place == 7, roll(o, cols - 1), jnp.where(place == 8, roll(o, 11), 0.0))
        return windows(o, ow, oe), ring, extras(windows(k, kw, ke), k)

    def extras(x, k):
        x = jnp.where(lane == EXTRA, roll(k, EXTRA + 3), x)
        x = jnp.where(lane == EXTRA + 1, roll(k, EXTRA + 1 - 2 * SLOT + 3), x)
        return jnp.where(lane == EXTRA + 2, roll(k, EXTRA + 2 - 3 * SLOT - 8), x)

    def put_strip(rs, parts_):
        strips[0, rs, :], beyond[rs, :], kstrip[rs, :] = parts_

    def open_rims(t, carry):
        rs = at(first + t)
        put_strip(rs, unfold(st[RIM, rs, :], st[KRIM, rs, :], zero, zero, zero, zero))
        return carry

    def main_coefs(tile):
        rs = at(tile)
        start = tile * 8
        below = pl.ds(start - 1, 8)
        above = pl.ds(start + 1, 8)
        d, dn = st[SCALE, rs, :], st[SCALE, above, :]
        ds_ = st[SCALE, below, :]
        coefm[0, rs, :] = d * st[EAST, rs, :]
        coefm[1, rs, :] = d * roll(st[EAST, rs, :], 1)
        coefm[2, rs, :] = ds_ * st[NORTH, below, :]
        coefm[3, rs, :] = ds_ * st[NEAST, below, :]
        coefm[4, rs, :] = ds_ * st[NWEST, below, :]
        coefm[5, rs, :] = dn * st[NORTH, rs, :]
        coefm[6, rs, :] = dn * roll(st[NWEST, rs, :], cols - 1)
        coefm[7, rs, :] = dn * roll(st[NEAST, rs, :], 1)

    def spread_tile(tile):
        rs = at(tile)
        x = kstrip[rs, :]

        def spread(g, shift=0):
            where = jnp.bitwise_and(place + (g * SLOT + shift), cols - 1)
            if shift < 0:
                where = jnp.where(place == 8, EXTRA + g // 2, where)
            if shift > 0:
                where = jnp.where(place == 7, EXTRA + 2, where)
            return jnp.take_along_axis(x, where, axis=1, mode="promise_in_bounds")
        d = spread(4)
        wide[0, rs, :] = d
        for g in range(1, 4):
            wide[g, rs, :] = spread(g)
        coefs[0, rs, :] = d * spread(0)
        coefs[1, rs, :] = d * spread(0, -1)
        coefs[6, rs, :] = spread(3, 1)
        coefs[7, rs, :] = spread(2, -1)
        edge = jnp.logical_or(jnp.logical_and(place >= 3, place < 6),
                              jnp.logical_and(place >= 10, place < 13))
        used = jnp.logical_and(edge, d > 0.0)
        coefs[8, rs, :] = jnp.where(used, 1.0 / jnp.where(used, d, 1.0), 0.0)

    def strip_coefs(tile):
        rs = at(tile)
        start = tile * 8
        below = pl.ds(start - 1, 8)
        above = pl.ds(start + 1, 8)
        ds_, dn = wide[0, below, :], wide[0, above, :]
        for g in range(1, 4):
            coefs[1 + g, rs, :] = ds_ * wide[g, below, :]
        coefs[5, rs, :] = dn * wide[1, rs, :]
        coefs[6, rs, :] = dn * coefs[6, rs, :]
        coefs[7, rs, :] = dn * coefs[7, rs, :]

    def all_coefs(t, carry):
        main_coefs(first + t)
        return carry
    lax.fori_loop(0, tiles, all_coefs, 0, unroll=split(tiles, 24))
    lax.fori_loop(0, tiles, open_rims, 0, unroll=split(tiles, 24))

    def parts(x, xe, xw, c):
        cross = c[0] * xe + c[1] * xw
        upper = c[2] * x + (c[3] * xe + c[4] * xw)
        lower = c[5] * x + (c[6] * xe + c[7] * xw)
        return cross, upper, lower

    def shift_up(u, u_next):
        return roll(jnp.where(sub == 0, u_next, u), 7, 0)

    def shift_down(d_prev, d):
        return roll(jnp.where(sub == 7, d_prev, d), 1, 0)

    def source(k, g, rs):
        return st[g, rs, :] if k == 0 else vk[k - 1, g, rs, :]

    def strip_parts(k, tile):
        rs = at(tile)
        x = strips[k, rs, :]
        xe, xw = roll(x, cols - 1), roll(x, 1)
        if k == 0:
            near = beyond[rs, :]
            xe, xw = jnp.where(place == 7, near, xe), jnp.where(place == 8, near, xw)
        return x, parts(x, xe, xw, [coefs[q, rs, :] for q in range(8)])

    def member_parts(k, g, tile, c=None):
        rs = at(tile)
        x = source(k, g, rs)
        if c is None:
            c = [coefm[q, rs, :] for q in range(8)]
        return x, parts(x, roll(x, cols - 1), roll(x, 1), c)

    batch = BATCH
    for k in range(ITERS):
        def sweep(p, carry):
            gs = [p * batch + i for i in range(batch)]
            state = []
            for g in gs:
                _, (cross, upper, lower) = member_parts(k, g, first)
                state.append((cross + shift_down(zero, lower), upper, lower, zero, zero, zero))

            def step(t, state):
                state = list(state)
                tile = first + 1 + t
                c = [coefm[q, at(tile), :] for q in range(8)]
                weight = cen[at(tile - first), :]
                for i, g in enumerate(gs):
                    sofar, u_old, d_old, w_old, acc0, acc1 = state[i]
                    x, (cross, upper, lower) = member_parts(k, g, tile, c)
                    out = sofar + shift_up(u_old, upper)
                    vk[k, g, at(tile - 1), :] = out
                    acc1 = acc1 + w_old * out
                    w = weight * x
                    acc0 = acc0 + w * x
                    state[i] = (cross + shift_down(d_old, lower), upper, lower, w, acc0, acc1)
                return tuple(state)
            state = lax.fori_loop(0, inner, step, tuple(state), unroll=split(inner, 22))
            for i, g in enumerate(gs):
                sofar, u_old, d_old, w_old, acc0, acc1 = state[i]
                _, (cross, upper, lower) = member_parts(k, g, last)
                out = sofar + shift_up(u_old, upper)
                vk[k, g, at(last - 1), :] = out
                vk[k, g, at(last), :] = cross + shift_down(d_old, lower) + shift_up(upper, zero)
                macc[2 * k, g] = acc0
                macc[2 * k + 1, g] = acc1 + w_old * out
            return carry
        lax.fori_loop(0, members // batch, sweep, 0)

    @pl.when(lat_last)
    def _():
        settle(fold.at[pl.ds(0, half - 1), sent], fold_sem.at[1])
        for c in relays:
            c.start()

    def join(lo_parts, mid, hi_parts):
        out = mid[0]
        out = out + shift_down(zero if lo_parts is None else lo_parts[2], mid[2])
        return out + shift_up(mid[1], zero if hi_parts is None else hi_parts[1])

    def bands(outer_tile, edge_tile, inner_tile):
        south_edge = outer_tile < edge_tile
        main_coefs(outer_tile)
        main_coefs(edge_tile)
        for k in range(ITERS):
            def band(g, carry):
                far, mid, near = (
                    member_parts(k, g, t) for t in (outer_tile, edge_tile, inner_tile))
                ordered = (far[1], mid[1], near[1]) if south_edge else (near[1], mid[1], far[1])
                if k + 1 < ITERS:
                    vk[k, g, at(outer_tile), :] = (
                        join(None, far[1], mid[1]) if south_edge else join(mid[1], far[1], None))
                out = join(*ordered)
                vk[k, g, at(edge_tile), :] = out
                x = mid[0]
                w = cen[at(edge_tile - first), :] * x
                macc[2 * k, g] = macc[2 * k, g] + w * x
                macc[2 * k + 1, g] = macc[2 * k + 1, g] + w * out
                return carry
            lax.fori_loop(0, members, band, 0, unroll=members)

    def take_rows(side, tile, seen):
        rs = at(tile)

        def clean(x):
            return jnp.where(seen, x, 0.0)
        for a in range(ARRAYS):
            if a not in (RIM, KRIM):
                st[a, rs, :] = clean(rowin[side, a])

    def take_corners(side, tile, seen):
        def clean(x):
            return jnp.where(seen, x, 0.0)
        o, k = clean(rowin[side, RIM]), clean(rowin[side, KRIM])
        ow, kw = (clean(diagin[2 * side, i]) for i in range(2))
        oe, ke = (roll(clean(diagin[2 * side + 1, i]), 10) for i in range(2))
        put_strip(at(tile), unfold(o, k, ow, kw, oe, ke))

    @pl.when(not_first)
    def _():
        settle(rowin.at[0, :, low], recv_sem.at[UP])
        take_rows(0, first - 1, sub > 4)

    @pl.when(lat_first)
    def _():
        rs = at(first - 1)
        for a in range(ARRAYS):
            st[a, rs, :] = zero
        put_strip(rs, (zero, zero, zero))

    bands(first - 1, first, first + 1)

    @pl.when(not_last)
    def _():
        settle(rowin.at[1, :, high], recv_sem.at[DOWN])
        take_rows(1, last + 1, sub < 3)
        bands(last + 1, last, last - 1)

    def merge(g, ref):
        def step(t, carry):
            fw, fe = packin[0, g, t], packin[1, g, t]
            for q in range(4):
                rs = at(first + t * 4 + q)
                x = ref[rs, :]
                keep = lane < EXTRA if g else lane >= 0
                x = jnp.where(jnp.logical_and(place < 3, keep),
                              roll(fw, (-3 * q) % cols) if q else fw, x)
                ref[rs, :] = jnp.where(jnp.logical_and(place > 12, keep), roll(fe, 10 - 3 * q), x)
            return carry
        lax.fori_loop(0, tiles // 4, step, 0, unroll=split(tiles // 4, 6))
    settle(packin.at[:, 1], recv_sem.at[SIDES_K])
    merge(1, kstrip)

    def edge_spread(t, carry):
        spread_tile(first + t)
        return carry
    lax.fori_loop(0, tiles - 1, edge_spread, 0, unroll=split(tiles - 1, 23))

    settle(packin.at[:, 0], recv_sem.at[SIDES])
    merge(0, strips.at[0])

    @pl.when(not_first)
    def _():
        settle(diagin.at[pl.ds(0, 2), :, low], recv_sem.at[UP_CORNERS])
        take_corners(0, first - 1, sub > 4)

    @pl.when(not_last)
    def _():
        settle(diagin.at[pl.ds(2, 2), :, high], recv_sem.at[DOWN_CORNERS])
        take_corners(1, last + 1, sub < 3)

    @pl.when(lat_last)
    def _():
        settle(fold.at[pl.ds(0, half), sent], fold_sem.at[2])
        total = lon_count * cols
        rs = at(last + 1)
        shown = jnp.where(place < 8, place - 3, place + (cols - 13))
        origin = lax.rem(partner[0, 0] - lo * cols + total, total)

        def view(shift):
            start = lax.rem(origin + shift + total, total)
            chunk = lax.div(start, cols)
            head = start - chunk * cols
            slots = [lax.rem(chunk + o + 2 * lon_count, lon_count) for o in (1, 0, -1, -2)]
            z = head - shown
            return (slots, jnp.bitwise_and(head - lane, cols - 1), lane <= head,
                    jnp.bitwise_and(z, cols - 1), (z >= cols, z >= 0, z >= -cols))

        def take(x, where):
            return jnp.take_along_axis(x, where, axis=1, mode="promise_in_bounds")
        views = {s: view(s) for s in (-1, 0, 1)}
        shifts = {EAST: -1, NEAST: -1, NWEST: 1}
        ghost = [zero, zero]
        blocks = []
        for i, a in enumerate(fold_arrays):
            slots, where, within, where_s, (far, near, back) = views[shifts.get(a, 0)]
            chunks = [jnp.where(sub < len(fold_picks[a]), fold[s, pl.ds(fold_start[i], 8), :], 0.0) for s in slots]
            block = jnp.where(within, take(chunks[1], where), take(chunks[2], where))
            st[a, rs, :] = block
            blocks.append(block)
            x = jnp.where(back, take(chunks[2], where_s), take(chunks[3], where_s))
            x = jnp.where(near, take(chunks[1], where_s), x)
            x = jnp.where(far, take(chunks[0], where_s), x)
            s, g = (0, a) if a < members else (1, COUPLED.index(a))
            ghost[s] = jnp.where(group == g, x, ghost[s])
            if a == NORTH:
                end = pl.ds(EDGE + rows - 1, 1)
                st[NORTH, end, :] = 0.5 * (st[NORTH, end, :] + block[2:3, :])
                spare[...] = x
                st[NEAST, end, :] = jnp.zeros((1, cols), f32)
                st[NWEST, end, :] = jnp.zeros((1, cols), f32)
        o, k = rim(blocks[:members]), rim(blocks[members:])
        ring = unfold(o, k, zero, zero, zero, zero)[1]
        put_strip(rs, (ghost[0], ring, extras(ghost[1], k)))
        end = pl.ds(EDGE + rows - 1, 1)
        mixed = 0.5 * (kstrip[end, :] + spare[pl.ds(2, 1), :])
        g1, l1 = group[0:1, :], lane[0:1, :]
        dropped = jnp.logical_or(jnp.logical_or(g1 == 2, g1 == 3),
                                 jnp.logical_or(l1 == EXTRA + 1, l1 == EXTRA + 2))
        kstrip[end, :] = jnp.where(dropped, 0.0, jnp.where(g1 == 1, mixed, kstrip[end, :]))
        bands(last + 1, last, last - 1)

    spread_tile(first - 1)
    spread_tile(last)
    spread_tile(last + 1)

    def edge_coefs(t, carry):
        strip_coefs(first - 1 + t)
        return carry
    lax.fori_loop(0, tiles + 2, edge_coefs, 0, unroll=split(tiles + 2, 26))

    for k in range(ITERS):
        _, (cross, upper, lower) = strip_parts(k, first - 1)

        def strip_step(t, carry):
            sofar, u_old, d_old, w_old, acc0, acc1 = carry
            tile = first + t
            x, (cross, upper, lower) = strip_parts(k, tile)
            out = sofar + shift_up(u_old, upper)
            strips[k + 1, at(tile - 1), :] = out
            acc1 = acc1 + w_old * out
            w_old = coefs[8, at(tile), :] * x
            acc0 = acc0 + w_old * x
            return cross + shift_down(d_old, lower), upper, lower, w_old, acc0, acc1
        sofar, u_old, d_old, w_old, acc0, acc1 = lax.fori_loop(
            0, tiles, strip_step,
            (cross + shift_down(zero, lower), upper, lower, zero, zero, zero),
            unroll=split(tiles, 24))
        _, (cross, upper, lower) = strip_parts(k, last + 1)
        out = sofar + shift_up(u_old, upper)
        strips[k + 1, at(last), :] = out
        strips[k + 1, at(last + 1), :] = cross + shift_down(d_old, lower) + shift_up(upper, zero)
        sacc[2 * k] = acc0
        sacc[2 * k + 1] = acc1 + w_old * out

    def column_sum(x):
        for s in (4, 2, 1):
            x = x + roll(x, s, 0)
        return x
    row = zero
    for i in range(2 * ITERS):
        total = macc[i, :, 0, :]
        for s in range(1, 8):
            total = total + macc[i, :, s, :]
        total = jnp.where(jnp.logical_and(lane > 2, lane < cols - 3), total, 0.0)
        total = total + jnp.where(group == sub, column_sum(sacc[i]), 0.0)
        total = jnp.sum(total, axis=1, keepdims=True)
        row = jnp.where(lane == 8 * i + sub, total, row)

    row = column_sum(row)

    outer = jnp.logical_or(lane < 3, lane > cols - 4)

    def close_rims(stages):
        for k in stages:
            def close(t, carry):
                rs = at(first + t)
                x = strips[k, rs, :]
                x = jnp.where(place < 3, roll(x, cols - 10), x)
                for m in range(members):
                    edge = roll(x, (cols - 3 - SLOT * m) % cols)
                    vk[k - 1, m, rs, :] = jnp.where(outer, edge, vk[k - 1, m, rs, :])
                return carry
            lax.fori_loop(0, tiles, close, 0, unroll=split(tiles, 8))

    everyone = lat_count * lon_count
    spots = [(i, j) for i in range(lat_count) for j in range(lon_count) if i or j]
    mine = pl.ds(la * lon_count + lo, 1)
    red[...] = row
    redin[mine, :] = row[0:1, :]
    pl.semaphore_wait(known, lat_count - 1)
    for i, j in reversed(spots):
        pltpu.make_async_remote_copy(
            src_ref=red.at[pl.ds(0, 1)], dst_ref=redin.at[mine],
            send_sem=red_sem.at[0], recv_sem=red_sem.at[1],
            device_id=(lax.rem(la + i, lat_count), lax.rem(lo + j, lon_count)),
            device_id_type=MESH).start()
    close_rims(range(1, ITERS + 1))
    settle(redin.at[pl.ds(0, everyone - 1)], red_sem.at[1])
    row = zero
    for i in range(-(-everyone // 8)):
        tile = redin[pl.ds(8 * i, 8), :]
        row = row + (tile if 8 * i + 8 <= everyone else jnp.where(sub < everyone - 8 * i, tile, 0.0))
    row = column_sum(row)

    m0, m1, m2, m3, m4, m5 = (
        jnp.broadcast_to(
            jnp.sum(jnp.where(lane == 8 * i + sub, row, 0.0), axis=1, keepdims=True), (8, cols))
        for i in range(2 * ITERS))
    a0 = m1 / m0
    h1 = m2 - a0 * m1
    a1 = (m3 - 2.0 * a0 * m2 + a0 * a0 * m1) / h1
    b1 = h1 / m0
    p1 = -(a0 + a1)
    p0 = a0 * a1 - b1
    h2 = m4 + p1 * m3 + p0 * m2
    a2 = (m5 + p1 * m4 + p0 * m3) / h2 + p1
    b2 = h2 / h1
    t2 = p1 - a2
    t1 = p0 - a2 * p1 - b2
    t0 = b2 * a0 - a2 * p0
    q3 = 1.0 / (1.0 + t2 + t1 + t0)
    q2, q1, q0 = t2 * q3, t1 * q3, t0 * q3
    for i, value in enumerate((q3 + q2 + q1, q2 + q3, q3, q0, q1, q2, q3)):
        mix[i] = value

    settle(pack, send_sem.at[SIDES])
    settle(redin.at[pl.ds(0, everyone - 1)], red_sem.at[0])

    @pl.when(not_last)
    def _():
        settle(st.at[0, pl.ds(0, 3 * (ARRAYS + 4))], send_sem.at[UP])

    @pl.when(not_first)
    def _():
        settle(st.at[0, pl.ds(0, 3 * (ARRAYS + 4))], send_sem.at[DOWN])

    @pl.when(lat_last)
    def _():
        settle(fold.at[pl.ds(0, 2 * half - 1), sent], fold_sem.at[0])


def finish(st, vk, mix, center, sol_out, res_out, obuf, store_sem):
    members, rows, cols = sol_out.shape

    def one(m, carry):
        s0, s1, s2, q0, q1, q2, q3 = (
            jnp.broadcast_to(mix[i, pl.ds(m, 1), :], (8, cols)) for i in range(7))
        for t in range(rows // 8):
            here, rs = pl.ds(8 * t, 8), pl.ds(EDGE + 8 * t, 8)
            v0, v1, v2, v3 = st[m, rs, :], vk[0, m, rs, :], vk[1, m, rs, :], vk[2, m, rs, :]
            obuf[0, m, here, :] = s0 * v0 + s1 * v1 + s2 * v2
            obuf[1, m, here, :] = center[here, :] * (q0 * v0 + q1 * v1 + q2 * v2 + q3 * v3)
        for o, dst in ((0, sol_out), (1, res_out)):
            pltpu.make_async_copy(obuf.at[o, m], dst.at[m], store_sem.at[0]).start()
        return carry
    lax.fori_loop(0, members, one, 0)
    pltpu.make_async_copy(obuf, obuf, store_sem.at[0]).wait()


def body(lat_count, lon_count, right_side, center, couplings, land_sea, fold_partner):
    members, rows, cols = right_side.shape
    f32 = jnp.float32
    hbm = pl.BlockSpec(memory_space=pltpu.HBM)
    vmem = pl.BlockSpec(memory_space=pltpu.VMEM)
    dma = pltpu.SemaphoreType.DMA
    shape = jax.ShapeDtypeStruct(right_side.shape, f32)
    high = rows + 2 * EDGE
    tiles = rows // 8
    folded = -(-3 * (members + len(COUPLED)) // 8) * 8 + 8
    st, vk, mix, cen = pl.pallas_call(
        functools.partial(kernel, lat_count, lon_count),
        out_shape=(pltpu.VMEM((ARRAYS, high, cols), f32),
                   pltpu.VMEM((ITERS, members, high, cols), f32),
                   pltpu.VMEM((7, 8, cols), f32),
                   pltpu.VMEM((rows, cols), f32)),
        in_specs=[hbm] * 5,
        out_specs=(vmem, vmem, vmem, vmem),
        scratch_shapes=[
            pltpu.VMEM((rows, cols), jnp.int32),
            pltpu.SMEM((1, cols), jnp.int32),
            pltpu.VMEM((ITERS + 1, high, cols), f32),
            pltpu.VMEM((high, cols), f32),
            pltpu.VMEM((high, cols), f32),
            pltpu.VMEM((8, high, cols), f32),
            pltpu.VMEM((9, high, cols), f32),
            pltpu.VMEM((4, high, cols), f32),
            pltpu.VMEM((2, 2, tiles // 4, 8, cols), f32),
            pltpu.VMEM((2, 2, tiles // 4, 8, cols), f32),
            pltpu.VMEM((2, ARRAYS, 8, cols), f32),
            pltpu.VMEM((4, 2, 8, cols), f32),
            pltpu.VMEM((lon_count, folded, cols), f32),
            pltpu.VMEM((2 * ITERS, members, 8, cols), f32),
            pltpu.VMEM((2 * ITERS, 8, cols), f32),
            pltpu.VMEM((8, cols), f32),
            pltpu.VMEM((8, cols), f32),
            pltpu.VMEM((-(-lat_count * lon_count // 8) * 8, cols), f32),
            dma((3,)), dma((3,)), dma((6,)), dma((3,)), dma((2,)),
            pltpu.SemaphoreType.REGULAR,
        ],
        compiler_params=pltpu.CompilerParams(
            collective_id=0, has_side_effects=True, vmem_limit_bytes=32 * 1024 * 1024),
    )(*(pltpu.with_memory_space_constraint(x, pltpu.HBM) for x in (
        right_side, center, couplings, land_sea, fold_partner.reshape(lon_count, cols))))
    return pl.pallas_call(
        finish,
        out_shape=(shape, shape),
        in_specs=[vmem] * 4,
        out_specs=(hbm, hbm),
        scratch_shapes=[
            pltpu.VMEM((2, members, rows, cols), f32),
            dma((1,)),
        ],
        compiler_params=pltpu.CompilerParams(vmem_limit_bytes=16 * 1024 * 1024),
    )(st, vk, mix, cen)


def solution(mesh):
    return jax.shard_map(
        functools.partial(body, mesh.shape["lat"], mesh.shape["lon"]),
        mesh=mesh,
        in_specs=(
            P(None, "lat", "lon"),
            P("lat", "lon"),
            P(None, "lat", "lon"),
            P("lat", "lon"),
            P(),
        ),
        out_specs=(P(None, "lat", "lon"), P(None, "lat", "lon")),
        check_vma=False,
    )
```

```python
import functools

import jax
import jax.numpy as jnp
from jax import lax
from jax.experimental import pallas as pl
from jax.experimental.pallas import tpu as pltpu
from jax.sharding import PartitionSpec as P

ITERS = 3
BATCH = 2
MESH = pl.DeviceIdType.MESH
EDGE = 16
SLOT = 16
RIM, KRIM, EAST, NORTH, NEAST, NWEST, SCALE, ARRAYS = range(8, 16)
EXTRA = 5 * SLOT
COUPLED = (EAST, NORTH, NEAST, NWEST, SCALE)
SIDES, UP, DOWN, UP_CORNERS, DOWN_CORNERS, SIDES_K = range(6)


def roll(x, shift, axis=1):
    return pltpu.roll(x, shift, axis)


def kernel(
    lat_count, lon_count,
    rhs, center_hbm, coup_hbm, land_hbm, partner_hbm, st, vk, mix, cen,
    land, partner, strips, kstrip, beyond, coefm, coefs, wide, pack, packin, loose, rowin, diagin, fold,
    macc, sacc, red, spare, redin,
    load_sem, send_sem, recv_sem, fold_sem, red_sem, known,
):
    f32 = jnp.float32
    members, rows, cols = rhs.shape
    tiles = rows // 8
    first, last = 2, tiles + 1
    inner = tiles - 2

    def split(count, most):
        return max(u for u in range(1, most + 1) if count % u == 0)

    la, lo = lax.axis_index("lat"), lax.axis_index("lon")
    lat_first, lat_last = la == 0, la == lat_count - 1
    not_first, not_last = la > 0, la < lat_count - 1
    north, south = lax.rem(la + 1, lat_count), lax.rem(la + lat_count - 1, lat_count)
    east, west = lax.rem(lo + 1, lon_count), lax.rem(lo + lon_count - 1, lon_count)
    lane = lax.broadcasted_iota(jnp.int32, (8, cols), 1)
    sub = lax.broadcasted_iota(jnp.int32, (8, cols), 0)
    place = jnp.bitwise_and(lane, SLOT - 1)
    group = lax.shift_right_logical(lane, 4)
    zero = jnp.zeros((8, cols), f32)

    def at(tile):
        start = tile * 8
        return pl.ds(start if isinstance(start, int) else pl.multiple_of(start, 8), 8)

    loads = []
    for i, (start, size) in enumerate(((0, 8), (rows - 8, 8), (8, rows - 16))):
        rs, own = pl.ds(start, size), pl.ds(EDGE + start, size)
        loads += [
            pltpu.make_async_copy(center_hbm.at[rs], cen.at[rs], load_sem.at[i // 2]),
            pltpu.make_async_copy(land_hbm.at[rs], land.at[rs], load_sem.at[i // 2]),
            pltpu.make_async_copy(coup_hbm.at[:, rs], st.at[pl.ds(EAST, 4), own],
                                  load_sem.at[i // 2]),
            pltpu.make_async_copy(rhs.at[:, rs], st.at[pl.ds(0, members), own],
                                  load_sem.at[i // 2]),
        ]
    loads.append(pltpu.make_async_copy(partner_hbm.at[pl.ds(0, 1)], partner, load_sem.at[2]))
    for c in loads[:8]:
        c.start()
    barrier = pltpu.get_barrier_semaphore()
    partners = [(la, lax.rem(lo + d, lon_count)) for d in range(1, lon_count)]
    partners += [(lax.rem(la + d, lat_count), lo) for d in range(1, lat_count)]
    for p in partners:
        pl.semaphore_signal(barrier, inc=1, device_id=p, device_id_type=MESH)

    @pl.when(not_last)
    def _():
        for p in ((north, east), (north, west)):
            pl.semaphore_signal(barrier, inc=1, device_id=p, device_id_type=MESH)

    @pl.when(not_first)
    def _():
        for p in ((south, east), (south, west)):
            pl.semaphore_signal(barrier, inc=1, device_id=p, device_id_type=MESH)
    arrivals = (len(partners) + 2 * jnp.where(not_last, 1, 0) + 2 * jnp.where(not_first, 1, 0))
    for c in loads[8:]:
        c.start()

    rim_lanes = [jnp.bitwise_and(lane - (SLOT * g - 3), cols - 1) < 12 for g in range(8)]

    def rim(arrays):
        out = zero
        for g, x in enumerate(arrays):
            out = jnp.where(rim_lanes[g], roll(x, g * SLOT + 3), out)
        return out

    def prep_tile(tile):
        rs = at(tile)
        near = at(tile - first)
        d = land[near, :].astype(f32) / cen[near, :]
        st[SCALE, rs, :] = d
        vals = []
        for m in range(members):
            v = st[m, rs, :] * d
            st[m, rs, :] = v
            vals.append(v)
        st[RIM, rs, :] = rim(vals)
        st[KRIM, rs, :] = rim([st[c, rs, :] for c in COUPLED[:4]] + [d])

    def prep(t, carry):
        prep_tile(first + 1 + t)
        return carry

    def fill(t, carry):
        packs = [zero] * 4
        for q in range(4):
            rs = at(first + t * 4 + q)
            here = jnp.logical_and(place >= 3 * q, place < 3 * q + 3)
            after = jnp.logical_and(place >= 3 * q + 3, place < 3 * q + 6)
            for g in range(2):
                x = st[RIM + g, rs, :]
                x = roll(x, 3 * q) if q else x
                packs[g] = jnp.where(here, x, packs[g])
                packs[2 + g] = jnp.where(after, x, packs[2 + g])
        for side in range(2):
            pack[side, 0, t] = packs[2 * side]
            loose[side, t] = packs[2 * side + 1]
        return carry

    packed = tiles // 4
    dense = packed % 3 == 0
    dense_count = packed // 3 * 2 if dense else packed
    used = len(COUPLED) * SLOT

    def squeeze(side):
        if not dense:
            for t in range(packed):
                pack[side, 1, t] = loose[side, t]
            return
        for h in range(packed // 3):
            a, b, c = (loose[side, 3 * h + i] for i in range(3))
            pack[side, 1, 2 * h] = jnp.where(lane < used, a, roll(b, used))
            pack[side, 1, 2 * h + 1] = jnp.where(lane < used, c, roll(b, 2 * SLOT))

    def unsqueeze(side):
        if not dense:
            for t in range(packed):
                loose[side, t] = packin[side, 1, t]
            return
        for h in range(packed // 3):
            x, y = packin[side, 1, 2 * h], packin[side, 1, 2 * h + 1]
            loose[side, 3 * h] = x
            loose[side, 3 * h + 1] = jnp.where(
                lane < 3 * SLOT, roll(x, cols - used), roll(y, cols - 2 * SLOT))
            loose[side, 3 * h + 2] = y

    top, bottom = pl.ds(EDGE + rows - 3, 3), pl.ds(EDGE, 3)

    def remote(src, dst, slot, landing, dev):
        return pltpu.make_async_remote_copy(
            src_ref=src, dst_ref=dst, send_sem=send_sem.at[slot], recv_sem=recv_sem.at[landing],
            device_id=dev, device_id_type=MESH)

    def side_copies(g, landing):
        part = pl.ds(0, dense_count if g else packed)
        return [remote(pack.at[i, g, part], packin.at[i, g, part], SIDES, landing, (la, dev))
                for i, dev in enumerate((east, west))]
    sides, sides_k = side_copies(0, SIDES), side_copies(1, SIDES_K)
    pair = pl.ds(RIM, 2)
    low, high = pl.ds(5, 3), pl.ds(0, 3)
    up = [remote(st.at[:, top], rowin.at[0, :, low], UP, UP, (north, lo)),
          remote(st.at[pair, top], diagin.at[0, :, low], UP, UP_CORNERS, (north, east)),
          remote(st.at[pair, top], diagin.at[1, :, low], UP, UP_CORNERS, (north, west))]
    down = [remote(st.at[:, bottom], rowin.at[1, :, high], DOWN, DOWN, (south, lo)),
            remote(st.at[pair, bottom], diagin.at[2, :, high], DOWN, DOWN_CORNERS, (south, east)),
            remote(st.at[pair, bottom], diagin.at[3, :, high], DOWN, DOWN_CORNERS, (south, west))]
    fold_arrays = list(range(members)) + list(COUPLED)
    fold_picks = {a: (0, 1, 2) for a in range(members)}
    fold_picks.update({EAST: (0, 1), NORTH: (1, 2, 0), NEAST: (1, 2), NWEST: (1, 2), SCALE: (0, 1)})
    fold_start = [0]
    for a in fold_arrays:
        fold_start.append(fold_start[-1] + len(fold_picks[a]))
    sent = pl.ds(0, fold_start[-1])
    mate = lo + 1 - 2 * lax.rem(lo, 2)
    half = lon_count // 2

    def fold_copy(sender, landing, dev):
        return pltpu.make_async_remote_copy(
            src_ref=fold.at[sender, sent], dst_ref=fold.at[sender, sent],
            send_sem=fold_sem.at[0], recv_sem=fold_sem.at[landing],
            device_id=(la, dev), device_id_type=MESH)
    folds = [fold_copy(lo, 2, mate)]
    folds += [fold_copy(lo, 1, lax.rem(lo + 2 * j, lon_count)) for j in range(1, half)]
    relays = [fold_copy(lax.rem(lo + lon_count - 2 * j, lon_count), 2, mate)
              for j in range(1, half)]

    def settle(ref, sem):
        pltpu.make_async_copy(ref, ref, sem).wait()

    blocks = members + 6
    settle(st.at[pl.ds(0, blocks), pl.ds(0, 16)], load_sem.at[0])
    prep_tile(first)
    prep_tile(last)

    late = lo >= half
    send_first = jnp.logical_and(lat_last, late)

    @pl.when(lat_last)
    def _():
        end = EDGE + rows - 1
        for i, a in enumerate(fold_arrays):
            for g, r in enumerate(fold_picks[a]):
                fold[lo, pl.ds(fold_start[i] + g, 1), :] = st[a, pl.ds(end - r, 1), :]
        for i in range(fold_start[-1], fold.shape[1]):
            fold[lo, pl.ds(i, 1), :] = jnp.zeros((1, cols), f32)

    def send_folds():
        if lat_count > 1:
            for c in down:
                c.start()
        for c in folds[half // 2:] + folds[:half // 2]:
            c.start()

    @pl.when(send_first)
    def _():
        pl.semaphore_wait(barrier, arrivals)
        send_folds()

    settle(st.at[pl.ds(0, blocks), pl.ds(0, rows - 16)], load_sem.at[1])
    loads[-1].wait()
    lax.fori_loop(0, inner, prep, 0, unroll=split(inner, 11))
    lax.fori_loop(0, tiles // 4, fill, 0, unroll=split(tiles // 4, 6))
    for side in range(2):
        squeeze(side)

    @pl.when(jnp.logical_not(send_first))
    def _():
        pl.semaphore_wait(barrier, arrivals)

    send_later = jnp.logical_and(lat_last, jnp.logical_not(late))

    @pl.when(send_later)
    def _():
        if lat_count > 1:
            for c in down:
                c.start()
        for c in folds[::-1]:
            c.start()

    for c in (sides_k[1], sides[1], sides_k[0], sides[0]):
        c.start()
    for d in range(1, lat_count):
        pl.semaphore_signal(known, inc=1, device_id=(lax.rem(la + d, lat_count), lo),
                            device_id_type=MESH)

    @pl.when(not_last)
    def _():
        for c in up:
            c.start()

    @pl.when(jnp.logical_and(not_first, not_last))
    def _():
        for c in down:
            c.start()

    def unfold(o, k, ow, kw, oe, ke):
        def windows(x, w, e):
            x = jnp.where(place < 8, x, roll(x, 10))
            x = jnp.where(place < 3, w, x)
            return jnp.where(place < 13, x, e)
        ring = jnp.where(place == 7, roll(o, cols - 1), jnp.where(place == 8, roll(o, 11), 0.0))
        return windows(o, ow, oe), ring, extras(windows(k, kw, ke), k)

    def extras(x, k):
        x = jnp.where(lane == EXTRA, roll(k, EXTRA + 3), x)
        x = jnp.where(lane == EXTRA + 1, roll(k, EXTRA + 1 - 2 * SLOT + 3), x)
        return jnp.where(lane == EXTRA + 2, roll(k, EXTRA + 2 - 3 * SLOT - 8), x)

    def put_strip(rs, parts_):
        strips[0, rs, :], beyond[rs, :], kstrip[rs, :] = parts_

    def open_rims(t, carry):
        rs = at(first + t)
        put_strip(rs, unfold(st[RIM, rs, :], st[KRIM, rs, :], zero, zero, zero, zero))
        return carry

    def main_coefs(tile):
        rs = at(tile)
        start = tile * 8
        below = pl.ds(start - 1, 8)
        above = pl.ds(start + 1, 8)
        d, dn = st[SCALE, rs, :], st[SCALE, above, :]
        ds_ = st[SCALE, below, :]
        coefm[0, rs, :] = d * st[EAST, rs, :]
        coefm[1, rs, :] = d * roll(st[EAST, rs, :], 1)
        coefm[2, rs, :] = ds_ * st[NORTH, below, :]
        coefm[3, rs, :] = ds_ * st[NEAST, below, :]
        coefm[4, rs, :] = ds_ * st[NWEST, below, :]
        coefm[5, rs, :] = dn * st[NORTH, rs, :]
        coefm[6, rs, :] = dn * roll(st[NWEST, rs, :], cols - 1)
        coefm[7, rs, :] = dn * roll(st[NEAST, rs, :], 1)

    def spread_tile(tile):
        rs = at(tile)
        x = kstrip[rs, :]

        def spread(g, shift=0):
            where = jnp.bitwise_and(place + (g * SLOT + shift), cols - 1)
            if shift < 0:
                where = jnp.where(place == 8, EXTRA + g // 2, where)
            if shift > 0:
                where = jnp.where(place == 7, EXTRA + 2, where)
            return jnp.take_along_axis(x, where, axis=1, mode="promise_in_bounds")
        d = spread(4)
        wide[0, rs, :] = d
        for g in range(1, 4):
            wide[g, rs, :] = spread(g)
        coefs[0, rs, :] = d * spread(0)
        coefs[1, rs, :] = d * spread(0, -1)
        coefs[6, rs, :] = spread(3, 1)
        coefs[7, rs, :] = spread(2, -1)
        edge = jnp.logical_or(jnp.logical_and(place >= 3, place < 6),
                              jnp.logical_and(place >= 10, place < 13))
        used = jnp.logical_and(edge, d > 0.0)
        coefs[8, rs, :] = jnp.where(used, 1.0 / jnp.where(used, d, 1.0), 0.0)

    def strip_coefs(tile):
        rs = at(tile)
        start = tile * 8
        below = pl.ds(start - 1, 8)
        above = pl.ds(start + 1, 8)
        ds_, dn = wide[0, below, :], wide[0, above, :]
        for g in range(1, 4):
            coefs[1 + g, rs, :] = ds_ * wide[g, below, :]
        coefs[5, rs, :] = dn * wide[1, rs, :]
        coefs[6, rs, :] = dn * coefs[6, rs, :]
        coefs[7, rs, :] = dn * coefs[7, rs, :]

    def all_coefs(t, carry):
        main_coefs(first + t)
        return carry
    lax.fori_loop(0, tiles, all_coefs, 0, unroll=split(tiles, 24))
    lax.fori_loop(0, tiles, open_rims, 0, unroll=split(tiles, 24))

    def parts(x, xe, xw, c):
        cross = c[0] * xe + c[1] * xw
        upper = c[2] * x + (c[3] * xe + c[4] * xw)
        lower = c[5] * x + (c[6] * xe + c[7] * xw)
        return cross, upper, lower

    def shift_up(u, u_next):
        return roll(jnp.where(sub == 0, u_next, u), 7, 0)

    def shift_down(d_prev, d):
        return roll(jnp.where(sub == 7, d_prev, d), 1, 0)

    def source(k, g, rs):
        return st[g, rs, :] if k == 0 else vk[k - 1, g, rs, :]

    def strip_parts(k, tile):
        rs = at(tile)
        x = strips[k, rs, :]
        xe, xw = roll(x, cols - 1), roll(x, 1)
        if k == 0:
            near = beyond[rs, :]
            xe, xw = jnp.where(place == 7, near, xe), jnp.where(place == 8, near, xw)
        return x, parts(x, xe, xw, [coefs[q, rs, :] for q in range(8)])

    def member_parts(k, g, tile, c=None):
        rs = at(tile)
        x = source(k, g, rs)
        if c is None:
            c = [coefm[q, rs, :] for q in range(8)]
        return x, parts(x, roll(x, cols - 1), roll(x, 1), c)

    batch = BATCH
    for k in range(ITERS):
        def sweep(p, carry):
            gs = [p * batch + i for i in range(batch)]
            state = []
            for g in gs:
                _, (cross, upper, lower) = member_parts(k, g, first)
                state.append((cross + shift_down(zero, lower), upper, lower, zero, zero, zero))

            def step(t, state):
                state = list(state)
                tile = first + 1 + t
                c = [coefm[q, at(tile), :] for q in range(8)]
                weight = cen[at(tile - first), :]
                for i, g in enumerate(gs):
                    sofar, u_old, d_old, w_old, acc0, acc1 = state[i]
                    x, (cross, upper, lower) = member_parts(k, g, tile, c)
                    out = sofar + shift_up(u_old, upper)
                    vk[k, g, at(tile - 1), :] = out
                    acc1 = acc1 + w_old * out
                    w = weight * x
                    acc0 = acc0 + w * x
                    state[i] = (cross + shift_down(d_old, lower), upper, lower, w, acc0, acc1)
                return tuple(state)
            state = lax.fori_loop(0, inner, step, tuple(state), unroll=split(inner, 22))
            for i, g in enumerate(gs):
                sofar, u_old, d_old, w_old, acc0, acc1 = state[i]
                _, (cross, upper, lower) = member_parts(k, g, last)
                out = sofar + shift_up(u_old, upper)
                vk[k, g, at(last - 1), :] = out
                vk[k, g, at(last), :] = cross + shift_down(d_old, lower) + shift_up(upper, zero)
                macc[2 * k, g] = acc0
                macc[2 * k + 1, g] = acc1 + w_old * out
            return carry
        lax.fori_loop(0, members // batch, sweep, 0)

    @pl.when(lat_last)
    def _():
        settle(fold.at[pl.ds(0, half - 1), sent], fold_sem.at[1])
        for c in relays:
            c.start()

    def join(lo_parts, mid, hi_parts):
        out = mid[0]
        out = out + shift_down(zero if lo_parts is None else lo_parts[2], mid[2])
        return out + shift_up(mid[1], zero if hi_parts is None else hi_parts[1])

    def bands(outer_tile, edge_tile, inner_tile):
        south_edge = outer_tile < edge_tile
        main_coefs(outer_tile)
        main_coefs(edge_tile)
        for k in range(ITERS):
            def band(g, carry):
                far, mid, near = (
                    member_parts(k, g, t) for t in (outer_tile, edge_tile, inner_tile))
                ordered = (far[1], mid[1], near[1]) if south_edge else (near[1], mid[1], far[1])
                if k + 1 < ITERS:
                    vk[k, g, at(outer_tile), :] = (
                        join(None, far[1], mid[1]) if south_edge else join(mid[1], far[1], None))
                out = join(*ordered)
                vk[k, g, at(edge_tile), :] = out
                x = mid[0]
                w = cen[at(edge_tile - first), :] * x
                macc[2 * k, g] = macc[2 * k, g] + w * x
                macc[2 * k + 1, g] = macc[2 * k + 1, g] + w * out
                return carry
            lax.fori_loop(0, members, band, 0, unroll=members)

    def take_rows(side, tile, seen):
        rs = at(tile)

        def clean(x):
            return jnp.where(seen, x, 0.0)
        for a in range(ARRAYS):
            if a not in (RIM, KRIM):
                st[a, rs, :] = clean(rowin[side, a])

    def take_corners(side, tile, seen):
        def clean(x):
            return jnp.where(seen, x, 0.0)
        o, k = clean(rowin[side, RIM]), clean(rowin[side, KRIM])
        ow, kw = (clean(diagin[2 * side, i]) for i in range(2))
        oe, ke = (roll(clean(diagin[2 * side + 1, i]), 10) for i in range(2))
        put_strip(at(tile), unfold(o, k, ow, kw, oe, ke))

    @pl.when(not_first)
    def _():
        settle(rowin.at[0, :, low], recv_sem.at[UP])
        take_rows(0, first - 1, sub > 4)

    @pl.when(lat_first)
    def _():
        rs = at(first - 1)
        for a in range(ARRAYS):
            st[a, rs, :] = zero
        put_strip(rs, (zero, zero, zero))

    bands(first - 1, first, first + 1)

    @pl.when(not_last)
    def _():
        settle(rowin.at[1, :, high], recv_sem.at[DOWN])
        take_rows(1, last + 1, sub < 3)
        bands(last + 1, last, last - 1)

    def merge(g, ref):
        def step(t, carry):
            fw, fe = (loose[i, t] if g else packin[i, 0, t] for i in range(2))
            for q in range(4):
                rs = at(first + t * 4 + q)
                x = ref[rs, :]
                keep = lane < EXTRA if g else lane >= 0
                x = jnp.where(jnp.logical_and(place < 3, keep),
                              roll(fw, (-3 * q) % cols) if q else fw, x)
                ref[rs, :] = jnp.where(jnp.logical_and(place > 12, keep), roll(fe, 10 - 3 * q), x)
            return carry
        lax.fori_loop(0, tiles // 4, step, 0, unroll=split(tiles // 4, 6))
    settle(packin.at[:, 1, pl.ds(0, dense_count)], recv_sem.at[SIDES_K])
    for side in range(2):
        unsqueeze(side)
    merge(1, kstrip)

    def edge_spread(t, carry):
        spread_tile(first + t)
        return carry
    lax.fori_loop(0, tiles - 1, edge_spread, 0, unroll=split(tiles - 1, 23))

    settle(packin.at[:, 0], recv_sem.at[SIDES])
    merge(0, strips.at[0])

    @pl.when(not_first)
    def _():
        settle(diagin.at[pl.ds(0, 2), :, low], recv_sem.at[UP_CORNERS])
        take_corners(0, first - 1, sub > 4)

    @pl.when(not_last)
    def _():
        settle(diagin.at[pl.ds(2, 2), :, high], recv_sem.at[DOWN_CORNERS])
        take_corners(1, last + 1, sub < 3)

    spread_tile(first - 1)

    @pl.when(lat_last)
    def _():
        settle(fold.at[pl.ds(0, half), sent], fold_sem.at[2])
        total = lon_count * cols
        rs = at(last + 1)
        shown = jnp.where(place < 8, place - 3, place + (cols - 13))
        origin = lax.rem(partner[0, 0] - lo * cols + total, total)

        def view(shift):
            start = lax.rem(origin + shift + total, total)
            chunk = lax.div(start, cols)
            head = start - chunk * cols
            slots = [lax.rem(chunk + o + 2 * lon_count, lon_count) for o in (1, 0, -1, -2)]
            z = head - shown
            return (slots, jnp.bitwise_and(head - lane, cols - 1), lane <= head,
                    jnp.bitwise_and(z, cols - 1), (z >= cols, z >= 0, z >= -cols))

        def take(x, where):
            return jnp.take_along_axis(x, where, axis=1, mode="promise_in_bounds")
        views = {s: view(s) for s in (-1, 0, 1)}
        shifts = {EAST: -1, NEAST: -1, NWEST: 1}
        ghost = [zero, zero]
        blocks = []
        for i, a in enumerate(fold_arrays):
            slots, where, within, where_s, (far, near, back) = views[shifts.get(a, 0)]
            chunks = [jnp.where(sub < len(fold_picks[a]), fold[s, pl.ds(fold_start[i], 8), :], 0.0) for s in slots]
            block = jnp.where(within, take(chunks[1], where), take(chunks[2], where))
            st[a, rs, :] = block
            blocks.append(block)
            x = jnp.where(back, take(chunks[2], where_s), take(chunks[3], where_s))
            x = jnp.where(near, take(chunks[1], where_s), x)
            x = jnp.where(far, take(chunks[0], where_s), x)
            s, g = (0, a) if a < members else (1, COUPLED.index(a))
            ghost[s] = jnp.where(group == g, x, ghost[s])
            if a == NORTH:
                end = pl.ds(EDGE + rows - 1, 1)
                st[NORTH, end, :] = 0.5 * (st[NORTH, end, :] + block[2:3, :])
                spare[...] = x
                st[NEAST, end, :] = jnp.zeros((1, cols), f32)
                st[NWEST, end, :] = jnp.zeros((1, cols), f32)
        o, k = rim(blocks[:members]), rim(blocks[members:])
        ring = unfold(o, k, zero, zero, zero, zero)[1]
        put_strip(rs, (ghost[0], ring, extras(ghost[1], k)))
        end = pl.ds(EDGE + rows - 1, 1)
        mixed = 0.5 * (kstrip[end, :] + spare[pl.ds(2, 1), :])
        g1, l1 = group[0:1, :], lane[0:1, :]
        dropped = jnp.logical_or(jnp.logical_or(g1 == 2, g1 == 3),
                                 jnp.logical_or(l1 == EXTRA + 1, l1 == EXTRA + 2))
        kstrip[end, :] = jnp.where(dropped, 0.0, jnp.where(g1 == 1, mixed, kstrip[end, :]))
        bands(last + 1, last, last - 1)

    spread_tile(last)
    spread_tile(last + 1)

    def edge_coefs(t, carry):
        strip_coefs(first - 1 + t)
        return carry
    lax.fori_loop(0, tiles + 2, edge_coefs, 0, unroll=split(tiles + 2, 26))

    for k in range(ITERS):
        _, (cross, upper, lower) = strip_parts(k, first - 1)

        def strip_step(t, carry):
            sofar, u_old, d_old, w_old, acc0, acc1 = carry
            tile = first + t
            x, (cross, upper, lower) = strip_parts(k, tile)
            out = sofar + shift_up(u_old, upper)
            strips[k + 1, at(tile - 1), :] = out
            acc1 = acc1 + w_old * out
            w_old = coefs[8, at(tile), :] * x
            acc0 = acc0 + w_old * x
            return cross + shift_down(d_old, lower), upper, lower, w_old, acc0, acc1
        sofar, u_old, d_old, w_old, acc0, acc1 = lax.fori_loop(
            0, tiles, strip_step,
            (cross + shift_down(zero, lower), upper, lower, zero, zero, zero),
            unroll=split(tiles, 24))
        _, (cross, upper, lower) = strip_parts(k, last + 1)
        out = sofar + shift_up(u_old, upper)
        strips[k + 1, at(last), :] = out
        strips[k + 1, at(last + 1), :] = cross + shift_down(d_old, lower) + shift_up(upper, zero)
        sacc[2 * k] = acc0
        sacc[2 * k + 1] = acc1 + w_old * out

    def column_sum(x):
        for s in (4, 2, 1):
            x = x + roll(x, s, 0)
        return x
    row = zero
    for i in range(2 * ITERS):
        total = macc[i, :, 0, :]
        for s in range(1, 8):
            total = total + macc[i, :, s, :]
        total = jnp.where(jnp.logical_and(lane > 2, lane < cols - 3), total, 0.0)
        total = total + jnp.where(group == sub, column_sum(sacc[i]), 0.0)
        total = jnp.sum(total, axis=1, keepdims=True)
        row = jnp.where(lane == 8 * i + sub, total, row)

    row = column_sum(row)

    outer = jnp.logical_or(lane < 3, lane > cols - 4)

    def close_rims(stages):
        for k in stages:
            def close(t, carry):
                rs = at(first + t)
                x = strips[k, rs, :]
                x = jnp.where(place < 3, roll(x, cols - 10), x)
                for m in range(members):
                    edge = roll(x, (cols - 3 - SLOT * m) % cols)
                    vk[k - 1, m, rs, :] = jnp.where(outer, edge, vk[k - 1, m, rs, :])
                return carry
            lax.fori_loop(0, tiles, close, 0, unroll=split(tiles, 8))

    everyone = lat_count * lon_count
    spots = [(i, j) for i in range(lat_count) for j in range(lon_count) if i or j]
    mine = pl.ds(la * lon_count + lo, 1)
    red[...] = row
    redin[mine, :] = row[0:1, :]
    pl.semaphore_wait(known, lat_count - 1)
    for i, j in reversed(spots):
        pltpu.make_async_remote_copy(
            src_ref=red.at[pl.ds(0, 1)], dst_ref=redin.at[mine],
            send_sem=red_sem.at[0], recv_sem=red_sem.at[1],
            device_id=(lax.rem(la + i, lat_count), lax.rem(lo + j, lon_count)),
            device_id_type=MESH).start()
    close_rims(range(1, ITERS + 1))
    settle(redin.at[pl.ds(0, everyone - 1)], red_sem.at[1])
    row = zero
    for i in range(-(-everyone // 8)):
        tile = redin[pl.ds(8 * i, 8), :]
        row = row + (tile if 8 * i + 8 <= everyone else jnp.where(sub < everyone - 8 * i, tile, 0.0))
    row = column_sum(row)

    m0, m1, m2, m3, m4, m5 = (
        jnp.broadcast_to(
            jnp.sum(jnp.where(lane == 8 * i + sub, row, 0.0), axis=1, keepdims=True), (8, cols))
        for i in range(2 * ITERS))
    a0 = m1 / m0
    h1 = m2 - a0 * m1
    a1 = (m3 - 2.0 * a0 * m2 + a0 * a0 * m1) / h1
    b1 = h1 / m0
    p1 = -(a0 + a1)
    p0 = a0 * a1 - b1
    h2 = m4 + p1 * m3 + p0 * m2
    a2 = (m5 + p1 * m4 + p0 * m3) / h2 + p1
    b2 = h2 / h1
    t2 = p1 - a2
    t1 = p0 - a2 * p1 - b2
    t0 = b2 * a0 - a2 * p0
    q3 = 1.0 / (1.0 + t2 + t1 + t0)
    q2, q1, q0 = t2 * q3, t1 * q3, t0 * q3
    for i, value in enumerate((q3 + q2 + q1, q2 + q3, q3, q0, q1, q2, q3)):
        mix[i] = value

    settle(st.at[0, pl.ds(0, 16 * (packed + dense_count))], send_sem.at[SIDES])
    settle(redin.at[pl.ds(0, everyone - 1)], red_sem.at[0])

    @pl.when(not_last)
    def _():
        settle(st.at[0, pl.ds(0, 3 * (ARRAYS + 4))], send_sem.at[UP])

    @pl.when(not_first)
    def _():
        settle(st.at[0, pl.ds(0, 3 * (ARRAYS + 4))], send_sem.at[DOWN])

    @pl.when(lat_last)
    def _():
        settle(fold.at[pl.ds(0, 2 * half - 1), sent], fold_sem.at[0])


def finish(st, vk, mix, center, sol_out, res_out, obuf, store_sem):
    members, rows, cols = sol_out.shape

    def one(m, carry):
        s0, s1, s2, q0, q1, q2, q3 = (
            jnp.broadcast_to(mix[i, pl.ds(m, 1), :], (8, cols)) for i in range(7))
        for t in range(rows // 8):
            here, rs = pl.ds(8 * t, 8), pl.ds(EDGE + 8 * t, 8)
            v0, v1, v2, v3 = st[m, rs, :], vk[0, m, rs, :], vk[1, m, rs, :], vk[2, m, rs, :]
            obuf[0, m, here, :] = s0 * v0 + s1 * v1 + s2 * v2
            obuf[1, m, here, :] = center[here, :] * (q0 * v0 + q1 * v1 + q2 * v2 + q3 * v3)
        for o, dst in ((0, sol_out), (1, res_out)):
            pltpu.make_async_copy(obuf.at[o, m], dst.at[m], store_sem.at[0]).start()
        return carry
    lax.fori_loop(0, members, one, 0)
    pltpu.make_async_copy(obuf, obuf, store_sem.at[0]).wait()


def body(lat_count, lon_count, right_side, center, couplings, land_sea, fold_partner):
    members, rows, cols = right_side.shape
    f32 = jnp.float32
    hbm = pl.BlockSpec(memory_space=pltpu.HBM)
    vmem = pl.BlockSpec(memory_space=pltpu.VMEM)
    dma = pltpu.SemaphoreType.DMA
    shape = jax.ShapeDtypeStruct(right_side.shape, f32)
    high = rows + 2 * EDGE
    tiles = rows // 8
    folded = -(-3 * (members + len(COUPLED)) // 8) * 8 + 8
    st, vk, mix, cen = pl.pallas_call(
        functools.partial(kernel, lat_count, lon_count),
        out_shape=(pltpu.VMEM((ARRAYS, high, cols), f32),
                   pltpu.VMEM((ITERS, members, high, cols), f32),
                   pltpu.VMEM((7, 8, cols), f32),
                   pltpu.VMEM((rows, cols), f32)),
        in_specs=[hbm] * 5,
        out_specs=(vmem, vmem, vmem, vmem),
        scratch_shapes=[
            pltpu.VMEM((rows, cols), jnp.int32),
            pltpu.SMEM((1, cols), jnp.int32),
            pltpu.VMEM((ITERS + 1, high, cols), f32),
            pltpu.VMEM((high, cols), f32),
            pltpu.VMEM((high, cols), f32),
            pltpu.VMEM((8, high, cols), f32),
            pltpu.VMEM((9, high, cols), f32),
            pltpu.VMEM((4, high, cols), f32),
            pltpu.VMEM((2, 2, tiles // 4, 8, cols), f32),
            pltpu.VMEM((2, 2, tiles // 4, 8, cols), f32),
            pltpu.VMEM((2, tiles // 4, 8, cols), f32),
            pltpu.VMEM((2, ARRAYS, 8, cols), f32),
            pltpu.VMEM((4, 2, 8, cols), f32),
            pltpu.VMEM((lon_count, folded, cols), f32),
            pltpu.VMEM((2 * ITERS, members, 8, cols), f32),
            pltpu.VMEM((2 * ITERS, 8, cols), f32),
            pltpu.VMEM((8, cols), f32),
            pltpu.VMEM((8, cols), f32),
            pltpu.VMEM((-(-lat_count * lon_count // 8) * 8, cols), f32),
            dma((3,)), dma((3,)), dma((6,)), dma((3,)), dma((2,)),
            pltpu.SemaphoreType.REGULAR,
        ],
        compiler_params=pltpu.CompilerParams(
            collective_id=0, has_side_effects=True, vmem_limit_bytes=32 * 1024 * 1024),
    )(*(pltpu.with_memory_space_constraint(x, pltpu.HBM) for x in (
        right_side, center, couplings, land_sea, fold_partner.reshape(lon_count, cols))))
    return pl.pallas_call(
        finish,
        out_shape=(shape, shape),
        in_specs=[vmem] * 4,
        out_specs=(hbm, hbm),
        scratch_shapes=[
            pltpu.VMEM((2, members, rows, cols), f32),
            dma((1,)),
        ],
        compiler_params=pltpu.CompilerParams(vmem_limit_bytes=16 * 1024 * 1024),
    )(st, vk, mix, cen)


def solution(mesh):
    return jax.shard_map(
        functools.partial(body, mesh.shape["lat"], mesh.shape["lon"]),
        mesh=mesh,
        in_specs=(
            P(None, "lat", "lon"),
            P("lat", "lon"),
            P(None, "lat", "lon"),
            P("lat", "lon"),
            P(),
        ),
        out_specs=(P(None, "lat", "lon"), P(None, "lat", "lon")),
        check_vma=False,
    )
```
